256 devices in a mesh: cells: 64 (over y, z, core), leaf: 4 (over x).
Axes of the slice: x: 4, y: 4, z: 8, core: 2. Of those that a mesh axis runs over, the one named last changes fastest.
Arguments:
- displacement: float32 [3, 119808], P(None, 'cells'), may hold values from -0.9 to 0.9
- point_leaf: int32 [119808], P('cells'), may hold values from 0 to 2047, as said below
- near_list: int32 [48, 2048], replicated, may hold values from -1 to 2047, as said below
- far_list: int32 [48, 2048], replicated, may hold values from -1 to 2047, as said below
- stiffness: float32 [312, 312], replicated, may hold values from -0.3125 to 0.3125
- up_inverse: float32 [168, 168], replicated, may hold values from -9 to 9
- down_inverse: float32 [168, 168], replicated, may hold values from -9 to 9
Outputs:
- velocity: float32 [3, 119808], P(None, 'cells')
The draws below stay inside these ranges and needn't reach their ends.
Inputs may be any that keep to these rules, and one draw needn't show every extreme that they name: `point_leaf`: leaf L belongs to owner L // 32. All 312 points of one cell lie in at most three consecutive leaves of one owner, and that owner's index differs from the index of cells that holds the cell by at most one, cyclically (the last owner and owner 0 count as adjacent). Among the 1872 points of one index of cells, at most 936 lie in the leaves of one owner, and on every index some owner receives exactly 936. `near_list`: column L holds L itself and distinct leaves L' with |L' // 16 - L // 16| <= 1; the other entries are -1. `far_list`: column L holds distinct leaves L' with |L' // 16 - L // 16| >= 2, at least half the column, followed by -1 in the remaining entries.
All inputs are finite; a program needn't handle non-finite values.
Results may differ from the reference program's by a relative error of at most 0.0003.
Values sent between devices are 32-bit elements; how exact they have to be, the bound alone decides.
A program may use at most 64 MiB of HBM per device.

```python
import math
import jax
import jax.numpy as jnp
import numpy as np
from jax import lax

NPT = 312
CPD = 6
SLICE = 16
EQUIV = 56
FAR = 48
NPTS = 119808
SLOTS = 2808
NLEAF = 2048
N_CELLS = 64


def draw_point_leaf(key, part):
    half = CPD // 2
    per_owner = 2 * SLICE
    lane_slots = 3 * half

    def one_device(device, device_key):
        pick_key, score_key, shuffle_key, home_key, step_key = jax.random.split(device_key, 5)
        favoured = jax.random.randint(pick_key, (), 0, 3)
        slot_ids = jnp.arange(lane_slots, dtype=jnp.int32)
        lane_of = slot_ids // half
        scores = jax.random.randint(score_key, (lane_slots,), 0, 4096) * lane_slots + slot_ids
        scores = scores + jnp.where(lane_of == favoured, 1 << 30, 0)
        chosen = lax.top_k(scores, CPD)[1].astype(jnp.int32)
        lane = jax.random.permutation(shuffle_key, chosen // half)
        owner = (device + lane - 1 + N_CELLS) % N_CELLS
        home = jax.random.randint(home_key, (CPD,), 0, per_owner)
        step = jax.random.randint(step_key, (CPD, NPT), -1, 2)
        within = jnp.clip(home[:, None] + step, 0, per_owner - 1)
        return (owner[:, None] * per_owner + within).reshape(-1)
    device_keys = jax.random.split(jax.random.fold_in(key, 101), N_CELLS)
    devices = jnp.arange(N_CELLS, dtype=jnp.int32)
    return jax.vmap(one_device)(devices, device_keys).reshape(-1).astype(jnp.int32)


def draw_near_list(key, part):
    leaves = jnp.arange(NLEAF, dtype=jnp.int32)
    slab = leaves // SLICE
    candidate = (slab[:, None] - 1) * SLICE + jnp.arange(3 * SLICE, dtype=jnp.int32)[None, :]
    keep = jax.random.randint(jax.random.fold_in(key, 202), (NLEAF, 3 * SLICE), 0, 4) > 0
    valid = (candidate >= 0) & (candidate < NLEAF) & (keep | (candidate == leaves[:, None]))
    return jnp.where(valid, candidate, -1).astype(jnp.int32).T


def draw_far_list(key, part):
    score_key = jax.random.fold_in(key, 303)
    count_key = jax.random.fold_in(key, 304)
    leaves = jnp.arange(NLEAF, dtype=jnp.int32)
    slab = leaves // SLICE
    distance = jnp.abs(slab[None, :] - slab[:, None])
    scores = jax.random.randint(score_key, (NLEAF, NLEAF), 0, 4096) * NLEAF + leaves[None, :]
    scores = scores + jnp.where(distance >= 2, 1 << 26, 0)
    chosen = lax.top_k(scores, FAR)[1].astype(jnp.int32)
    lengths = jax.random.randint(count_key, (NLEAF,), FAR // 2, FAR + 1)
    position = jnp.arange(FAR, dtype=jnp.int32)[None, :]
    return jnp.where(position < lengths[:, None], chosen, -1).astype(jnp.int32).T


def shard_levels(own_key, extent, cuts, smallest, high):
    factor_of = 1.0
    for dim, parts in cuts:
        draws = jax.random.uniform(jax.random.fold_in(jax.random.fold_in(own_key, 6), dim), (parts,), jnp.float32, smallest / len(cuts), high / len(cuts))
        factor_of = factor_of * jnp.repeat(jnp.exp(draws), extent[dim] // parts).reshape((-1,) + (1,) * (len(extent) - 1 - dim))
    return factor_of


def gaussian(rng, extent, scale, bound, kind=jnp.bfloat16):
    values = jax.random.normal(rng, extent, jnp.float32) * scale
    return jnp.minimum(jnp.maximum(values, -bound), bound).astype(kind)


def setup_inputs(seed: int = 0) -> dict:
    key_of = jax.random.split(jax.random.key(seed), 8)
    displacement = jnp.clip(jax.random.uniform(key_of[0], (3, NPTS), jnp.float32, -0.9, 0.9) * shard_levels(key_of[0], (3, NPTS), ((1, 64),), -0.4, 0.0), -0.9, 0.9)
    point_leaf = draw_point_leaf(jax.random.fold_in(key_of[7], 71), 0)
    near_list = draw_near_list(jax.random.fold_in(key_of[7], 71), 0)
    far_list = draw_far_list(jax.random.fold_in(key_of[7], 71), 0)
    stiffness = gaussian(key_of[4], (NPT, NPT), NPT ** -0.5, 0.3125, jnp.float32)
    up_inverse = gaussian(key_of[5], (3 * EQUIV, 3 * EQUIV), 1.5, 9.0, jnp.float32)
    down_inverse = gaussian(key_of[6], (3 * EQUIV, 3 * EQUIV), 1.5, 9.0, jnp.float32)
    return {"displacement": displacement, "point_leaf": point_leaf, "near_list": near_list, "far_list": far_list, "stiffness": stiffness, "up_inverse": up_inverse, "down_inverse": down_inverse}


inv_eight_pi = 1.0 / (8.0 * math.pi)
smooth_sq = 0.0625
inner_radius = 1.05
outer_radius = 2.95
highest = lax.Precision.HIGHEST

def surface_table():
    ladder = [-1.0, -1.0 / 3.0, 1.0 / 3.0, 1.0]
    corners = [(xshift, yshift, zshift) for xshift in ladder for yshift in ladder for zshift in ladder if max(abs(xshift), abs(yshift), abs(zshift)) == 1.0]
    return np.array(corners, dtype=np.float32).T

def leaf_centers(leaves):
    along = leaves // SLICE
    across = leaves % SLICE // 4
    height = leaves % 4
    return jnp.stack([2 * along + 1, 2 * across + 1, 2 * height + 1]).astype(jnp.float32)

def stokeslet(target, source, strength):
    offset = target - source
    radius_sq = lax.optimization_barrier(jnp.sum(offset * offset, axis=0))
    inner = lax.optimization_barrier(jnp.sum(offset * strength, axis=0))
    shifted = radius_sq + smooth_sq
    factor = inv_eight_pi * lax.rsqrt(shifted) / shifted
    return factor * ((radius_sq + 2.0 * smooth_sq) * strength + inner * offset)

def reference(displacement, point_leaf, near_list, far_list, stiffness, up_inverse, down_inverse):
    near_rows_all = near_list.T
    far_rows_all = far_list.T
    surface = jnp.asarray(surface_table())
    npoints = displacement.shape[1]
    membrane = displacement.reshape(3, npoints // NPT, NPT)
    forces = jnp.einsum('acn,nm->acm', membrane, stiffness, precision=highest).reshape(3, npoints)
    point_mid = leaf_centers(point_leaf)
    positions = point_mid + displacement
    check_up = point_mid[:, None, :] + outer_radius * surface[:, :, None]
    upward_terms = stokeslet(check_up, positions[:, None, :], forces[:, None, :]).reshape(3 * EQUIV, npoints)
    upward = jax.ops.segment_sum(upward_terms.T, point_leaf, num_segments=NLEAF).T
    density = jnp.dot(up_inverse, upward, precision=highest)
    leaf_ids = jnp.arange(NLEAF, dtype=jnp.int32)

    def far_one(entry):
        target, sources = entry
        usable = (sources >= 0).astype(density.dtype)
        safe = jnp.maximum(sources, 0)
        check = leaf_centers(target)[:, None, None, None] + inner_radius * surface[:, :, None, None]
        equiv = leaf_centers(safe)[:, None, :] + inner_radius * surface[:, :, None]
        push = jnp.take(density, safe, axis=1).reshape(3, EQUIV, -1) * usable
        return lax.optimization_barrier(jnp.sum(stokeslet(check, equiv[:, None], push[:, None]), axis=(2, 3)))
    downward = lax.map(far_one, (leaf_ids, far_rows_all))
    downward = downward.reshape(NLEAF, 3 * EQUIV).T
    local = jnp.dot(down_inverse, downward, precision=highest)
    equiv_down = point_mid[:, None, :] + outer_radius * surface[:, :, None]
    spread = jnp.take(local, point_leaf, axis=1).reshape(3, EQUIV, npoints)
    far_velocity = lax.optimization_barrier(jnp.sum(stokeslet(positions[:, None, :], equiv_down, spread), axis=1))
    owner_of = point_leaf // (2 * SLICE)
    order = jnp.argsort(point_leaf, stable=True).astype(jnp.int32)
    counts = jnp.zeros((N_CELLS,), jnp.int32).at[owner_of].add(1)
    starts = (jnp.cumsum(counts) - counts).astype(jnp.int32)
    margin = 3 * SLOTS
    sorted_leaf = jnp.concatenate([point_leaf[order], -jnp.ones((margin,), jnp.int32)])
    sorted_pos = jnp.concatenate([positions[:, order], jnp.zeros((3, margin), positions.dtype)], axis=1)
    sorted_force = jnp.concatenate([forces[:, order], jnp.zeros((3, margin), forces.dtype)], axis=1)
    near_cols = jnp.where(near_rows_all >= 0, near_rows_all, NLEAF)
    near_table = jnp.zeros((NLEAF, NLEAF + 1), positions.dtype).at[leaf_ids[:, None], near_cols].set(1.0)[:, :NLEAF]

    def per_owner(owner):
        begin = starts[jnp.maximum(owner - 1, 0)]
        src_leaf = lax.dynamic_slice_in_dim(sorted_leaf, begin, margin, 0)
        src_pos = lax.dynamic_slice_in_dim(sorted_pos, begin, margin, 1)
        src_force = lax.dynamic_slice_in_dim(sorted_force, begin, margin, 1)
        src_safe = jnp.maximum(src_leaf, 0)
        src_live = (src_leaf >= 0).astype(positions.dtype)

        def per_block(index):
            first = starts[owner] + index * NPT
            tgt_leaf = lax.dynamic_slice_in_dim(sorted_leaf, first, NPT, 0)
            tgt_pos = lax.dynamic_slice_in_dim(sorted_pos, first, NPT, 1)
            tgt_live = (tgt_leaf // (2 * SLICE) == owner).astype(positions.dtype)
            rows = near_table[jnp.maximum(tgt_leaf, 0)]
            weight = jnp.take(rows, src_safe, axis=1) * src_live[None, :] * tgt_live[:, None]
            pulls = stokeslet(tgt_pos[:, :, None], src_pos[:, None, :], src_force[:, None, :])
            return lax.optimization_barrier(jnp.sum(pulls * weight[None], axis=2))
        blocks = lax.map(per_block, jnp.arange(SLOTS // NPT, dtype=jnp.int32))
        return jnp.transpose(blocks, (1, 0, 2)).reshape(3, SLOTS)
    near_blocks = lax.map(per_owner, jnp.arange(N_CELLS, dtype=jnp.int32))
    near_flat = jnp.transpose(near_blocks, (1, 0, 2)).reshape(3, N_CELLS * SLOTS)
    slot_ids = jnp.arange(SLOTS, dtype=jnp.int32)
    valid = slot_ids[None, :] < counts[:, None]
    place = jnp.where(valid, starts[:, None] + slot_ids[None, :], npoints).reshape(-1).astype(jnp.int32)
    near_sorted = jnp.zeros((3, npoints + 1), positions.dtype).at[:, place].add(near_flat)[:, :npoints]
    near_velocity = jnp.zeros((3, npoints), positions.dtype).at[:, order].set(near_sorted)
    return near_velocity + far_velocity
```

```python
import math

import jax
import jax.numpy as jnp
import numpy as np
from jax import lax
from jax.experimental import pallas as pl
from jax.experimental.pallas import tpu as pltpu
from jax.sharding import PartitionSpec as P

NPT = 312
CPD = 6
SLICE = 16
EQUIV = 56
FAR = 48
ROWS = 3 * EQUIV
PER_OWNER = 2 * SLICE
WIDE = 384
OFFSETS = (1, -1, 2, -2, 3, -3)
CELLS = CPD * (len(OFFSETS) + 1)
OWNABLE = 3 * CPD
SHARE = NPT // 4
SHARE_PAD = 80
COUNT = 127

inv_eight_pi = 1.0 / (8.0 * math.pi)
smooth_sq = 0.0625
inner_radius = 1.05
outer_radius = 2.95
MESH = pl.DeviceIdType.MESH
VMEM = pl.BlockSpec(memory_space=pltpu.VMEM)
SMEM = pl.BlockSpec(memory_space=pltpu.SMEM)
f32 = jnp.float32
bf16 = jnp.bfloat16
i32 = jnp.int32


def surface_table():
    ladder = [-1.0, -1.0 / 3.0, 1.0 / 3.0, 1.0]
    corners = [
        (a, b, c)
        for a in ladder
        for b in ladder
        for c in ladder
        if max(abs(a), abs(b), abs(c)) == 1.0
    ]
    return np.array(corners, dtype=np.float32)


def iota(shape, dim):
    return lax.broadcasted_iota(i32, shape, dim)


def dot(a, b):
    return jnp.dot(a, b, preferred_element_type=f32)


def dot_nt(a, b):
    return lax.dot_general(a, b, (((1,), (1,)), ((), ())), preferred_element_type=f32)


def halves(value):
    top = value.astype(bf16)
    return top, (value - top.astype(f32)).astype(bf16)


def dot_wide(a, b):
    a_top, a_low = halves(a)
    b_top, b_low = halves(b)
    return dot(a_top, b_top) + (dot(a_top, b_low) + dot(a_low, b_top))


def spread_kernel(axis, offsets, x_ref, o_ref, send_sem, recv_sem):
    count = lax.axis_size(axis)
    me = lax.axis_index(axis)
    targets = [{axis: lax.rem(me + (off + count), count)} for off in offsets]
    barrier = pltpu.get_barrier_semaphore()
    for target in targets:
        pl.semaphore_signal(barrier, inc=1, device_id=target, device_id_type=MESH)
    pl.semaphore_wait(barrier, len(targets))
    copies = [
        pltpu.make_async_remote_copy(
            src_ref=x_ref,
            dst_ref=o_ref.at[slot],
            send_sem=send_sem.at[slot],
            recv_sem=recv_sem.at[slot],
            device_id=target,
            device_id_type=MESH,
        )
        for slot, target in enumerate(targets)
    ]
    for copy in copies:
        copy.start()
    for copy in copies:
        copy.wait()


def spread(x, axis, offsets, collective_id):
    count = len(offsets)

    def kernel(*refs):
        spread_kernel(axis, offsets, *refs)

    return pl.pallas_call(
        kernel,
        out_shape=jax.ShapeDtypeStruct((count, *x.shape), x.dtype),
        in_specs=[VMEM],
        out_specs=VMEM,
        scratch_shapes=[pltpu.SemaphoreType.DMA((count,)), pltpu.SemaphoreType.DMA((count,))],
        compiler_params=pltpu.CompilerParams(collective_id=collective_id, has_side_effects=True),
        name=f"spread_{collective_id}",
    )(x)


def leaf_sum(x, collective_id):
    offsets = (1, 2, 3)

    def kernel(x_ref, o_ref, held, send_sem, recv_sem):
        spread_kernel("leaf", offsets, x_ref, held, send_sem, recv_sem)
        o_ref[...] = (x_ref[...] + held[1]) + (held[0] + held[2])

    return pl.pallas_call(
        kernel,
        out_shape=jax.ShapeDtypeStruct(x.shape, x.dtype),
        in_specs=[VMEM],
        out_specs=VMEM,
        scratch_shapes=[
            pltpu.VMEM((3, *x.shape), x.dtype),
            pltpu.SemaphoreType.DMA((3,)),
            pltpu.SemaphoreType.DMA((3,)),
        ],
        compiler_params=pltpu.CompilerParams(collective_id=collective_id, has_side_effects=True),
        name="leaf_sum",
    )(x)


def gather_kernel(x_ref, o_ref, own_sem, z_send, z_recv, y_send, y_recv, c_send, c_recv):
    me = lax.axis_index("cells")
    core = lax.rem(me, 2)
    z = lax.rem(me // 2, 8)
    y = me // 16

    def device(y_at, z_at, core_at):
        return {"cells": (y_at * 8 + z_at) * 2 + core_at}

    z_targets = [device(y, lax.rem(z + k, 8), core) for k in range(1, 8)]
    y_targets = [device(lax.rem(y + k, 4), z, core) for k in range(1, 4)]
    c_target = device(y, z, 1 - core)
    barrier = pltpu.get_barrier_semaphore()
    for target in (*z_targets, *y_targets, c_target):
        pl.semaphore_signal(barrier, inc=1, device_id=target, device_id_type=MESH)
    row = core * 4 + y
    own = pltpu.make_async_copy(x_ref, o_ref.at[row, z], own_sem)
    own.start()
    pl.semaphore_wait(barrier, 11)
    z_copies = [
        pltpu.make_async_remote_copy(
            src_ref=x_ref,
            dst_ref=o_ref.at[row, z],
            send_sem=z_send.at[k],
            recv_sem=z_recv.at[k],
            device_id=target,
            device_id_type=MESH,
        )
        for k, target in enumerate(z_targets)
    ]
    for copy in z_copies:
        copy.start()
    own.wait()
    for copy in z_copies:
        copy.wait()
    y_copies = [
        pltpu.make_async_remote_copy(
            src_ref=o_ref.at[row],
            dst_ref=o_ref.at[row],
            send_sem=y_send.at[k],
            recv_sem=y_recv.at[k],
            device_id=target,
            device_id_type=MESH,
        )
        for k, target in enumerate(y_targets)
    ]
    for copy in y_copies:
        copy.start()
    c_copies = []
    for k in range(4):
        at = core * 4 + lax.rem(y - k + 4, 4)
        if k:
            y_copies[k - 1].wait_recv()
        copy = pltpu.make_async_remote_copy(
            src_ref=o_ref.at[at],
            dst_ref=o_ref.at[at],
            send_sem=c_send.at[k],
            recv_sem=c_recv.at[k],
            device_id=c_target,
            device_id_type=MESH,
        )
        copy.start()
        c_copies.append(copy)
    for copy in y_copies:
        copy.wait_send()
    for copy in c_copies:
        copy.wait()


def gather_blocks(x, collective_id):
    return pl.pallas_call(
        gather_kernel,
        out_shape=jax.ShapeDtypeStruct((8, 8, *x.shape), x.dtype),
        in_specs=[VMEM],
        out_specs=VMEM,
        scratch_shapes=[
            pltpu.SemaphoreType.DMA,
            pltpu.SemaphoreType.DMA((7,)),
            pltpu.SemaphoreType.DMA((7,)),
            pltpu.SemaphoreType.DMA((3,)),
            pltpu.SemaphoreType.DMA((3,)),
            pltpu.SemaphoreType.DMA((4,)),
            pltpu.SemaphoreType.DMA((4,)),
        ],
        compiler_params=pltpu.CompilerParams(collective_id=collective_id, has_side_effects=True),
        name="gather_blocks",
    )(x)


DX, DY, DZ, FX, FY, FZ, PX, PY, PZ, REL = range(10)


def prepare_kernel(own_ref, recv_ref, stiff_ref, comp_ref, lists_ref, disp, force):
    me = lax.axis_index("cells")
    disp[...] = jnp.zeros_like(disp)
    for home in range(len(OFFSETS) + 1):
        for k in range(CPD):
            at = slice(NPT * k, NPT * (k + 1))
            piece = own_ref[:, at] if home == 0 else recv_ref[home - 1, :, at]
            for a in range(4):
                row = 48 * a + home * CPD + k
                disp[row : row + 1, 0:NPT] = piece[a : a + 1, :]
    comp_ref[...] = jnp.zeros_like(comp_ref)
    force[...] = dot_wide(disp[0:144, 0:NPT], stiff_ref[...])
    live = iota((CELLS, WIDE), 1) < NPT
    leaf = disp[144 : 144 + CELLS, :].astype(i32)
    for a in range(3):
        comp_ref[DX + a, 0:48, :] = disp[48 * a : 48 * a + 48, :]
        comp_ref[FX + a, 0:48, 0:NPT] = force[48 * a : 48 * a + 48, :]
    rel = jnp.where(live, (leaf - PER_OWNER * (me - 4)) & 2047, -1)
    comp_ref[REL, 0:CELLS, :] = rel.astype(f32)
    comp_ref[PX, 0:CELLS, :] = comp_ref[DX, 0:CELLS, :] + (2 * (rel >> 4) + 1).astype(f32)
    comp_ref[PY, 0:CELLS, :] = comp_ref[DY, 0:CELLS, :] + (2 * ((rel >> 2) & 3) + 1).astype(f32)
    comp_ref[PZ, 0:CELLS, :] = comp_ref[DZ, 0:CELLS, :] + (2 * (rel & 3) + 1).astype(f32)
    relf = rel.astype(f32)
    first = jnp.min(jnp.where(live, relf, 1e9), axis=1, keepdims=True)
    last = jnp.max(relf, axis=1, keepdims=True)
    low = jnp.floor(first * (1.0 / 16.0))
    high = jnp.floor(last * (1.0 / 16.0))
    lane = iota((CELLS, 128), 1)
    which = iota((CELLS, 1), 0).astype(f32)
    flags = []
    for t in range(CPD):
        low_t, high_t = low[t : t + 1], high[t : t + 1]
        flags.append(jnp.where((high >= low_t - 1.0) & (low <= high_t + 1.0), 1.0, 0.0))
    owner = jnp.floor(low * 0.5)
    flags.append(jnp.where((owner == 4.0) & (which < float(OWNABLE)), 1.0, 0.0))
    table = jnp.zeros((CELLS, 128), f32)
    for t, flag in enumerate(flags):
        table = table + jnp.where(lane == t, flag, 0.0)
    before = (iota((CELLS, CELLS), 0) > iota((CELLS, CELLS), 1)).astype(f32)
    rank = dot(before, table)
    total = jnp.sum(table, axis=0, keepdims=True)
    lane_row = iota((1, 128), 1)
    for t, flag in enumerate(flags):
        hit = (rank[:, t : t + 1] == lane.astype(f32)) & (flag > 0.0)
        row = jnp.sum(jnp.where(hit, which, 0.0), axis=0, keepdims=True)
        row = jnp.where(lane_row == COUNT, total[:, t : t + 1], row)
        lists_ref[t : t + 1, :] = row.astype(i32)
    row = jnp.zeros((1, 128), f32)
    for t in range(CPD):
        row = row + jnp.where(lane_row == t, owner[t : t + 1] - 3.0, 0.0)
        row = row + jnp.where(lane_row == 8 + t, first[t : t + 1], 0.0)
    lists_ref[7:8, :] = row.astype(i32)


def prepare(own, recv, stiffness):
    return pl.pallas_call(
        prepare_kernel,
        out_shape=(
            jax.ShapeDtypeStruct((10, 48, WIDE), f32),
            jax.ShapeDtypeStruct((8, 128), i32),
        ),
        in_specs=[VMEM] * 3,
        out_specs=(VMEM, VMEM),
        scratch_shapes=[pltpu.VMEM((192, WIDE), f32), pltpu.VMEM((144, NPT), f32)],
        name="prepare",
    )(own, recv, stiffness)


def pull(offset, strength):
    dx, dy, dz = offset
    fx, fy, fz = strength
    shifted = (dx * dx + dy * dy) + (dz * dz + smooth_sq)
    inner = (dx * fx + dy * fy) + dz * fz
    root = lax.rsqrt(shifted)
    cube = root * root * root
    return root + smooth_sq * cube, cube * inner


def upward_kernel(lists, comp_ref, surf_ref, inverse_ref, block_ref, terms, total, density):
    portion = lax.axis_index("leaf")
    total[...] = jnp.zeros_like(total)

    def one_cell(index, carry):
        c = lists[6, index]
        d = [comp_ref[DX + a, pl.ds(c, 1), :] for a in range(3)]
        f = [comp_ref[FX + a, pl.ds(c, 1), :] for a in range(3)]
        rel = comp_ref[REL, pl.ds(c, 1), :].astype(i32) - 4 * PER_OWNER
        member = (iota((PER_OWNER, WIDE), 0) == rel).astype(f32).astype(bf16)
        for g in range(EQUIV // 8):
            at = slice(8 * g, 8 * g + 8)
            r = [outer_radius * surf_ref[at, a : a + 1] - d[a] for a in range(3)]
            even, along = pull(r, f)
            for a in range(3):
                terms[EQUIV * a + 8 * g : EQUIV * a + 8 * g + 8, :] = even * f[a] + along * r[a]
        top, low = halves(terms[...])
        total[...] += dot_nt(top, member) + dot_nt(low, member)
        return carry

    lax.fori_loop(0, lists[6, COUNT], one_cell, 0)
    density[...] = dot_wide(inverse_ref[...], total[...] * inv_eight_pi)
    block_ref[...] = jnp.zeros_like(block_ref)
    for part in range(4):

        @pl.when(portion == part)
        def _():
            for a in range(3):
                rows = density[EQUIV * a + 14 * part : EQUIV * a + 14 * part + 14, :]
                block_ref[0:14, PER_OWNER * a : PER_OWNER * (a + 1)] = rows


def upward(lists, comp, surf, up_inverse):
    return pl.pallas_call(
        upward_kernel,
        out_shape=jax.ShapeDtypeStruct((16, 128), f32),
        in_specs=[SMEM, VMEM, VMEM, VMEM],
        out_specs=VMEM,
        scratch_shapes=[
            pltpu.VMEM((ROWS, WIDE), f32),
            pltpu.VMEM((ROWS, PER_OWNER), f32),
            pltpu.VMEM((ROWS, PER_OWNER), f32),
        ],
        name="upward",
    )(lists, comp, surf, up_inverse)


def far_kernel(
    points, gat_ref, far_ref, surf_ref, inverse_ref, local_ref, far4, sources, packed, pushes, mids, total
):
    me = lax.axis_index("cells")
    portion = lax.axis_index("leaf")
    lane = iota((16, 128), 1)

    def one_tile(tile, carry):
        for half in range(2):
            rows = [jnp.zeros((16, 128), f32) for _ in range(3)]
            for v in range(4):
                at = 8 * tile + 4 * half + v
                value = gat_ref[at // 8, at - at // 8 * 8]
                for a in range(3):
                    shift = (PER_OWNER * (v - a)) % 128
                    moved = pltpu.roll(value, shift, 1) if shift else value
                    rows[a] = jnp.where(lane // PER_OWNER == v, moved, rows[a])
            top, low = halves(jnp.concatenate(rows, axis=0))
            packed[tile, 0:48, 128 * half : 128 * half + 128] = top
            packed[tile, 48:96, 128 * half : 128 * half + 128] = low
        return carry

    lax.fori_loop(0, 8, one_tile, 0)

    block = pl.multiple_of(me // 4 * 128, 128)
    entries = far_ref[:, pl.ds(block, 128)]
    mine = lax.rem(me, 4)
    lane48 = iota((FAR, 128), 1) // PER_OWNER
    picked = jnp.zeros((FAR, 128), i32)
    for place in range(4):
        moved = entries
        for k in range(1, 4):
            turned = pltpu.roll(entries, PER_OWNER * k, 1)
            moved = jnp.where(lax.rem(mine + k, 4) == place, turned, moved)
        far4[place] = moved
    for place in range(4):
        rows = far4[place, pl.ds(place, FAR // 4, stride=4), :]
        chosen = iota((FAR // 4, 128), 1) // PER_OWNER == place
        if place == 0:
            merged = rows
        else:
            merged = jnp.where(chosen, rows, merged)
    owner = merged >> 5
    spot = (((owner & 1) << 5) + (owner >> 1)) * PER_OWNER + (merged & 31)
    sources[0:12, :] = jnp.where(merged >= 0, spot, -1)
    target = me * PER_OWNER + (iota((12, 128), 1) & 31)
    mids[0, 0:12, :] = (2 * ((target >> 4) - (merged >> 4))).astype(f32)
    mids[1, 0:12, :] = (2 * (((target >> 2) & 3) - ((merged >> 2) & 3))).astype(f32)
    mids[2, 0:12, :] = (2 * ((target & 3) - (merged & 3))).astype(f32)

    def one_gather(index, carry):
        first = sources[pl.ds(2 * index, 1), :]
        second = sources[pl.ds(2 * index + 1, 1), :]
        wanted = jnp.concatenate([first, second], axis=1)
        found = jnp.zeros((96, 256), f32)
        for tile in range(8):
            onehot = (iota((256, 256), 0) + 256 * tile == wanted).astype(f32).astype(bf16)
            found = found + dot(packed[tile], onehot)
        value = found[0:48] + found[48:96]
        pushes[2 * index] = value[:, 0:128]
        pushes[2 * index + 1] = value[:, 128:256]
        return carry

    lax.fori_loop(0, 6, one_gather, 0)
    total[...] = jnp.zeros_like(total)

    def one_block(index, carry):
        mid = [mids[a, pl.ds(index, 1), :] for a in range(3)]
        for g in range(EQUIV // 8):
            at = slice(8 * g, 8 * g + 8)
            check = [mid[a] + inner_radius * surf_ref[at, a : a + 1] for a in range(3)]
            sums = [total[EQUIV * a + 8 * g : EQUIV * a + 8 * g + 8, :] for a in range(3)]
            for j in range(14):
                f = [pushes[index, 16 * a + j : 16 * a + j + 1, :] for a in range(3)]
                r = [check[a] - points[3 * (14 * portion + j) + a] for a in range(3)]
                even, along = pull(r, f)
                sums = [sums[a] + (even * f[a] + along * r[a]) for a in range(3)]
            for a in range(3):
                total[EQUIV * a + 8 * g : EQUIV * a + 8 * g + 8, :] = sums[a]
        return carry

    lax.fori_loop(0, 12, one_block, 0)
    value = total[...] * inv_eight_pi
    value = value + pltpu.roll(value, 64, 1)
    value = value + pltpu.roll(value, 32, 1)
    local_ref[...] = dot_wide(inverse_ref[...], value)


def far_field(points, gathered, far_list, surf, down_inverse):
    return pl.pallas_call(
        far_kernel,
        out_shape=jax.ShapeDtypeStruct((ROWS, 128), f32),
        in_specs=[SMEM, VMEM, VMEM, VMEM, VMEM],
        out_specs=VMEM,
        scratch_shapes=[
            pltpu.VMEM((4, FAR, 128), i32),
            pltpu.VMEM((16, 128), i32),
            pltpu.VMEM((8, 96, 256), bf16),
            pltpu.VMEM((12, FAR, 128), f32),
            pltpu.VMEM((3, 16, 128), f32),
            pltpu.VMEM((ROWS, 128), f32),
        ],
        name="far_field",
    )(points, gathered, far_list, surf, down_inverse)


def near_kernel(lists, comp_ref, near_ref, out_ref, relation, reach, spots, match, sums, weight):
    me = lax.axis_index("cells")
    portion = lax.axis_index("leaf")
    start = lax.rem(me + 63, 64)
    block = start // 4
    left = near_ref[:, pl.ds(pl.multiple_of(block * 128, 128), 128)]
    right = near_ref[:, pl.ds(pl.multiple_of(lax.rem(block + 1, 16) * 128, 128), 128)]
    both = jnp.concatenate([left, right], axis=1)
    listed = both[:, 0:128]
    for k in range(1, 4):
        listed = jnp.where(lax.rem(start, 4) == k, both[:, 32 * k : 32 * k + 128], listed)
    listed = jnp.where(listed >= 0, (listed - PER_OWNER * (me - 2)) & 2047, -1)
    source_leaf = iota((160, 128), 0)
    near = jnp.zeros((160, 128), f32)
    for k in range(48):
        near = near + jnp.where(listed[k : k + 1, :] == source_leaf, 1.0, 0.0)
    relation[...] = near.astype(bf16)
    row8, lane8 = iota((8, 128), 0), iota((8, 128), 1)
    leaf_rows = [
        jnp.where((lane8 == lists[7, 8 + t] - 3 * PER_OWNER + row8) & (row8 < 3), 1.0, 0.0)
        for t in range(CPD)
    ]
    wanted = dot_nt(jnp.concatenate(leaf_rows, axis=0).astype(bf16), relation[...]).astype(bf16)

    def one_source(c, carry):
        rel = comp_ref[REL, pl.ds(c, 1), :].astype(i32) - 2 * PER_OWNER
        onehot = (iota((160, WIDE), 0) == rel).astype(f32).astype(bf16)
        reach[c] = dot(wanted, onehot)
        return carry

    lax.fori_loop(0, CELLS, one_source, 0)

    pick_row, pick_lane = iota((SHARE_PAD, WIDE), 0), iota((SHARE_PAD, WIDE), 1)
    pick = (pick_lane == pick_row + SHARE * portion) & (pick_row < SHARE)
    pick16 = pick.astype(f32).astype(bf16)
    for t in range(CPD):
        rows = jnp.concatenate([comp_ref[k, t : t + 1, :] for k in (PX, PY, PZ, REL)], axis=0)
        top = rows.astype(bf16)
        rest = rows - top.astype(f32)
        middle = rest.astype(bf16)
        low = (rest - middle.astype(f32)).astype(bf16)
        columns = dot_nt(pick16, top) + (dot_nt(pick16, middle) + dot_nt(pick16, low))
        for a in range(3):
            spots[t, a] = jnp.broadcast_to(columns[:, a : a + 1], (SHARE_PAD, 128))
        leaf_at = columns[:, 3:4] - lists[7, 8 + t].astype(f32)
        match[t] = (leaf_at == iota((SHARE_PAD, 8), 1).astype(f32)).astype(f32)

    def one_target(t, carry):
        sums[...] = jnp.zeros_like(sums)

        def one_pair(index, carry):
            c = lists[t, index]
            weight[...] = dot(match[t], reach[c, pl.ds(pl.multiple_of(8 * t, 8), 8), :])
            p = [comp_ref[PX + a, pl.ds(c, 1), :] for a in range(3)]
            f = [comp_ref[FX + a, pl.ds(c, 1), :] for a in range(3)]
            for g in range(SHARE_PAD // 8):
                at = slice(8 * g, 8 * g + 8)
                for b in range(WIDE // 128):
                    lanes = slice(128 * b, 128 * b + 128)
                    pb = [value[:, lanes] for value in p]
                    fb = [value[:, lanes] for value in f]
                    r = [spots[t, a, at, :] - pb[a] for a in range(3)]
                    shifted = (r[0] * r[0] + r[1] * r[1]) + (r[2] * r[2] + smooth_sq)
                    inner = (r[0] * fb[0] + r[1] * fb[1]) + r[2] * fb[2]
                    root = lax.rsqrt(shifted)
                    held = root * weight[at, lanes]
                    cube = root * root * held
                    even = held + smooth_sq * cube
                    along = cube * inner
                    part = [even * fb[a] + along * r[a] for a in range(3)]
                    if b == 0:
                        added = part
                    else:
                        added = [added[a] + part[a] for a in range(3)]
                for a in range(3):
                    sums[a, at, :] += added[a]
            return carry

        lax.fori_loop(0, lists[t, COUNT], one_pair, 0)
        for a in range(3):
            column = jnp.sum(sums[a], axis=1, keepdims=True) * inv_eight_pi
            row = jnp.sum(jnp.where(pick, column, 0.0), axis=0, keepdims=True)
            out_ref[a, pl.ds(t, 1), :] = row
        return carry

    lax.fori_loop(0, CPD, one_target, 0)


def near_field(lists, comp, near_list):
    return pl.pallas_call(
        near_kernel,
        out_shape=jax.ShapeDtypeStruct((3, 8, WIDE), f32),
        in_specs=[SMEM, VMEM, VMEM],
        out_specs=VMEM,
        scratch_shapes=[
            pltpu.VMEM((160, 128), bf16),
            pltpu.VMEM((CELLS, 8 * CPD, WIDE), f32),
            pltpu.VMEM((CPD, 3, SHARE_PAD, 128), f32),
            pltpu.VMEM((CPD, SHARE_PAD, 8), f32),
            pltpu.VMEM((3, SHARE_PAD, 128), f32),
            pltpu.VMEM((SHARE_PAD, WIDE), f32),
        ],
        name="near_field",
    )(lists, comp, near_list)


def evaluate_kernel(lists, comp_ref, near_ref, own_ref, recv_ref, surf_ref, out_ref, local, pushes):
    for place in range(3):
        value = own_ref[:, 0:PER_OWNER] if place == 1 else recv_ref[place // 2, :, 0:PER_OWNER]
        top, low = halves(value)
        local[place, 0:ROWS, :] = top
        local[place, ROWS : 2 * ROWS, :] = low
    for t in range(CPD):
        place = lists[7, t]
        rel = comp_ref[REL, t : t + 1, :].astype(i32)
        leaf = jnp.where(rel >= 0, rel & 31, -1)
        member = (iota((PER_OWNER, WIDE), 0) == leaf).astype(f32).astype(bf16)
        spread_out = dot(local[place], member)
        pushes[...] = spread_out[0:ROWS] + spread_out[ROWS : 2 * ROWS]
        d = [comp_ref[DX + a, t : t + 1, :] for a in range(3)]
        sums = [jnp.zeros((8, WIDE), f32) for _ in range(3)]
        for g in range(EQUIV // 8):
            at = slice(8 * g, 8 * g + 8)
            r = [d[a] - outer_radius * surf_ref[at, a : a + 1] for a in range(3)]
            f = [pushes[EQUIV * a + 8 * g : EQUIV * a + 8 * g + 8, :] for a in range(3)]
            even, along = pull(r, f)
            sums = [sums[a] + (even * f[a] + along * r[a]) for a in range(3)]
        for a in range(3):
            row = jnp.sum(sums[a], axis=0, keepdims=True) * inv_eight_pi + near_ref[a, t : t + 1, :]
            out_ref[a : a + 1, NPT * t : NPT * (t + 1)] = row[:, 0:NPT]


def evaluate(lists, comp, near, local, received, surf, npoints):
    return pl.pallas_call(
        evaluate_kernel,
        out_shape=jax.ShapeDtypeStruct((3, npoints), f32),
        in_specs=[SMEM] + [VMEM] * 5,
        out_specs=VMEM,
        scratch_shapes=[
            pltpu.VMEM((3, 2 * ROWS, PER_OWNER), bf16),
            pltpu.VMEM((ROWS, WIDE), f32),
        ],
        name="evaluate",
    )(lists, comp, near, local, received, surf)


def body(displacement, point_leaf, near_list, far_list, stiffness, up_inverse, down_inverse):
    table = surface_table()
    surf = jnp.asarray(np.pad(table, ((0, 0), (0, 5))))
    points = jnp.asarray((inner_radius * table).astype(np.float32).reshape(-1))
    own = jnp.concatenate([displacement, point_leaf.astype(f32)[None, :]], axis=0)
    recv = spread(own, "cells", OFFSETS, 0)
    comp, lists = prepare(own, recv, stiffness)
    block = upward(lists, comp, surf, up_inverse)
    gathered = gather_blocks(block, 1)
    near = near_field(lists, comp, near_list)
    local = far_field(points, gathered, far_list, surf, down_inverse)
    received = spread(local, "cells", (1, -1), 2)
    part = evaluate(lists, comp, near, local, received, surf, displacement.shape[1])
    return leaf_sum(part, 3)


def solution(mesh):
    in_specs = (P(None, "cells"), P("cells"), P(), P(), P(), P(), P())
    out_specs = P(None, "cells")
    return jax.shard_map(body, mesh=mesh, in_specs=in_specs, out_specs=out_specs, check_vma=False)
```

```python
import math

import jax
import jax.numpy as jnp
import numpy as np
from jax import lax
from jax.experimental import pallas as pl
from jax.experimental.pallas import tpu as pltpu
from jax.sharding import PartitionSpec as P

NPT = 312
CPD = 6
SLICE = 16
EQUIV = 56
FAR = 48
ROWS = 3 * EQUIV
PER_OWNER = 2 * SLICE
WIDE = 384
OFFSETS = (1, -1, 2, -2, 3, -3)
CELLS = CPD * (len(OFFSETS) + 1)
OWNABLE = 3 * CPD
SHARE = NPT // 4
SHARE_PAD = 80
COUNT = 127

inv_eight_pi = 1.0 / (8.0 * math.pi)
smooth_sq = 0.0625
inner_radius = 1.05
outer_radius = 2.95
MESH = pl.DeviceIdType.MESH
VMEM = pl.BlockSpec(memory_space=pltpu.VMEM)
SMEM = pl.BlockSpec(memory_space=pltpu.SMEM)
f32 = jnp.float32
bf16 = jnp.bfloat16
i32 = jnp.int32


def surface_table():
    ladder = [-1.0, -1.0 / 3.0, 1.0 / 3.0, 1.0]
    corners = [
        (a, b, c)
        for a in ladder
        for b in ladder
        for c in ladder
        if max(abs(a), abs(b), abs(c)) == 1.0
    ]
    return np.array(corners, dtype=np.float32)


def iota(shape, dim):
    return lax.broadcasted_iota(i32, shape, dim)


def dot(a, b):
    return jnp.dot(a, b, preferred_element_type=f32)


def dot_nt(a, b):
    return lax.dot_general(a, b, (((1,), (1,)), ((), ())), preferred_element_type=f32)


def halves(value):
    top = value.astype(bf16)
    return top, (value - top.astype(f32)).astype(bf16)


def dot_wide(a, b):
    a_top, a_low = halves(a)
    b_top, b_low = halves(b)
    return dot(a_top, b_top) + (dot(a_top, b_low) + dot(a_low, b_top))


DX, DY, DZ, FX, FY, FZ, PX, PY, PZ, REL = range(10)
FEATURES = 24
DEPTH = FEATURES + 8 * CPD
FAR_AWAY = 1e30
DUMMY = CELLS
BATCH = 3


def thirds(value):
    top = value.astype(bf16).astype(f32)
    rest = value - top
    middle = rest.astype(bf16).astype(f32)
    return top, middle, rest - middle


def pull(offset, strength):
    dx, dy, dz = offset
    fx, fy, fz = strength
    shifted = (dx * dx + dy * dy) + (dz * dz + smooth_sq)
    inner = (dx * fx + dy * fy) + dz * fz
    root = lax.rsqrt(shifted)
    cube = root * root * root
    return root + smooth_sq * cube, cube * inner


def remote(src, dst, send_sem, recv_sem, target):
    return pltpu.make_async_remote_copy(
        src_ref=src,
        dst_ref=dst,
        send_sem=send_sem,
        recv_sem=recv_sem,
        device_id=target,
        device_id_type=MESH,
    )


def greet(targets):
    barrier = pltpu.get_barrier_semaphore()
    for target in targets:
        pl.semaphore_signal(barrier, inc=1, device_id=target, device_id_type=MESH)
    pl.semaphore_wait(barrier, len(targets))


def beside(axis, offsets):
    count = lax.axis_size(axis)
    me = lax.axis_index(axis)
    return [{axis: lax.rem(me + (off + count), count)} for off in offsets]


def first_kernel(
    disp_ref,
    leaf_ref,
    near_ref,
    stiff_ref,
    surf_ref,
    inverse_ref,
    comp_ref,
    lists_ref,
    gat_ref,
    wanted_ref,
    lefts_ref,
    spots_ref,
    held_disp,
    held_leaf,
    disp,
    leaves,
    force,
    listed_ref,
    relation,
    wide,
    terms_top,
    terms_low,
    member_ref,
    total,
    density,
    block_ref,
    send_disp,
    recv_disp,
    send_leaf,
    recv_leaf,
    own_sem,
    z_send,
    z_recv,
    y_send,
    y_recv,
    c_send,
    c_recv,
):
    me = lax.axis_index("cells")
    portion = lax.axis_index("leaf")
    core = lax.rem(me, 2)
    z = lax.rem(me // 2, 8)
    y = me // 16

    def device(y_at, z_at, core_at):
        return {"cells": (y_at * 8 + z_at) * 2 + core_at}

    sides = beside("cells", OFFSETS)
    z_targets = [device(y, lax.rem(z + k, 8), core) for k in range(1, 8)]
    y_targets = [device(lax.rem(y + k, 4), z, core) for k in range(1, 4)]
    c_target = device(y, z, 1 - core)
    greet([*sides, *z_targets, *y_targets, c_target])
    copies = []
    for slot, target in enumerate(sides):
        copies.append(
            remote(disp_ref, held_disp.at[slot], send_disp.at[slot], recv_disp.at[slot], target)
        )
        copies.append(
            remote(leaf_ref, held_leaf.at[slot], send_leaf.at[slot], recv_leaf.at[slot], target)
        )
    for copy in copies:
        copy.start()

    comp_ref[...] = jnp.zeros_like(comp_ref)
    disp[...] = jnp.zeros_like(disp)
    leaves[...] = jnp.zeros_like(leaves)

    def place_cells(home, points, leaf_row):
        for k in range(CPD):
            at = slice(NPT * k, NPT * (k + 1))
            row = home * CPD + k
            for a in range(3):
                disp[48 * a + row : 48 * a + row + 1, 0:NPT] = points[a : a + 1, at]
            leaves[row : row + 1, 0:NPT] = leaf_row[:, at]

    def fill_table(rows):
        live = iota((rows, WIDE), 1) < NPT
        rel = jnp.where(live, (leaves[0:rows, :] - PER_OWNER * (me - 4)) & 2047, -1)
        for a in range(3):
            comp_ref[DX + a, 0:rows, :] = disp[48 * a : 48 * a + rows, :]
        comp_ref[REL, 0:rows, :] = rel.astype(f32)
        comp_ref[PX, 0:rows, :] = comp_ref[DX, 0:rows, :] + (2 * (rel >> 4) + 1).astype(f32)
        comp_ref[PY, 0:rows, :] = comp_ref[DY, 0:rows, :] + (2 * ((rel >> 2) & 3) + 1).astype(f32)
        comp_ref[PZ, 0:rows, :] = comp_ref[DZ, 0:rows, :] + (2 * (rel & 3) + 1).astype(f32)
        relf = rel.astype(f32)
        first = jnp.min(jnp.where(live, relf, 1e9), axis=1, keepdims=True)
        last = jnp.max(relf, axis=1, keepdims=True)
        return first, last

    place_cells(0, disp_ref[...], leaf_ref[...])
    first, last = fill_table(8)

    start = lax.rem(me + 63, 64)
    block = start // 4
    left = near_ref[:, pl.ds(pl.multiple_of(block * 128, 128), 128)]
    right = near_ref[:, pl.ds(pl.multiple_of(lax.rem(block + 1, 16) * 128, 128), 128)]
    both = jnp.concatenate([left, right], axis=1)
    listed = both[:, 0:128]
    for k in range(1, 4):
        listed = jnp.where(lax.rem(start, 4) == k, both[:, 32 * k : 32 * k + 128], listed)
    listed_ref[...] = jnp.where(listed >= 0, (listed - PER_OWNER * (me - 2)) & 2047, -1)
    source_leaf = iota((160, 128), 0)

    def eight_entries(index, near):
        rows = listed_ref[pl.ds(pl.multiple_of(8 * index, 8), 8), :]
        for k in range(8):
            near = near + jnp.where(rows[k : k + 1, :] == source_leaf, 1.0, 0.0)
        return near

    near = lax.fori_loop(0, 6, eight_entries, jnp.zeros((160, 128), f32))
    relation[...] = near.astype(bf16)
    row8, lane8 = iota((8, 128), 0).astype(f32), iota((8, 128), 1).astype(f32)
    leaf_rows = [
        jnp.where((lane8 == first[t : t + 1] - 3.0 * PER_OWNER + row8) & (row8 < 3.0), 1.0, 0.0)
        for t in range(CPD)
    ]
    wanted_ref[...] = dot_nt(jnp.concatenate(leaf_rows, axis=0).astype(bf16), relation[...])

    pick_row, pick_lane = iota((SHARE_PAD, WIDE), 0), iota((SHARE_PAD, WIDE), 1)
    pick16 = ((pick_lane == pick_row + SHARE * portion) & (pick_row < SHARE)).astype(f32).astype(bf16)
    slot = iota((SHARE_PAD, 128), 1)
    slot_turn = lax.rem(slot, 6)
    left_first = (slot < 18) & (slot_turn < 3) | (slot == 18)
    left_second = (slot < 18) & (slot_turn >= 3) & (slot_turn < 5) | (slot == 19)
    row32 = iota((32, WIDE), 0)

    def one_own(t, carry):
        rel = comp_ref[REL, pl.ds(t, 1), :]
        px, py, pz = [comp_ref[PX + a, pl.ds(t, 1), :] for a in range(3)]
        lowest = jnp.min(jnp.where(rel >= 0.0, rel, 1e9), axis=1, keepdims=True)
        owner = jnp.floor(lowest * (1.0 / PER_OWNER))
        py4, pz4 = py - 4.0, pz - 4.0
        extra = iota((8, WIDE), 0)
        place = jnp.where(extra == 0, px, jnp.where(extra == 1, py, jnp.where(extra == 2, pz, rel)))
        top, middle, low = thirds(place)
        spot = dot_nt(pick16, top.astype(bf16)) + (
            dot_nt(pick16, middle.astype(bf16)) + dot_nt(pick16, low.astype(bf16))
        )
        for a in range(3):
            spots_ref[t, a] = jnp.broadcast_to(spot[:, a : a + 1], (SHARE_PAD, 128))
        leaf_at = (spot[:, 3:4] - lowest).astype(i32)
        matched = (slot - (FEATURES + 8 * t) == leaf_at) & (leaf_at >= 0) & (leaf_at < 3)
        for w in range(3):
            px4 = px - (4.0 * (owner + float(w - 1)) + 2.0)
            square = (px4 * px4 + py4 * py4) + pz4 * pz4
            rows = jnp.where(
                row32 < 6,
                px4,
                jnp.where(row32 < 12, py4, jnp.where(row32 < 18, pz4, square)),
            )
            rows = jnp.concatenate([rows, jnp.zeros((96, WIDE), f32)], axis=0)
            top, middle, low = thirds(rows)
            value = dot_nt(pick16, top.astype(bf16)) + (
                dot_nt(pick16, middle.astype(bf16)) + dot_nt(pick16, low.astype(bf16))
            )
            top, middle, low = thirds(value)
            chosen = jnp.where(left_first, top, jnp.where(left_second, middle, low))
            chosen = jnp.where((slot >= 21) & (slot < 24), 1.0, chosen)
            chosen = jnp.where(slot >= FEATURES, jnp.where(matched, 1.0, 0.0), chosen)
            lefts_ref[3 * t + w] = chosen[:, 0:DEPTH].astype(bf16)
        return carry

    lax.fori_loop(0, CPD, one_own, 0)
    for a in range(3):
        wide[a] = jnp.broadcast_to(outer_radius * surf_ref[:, a : a + 1], (EQUIV, 128))

    for copy in copies:
        copy.wait()
    for home in range(1, len(OFFSETS) + 1):
        place_cells(home, held_disp[home - 1], held_leaf[home - 1])
    first, last = fill_table(48)
    force[...] = dot_wide(disp[0:144, 0:NPT], stiff_ref[...])
    for a in range(3):
        comp_ref[FX + a, 0:48, 0:NPT] = force[48 * a : 48 * a + 48, :]

    total[...] = jnp.zeros_like(total)

    def one_home(home, carry):
        for k in range(CPD):
            c = CPD * home + k
            d = [comp_ref[DX + a, pl.ds(c, 1), :] for a in range(3)]
            f = [comp_ref[FX + a, pl.ds(c, 1), :] for a in range(3)]
            rel = comp_ref[REL, pl.ds(c, 1), :].astype(i32) - 4 * PER_OWNER
            member = (iota((PER_OWNER, WIDE), 0) == rel).astype(f32).astype(bf16)
            member_ref[:, WIDE * k : WIDE * (k + 1)] = member
            for b in range(WIDE // 128):
                lanes = slice(128 * b, 128 * b + 128)
                out = slice(WIDE * k + 128 * b, WIDE * k + 128 * b + 128)
                for g in range(EQUIV // 8):
                    at = slice(8 * g, 8 * g + 8)
                    r = [wide[a, at, :] - d[a][:, lanes] for a in range(3)]
                    fb = [f[a][:, lanes] for a in range(3)]
                    even, along = pull(r, fb)
                    for a in range(3):
                        row = EQUIV * a + 8 * g
                        top, low = halves(even * fb[a] + along * r[a])
                        terms_top[row : row + 8, out] = top
                        terms_low[row : row + 8, out] = low
        total[...] += dot_nt(terms_top[...], member_ref[...]) + dot_nt(terms_low[...], member_ref[...])
        return carry

    lax.fori_loop(0, 3, one_home, 0)
    density[...] = dot_wide(inverse_ref[...], total[...] * inv_eight_pi)
    block_ref[...] = jnp.zeros_like(block_ref)
    for part in range(4):

        @pl.when(portion == part)
        def _():
            for a in range(3):
                rows = density[EQUIV * a + 14 * part : EQUIV * a + 14 * part + 14, :]
                block_ref[0:14, PER_OWNER * a : PER_OWNER * (a + 1)] = rows

    row = core * 4 + y
    own = pltpu.make_async_copy(block_ref, gat_ref.at[row, z], own_sem)
    own.start()
    z_copies = [
        remote(block_ref, gat_ref.at[row, z], z_send.at[k], z_recv.at[k], target)
        for k, target in enumerate(z_targets)
    ]
    for copy in z_copies:
        copy.start()

    low = jnp.floor(first * (1.0 / 16.0))
    high = jnp.floor(last * (1.0 / 16.0))
    lane = iota((48, 128), 1)
    which = iota((48, 1), 0).astype(f32)
    real = which < float(CELLS)
    flags = []
    for t in range(CPD):
        low_t, high_t = low[t : t + 1], high[t : t + 1]
        flags.append(jnp.where((high >= low_t - 1.0) & (low <= high_t + 1.0) & real, 1.0, 0.0))
    owner = jnp.floor(low * 0.5)
    union = flags[0]
    for t in range(1, CPD):
        union = jnp.maximum(union, flags[t])
    flags.append(union)
    table = jnp.zeros((48, 128), f32)
    for t, flag in enumerate(flags):
        table = table + jnp.where(lane == t, flag, 0.0)
    before = (iota((48, 48), 0) > iota((48, 48), 1)).astype(f32)
    rank = dot(before, table)
    count = jnp.sum(table, axis=0, keepdims=True)
    lane_row = iota((1, 128), 1)
    lists_ref[...] = jnp.zeros_like(lists_ref)
    for t, flag in enumerate(flags):
        hit = (rank[:, t : t + 1] == lane.astype(f32)) & (flag > 0.0)
        line = jnp.sum(jnp.where(hit, which, 0.0), axis=0, keepdims=True)
        line = jnp.where(lane_row.astype(f32) >= count[:, t : t + 1], float(DUMMY), line)
        line = jnp.where(lane_row == COUNT, count[:, t : t + 1], line)
        lists_ref[t : t + 1, :] = line.astype(i32)
    square = iota((48, 128), 0) == lane
    line = jnp.sum(jnp.where(square, owner, 0.0), axis=0, keepdims=True)
    lists_ref[7:8, :] = line.astype(i32)

    own.wait()
    for copy in z_copies:
        copy.wait()
    y_copies = [
        remote(gat_ref.at[row], gat_ref.at[row], y_send.at[k], y_recv.at[k], target)
        for k, target in enumerate(y_targets)
    ]
    for copy in y_copies:
        copy.start()
    c_copies = []
    for k in range(4):
        at = core * 4 + lax.rem(y - k + 4, 4)
        if k:
            y_copies[k - 1].wait_recv()
        copy = remote(gat_ref.at[at], gat_ref.at[at], c_send.at[k], c_recv.at[k], c_target)
        copy.start()
        c_copies.append(copy)
    for copy in y_copies:
        copy.wait_send()
    for copy in c_copies:
        copy.wait()


def first(displacement, leaf_row, near_list, stiffness, surf, up_inverse):
    npoints = displacement.shape[1]
    sides = len(OFFSETS)
    dma = pltpu.SemaphoreType.DMA
    return pl.pallas_call(
        first_kernel,
        out_shape=(
            jax.ShapeDtypeStruct((10, 48, WIDE), f32),
            jax.ShapeDtypeStruct((8, 128), i32),
            jax.ShapeDtypeStruct((8, 8, 16, 128), f32),
            jax.ShapeDtypeStruct((8 * CPD, 160), f32),
            jax.ShapeDtypeStruct((3 * CPD, SHARE_PAD, DEPTH), bf16),
            jax.ShapeDtypeStruct((CPD, 3, SHARE_PAD, 128), f32),
        ),
        in_specs=[VMEM] * 6,
        out_specs=(VMEM,) * 6,
        scratch_shapes=[
            pltpu.VMEM((sides, 3, npoints), f32),
            pltpu.VMEM((sides, 1, npoints), i32),
            pltpu.VMEM((144, WIDE), f32),
            pltpu.VMEM((48, WIDE), i32),
            pltpu.VMEM((144, NPT), f32),
            pltpu.VMEM((FAR, 128), i32),
            pltpu.VMEM((160, 128), bf16),
            pltpu.VMEM((3, EQUIV, 128), f32),
            pltpu.VMEM((ROWS, CPD * WIDE), bf16),
            pltpu.VMEM((ROWS, CPD * WIDE), bf16),
            pltpu.VMEM((PER_OWNER, CPD * WIDE), bf16),
            pltpu.VMEM((ROWS, PER_OWNER), f32),
            pltpu.VMEM((ROWS, PER_OWNER), f32),
            pltpu.VMEM((16, 128), f32),
            dma((sides,)),
            dma((sides,)),
            dma((sides,)),
            dma((sides,)),
            dma,
            dma((7,)),
            dma((7,)),
            dma((3,)),
            dma((3,)),
            dma((4,)),
            dma((4,)),
        ],
        compiler_params=pltpu.CompilerParams(collective_id=0, has_side_effects=True),
        name="first",
    )(displacement, leaf_row, near_list, stiffness, surf, up_inverse)


def near_kernel(
    lists, comp_ref, wanted_ref, lefts, spots, out_ref, rights, even_pairs, odd_pairs, sums
):
    portion = lax.axis_index("leaf")
    wanted = wanted_ref[...].astype(bf16)
    feature = iota((FEATURES, WIDE), 0)
    turn = lax.rem(feature, 6)
    first = (feature < 18) & ((turn == 0) | (turn == 3) | (turn == 5)) | (feature == 21)
    second = (feature < 18) & ((turn == 1) | (turn == 4)) | (feature == 22)

    def factors(x, y, z, last):
        value = jnp.where(
            feature < 6, x, jnp.where(feature < 12, y, jnp.where(feature < 18, z, last))
        )
        top, middle, low = thirds(value)
        return jnp.where(first, top, jnp.where(second, middle, low))

    def some_sources(index, carry):
        cells = [lists[6, BATCH * index + k] for k in range(BATCH)]
        rels = [comp_ref[REL, pl.ds(c, 1), :].astype(i32) for c in cells]
        hits = [
            (iota((160, WIDE), 0) == rel - 2 * PER_OWNER).astype(f32).astype(bf16) for rel in rels
        ]
        reaches = [dot(wanted, hit) for hit in hits]
        for k, c in enumerate(cells):
            rel = rels[k]
            px = comp_ref[PX, pl.ds(c, 1), :] - (4 * (rel >> 5) + 2).astype(f32)
            py = comp_ref[PY, pl.ds(c, 1), :] - 4.0
            pz = comp_ref[PZ, pl.ds(c, 1), :] - 4.0
            fx, fy, fz = [comp_ref[FX + a, pl.ds(c, 1), :] for a in range(3)]
            square = (px * px + py * py) + (pz * pz + smooth_sq)
            along = (px * fx + py * fy) + pz * fz
            near_rows = factors(-2.0 * px, -2.0 * py, -2.0 * pz, square)
            near_rows = jnp.where((feature >= 18) & (feature < 21), 1.0, near_rows)
            push_rows = factors(fx, fy, fz, -along)
            push_rows = jnp.where((feature >= 18) & (feature < 21), 0.0, push_rows)
            mask_rows = FAR_AWAY - FAR_AWAY * reaches[k]
            rights[c, :, 0:WIDE] = jnp.concatenate([near_rows, mask_rows], axis=0).astype(bf16)
            rights[c, 0:FEATURES, WIDE : 2 * WIDE] = push_rows.astype(bf16)
            rights[c, FEATURES:DEPTH, WIDE : 2 * WIDE] = jnp.zeros((8 * CPD, WIDE), bf16)
        return carry

    lax.fori_loop(0, (lists[6, COUNT] + (BATCH - 1)) // BATCH, some_sources, 0)
    rights[DUMMY] = jnp.where(iota((DEPTH, 2 * WIDE), 0) == 21, FAR_AWAY, 0.0).astype(bf16)

    def multiply(t, index, products):
        c = lists[t, index]
        w = jnp.clip(lists[7, c] - lists[7, t] + 1, 0, 2)
        products[...] = dot(lefts[3 * t + w], rights[c])

    def add_pair(t, index, products):
        c = lists[t, index]
        p = [comp_ref[PX + a, pl.ds(c, 1), :] for a in range(3)]
        f = [comp_ref[FX + a, pl.ds(c, 1), :] for a in range(3)]
        for g in range(SHARE_PAD // 8):
            at = slice(8 * g, 8 * g + 8)
            added = None
            for b in range(WIDE // 128):
                lanes = slice(128 * b, 128 * b + 128)
                shifted = products[at, lanes]
                inner = products[at, WIDE + 128 * b : WIDE + 128 * b + 128]
                root = lax.rsqrt(shifted)
                cube = root * root * root
                even = root + smooth_sq * cube
                along = cube * inner
                part = [even * f[a][:, lanes] - along * p[a][:, lanes] for a in range(3)]
                part.append(along)
                if added is None:
                    added = part
                else:
                    added = [u + v for u, v in zip(added, part)]
            for a in range(4):
                sums[a, at, :] += added[a]

    pick_row, pick_lane = iota((SHARE_PAD, WIDE), 0), iota((SHARE_PAD, WIDE), 1)
    pick = (pick_lane == pick_row + SHARE * portion) & (pick_row < SHARE)

    def one_target(t, carry):
        sums[...] = jnp.zeros_like(sums)
        multiply(t, 0, even_pairs)

        def two_pairs(index, carry):
            multiply(t, 2 * index + 1, odd_pairs)
            add_pair(t, 2 * index, even_pairs)
            multiply(t, 2 * index + 2, even_pairs)
            add_pair(t, 2 * index + 1, odd_pairs)
            return carry

        lax.fori_loop(0, (lists[t, COUNT] + 1) // 2, two_pairs, 0)
        for a in range(3):
            total = sums[a] + spots[t, a] * sums[3]
            column = jnp.sum(total, axis=1, keepdims=True) * inv_eight_pi
            row = jnp.sum(jnp.where(pick, column, 0.0), axis=0, keepdims=True)
            out_ref[a, pl.ds(t, 1), :] = row
        return carry

    lax.fori_loop(0, CPD, one_target, 0)


def near_field(lists, comp, wanted, lefts, spots):
    return pl.pallas_call(
        near_kernel,
        out_shape=jax.ShapeDtypeStruct((3, 8, WIDE), f32),
        in_specs=[SMEM] + [VMEM] * 4,
        out_specs=VMEM,
        scratch_shapes=[
            pltpu.VMEM((CELLS + 1, DEPTH, 2 * WIDE), bf16),
            pltpu.VMEM((SHARE_PAD, 2 * WIDE), f32),
            pltpu.VMEM((SHARE_PAD, 2 * WIDE), f32),
            pltpu.VMEM((4, SHARE_PAD, 128), f32),
        ],
        name="near_field",
    )(lists, comp, wanted, lefts, spots)


def far_part(
    points, gat_ref, far_ref, surf_ref, inverse_ref, local_ref, far4, sources, packed, pushes, mids, total
):
    me = lax.axis_index("cells")
    portion = lax.axis_index("leaf")
    lane = iota((16, 128), 1)

    def one_tile(tile, carry):
        for half in range(2):
            rows = [jnp.zeros((16, 128), f32) for _ in range(3)]
            for v in range(4):
                at = 8 * tile + 4 * half + v
                value = gat_ref[at // 8, at - at // 8 * 8]
                for a in range(3):
                    shift = (PER_OWNER * (v - a)) % 128
                    moved = pltpu.roll(value, shift, 1) if shift else value
                    rows[a] = jnp.where(lane // PER_OWNER == v, moved, rows[a])
            top, low = halves(jnp.concatenate(rows, axis=0))
            packed[tile, 0:48, 128 * half : 128 * half + 128] = top
            packed[tile, 48:96, 128 * half : 128 * half + 128] = low
        return carry

    lax.fori_loop(0, 8, one_tile, 0)

    block = pl.multiple_of(me // 4 * 128, 128)
    entries = far_ref[:, pl.ds(block, 128)]
    mine = lax.rem(me, 4)
    lane48 = iota((FAR, 128), 1) // PER_OWNER
    picked = jnp.zeros((FAR, 128), i32)
    for place in range(4):
        moved = entries
        for k in range(1, 4):
            turned = pltpu.roll(entries, PER_OWNER * k, 1)
            moved = jnp.where(lax.rem(mine + k, 4) == place, turned, moved)
        far4[place] = moved
    for place in range(4):
        rows = far4[place, pl.ds(place, FAR // 4, stride=4), :]
        chosen = iota((FAR // 4, 128), 1) // PER_OWNER == place
        if place == 0:
            merged = rows
        else:
            merged = jnp.where(chosen, rows, merged)
    owner = merged >> 5
    spot = (((owner & 1) << 5) + (owner >> 1)) * PER_OWNER + (merged & 31)
    sources[0:12, :] = jnp.where(merged >= 0, spot, -1)
    target = me * PER_OWNER + (iota((12, 128), 1) & 31)
    mids[0, 0:12, :] = (2 * ((target >> 4) - (merged >> 4))).astype(f32)
    mids[1, 0:12, :] = (2 * (((target >> 2) & 3) - ((merged >> 2) & 3))).astype(f32)
    mids[2, 0:12, :] = (2 * ((target & 3) - (merged & 3))).astype(f32)

    def one_gather(index, carry):
        first = sources[pl.ds(2 * index, 1), :]
        second = sources[pl.ds(2 * index + 1, 1), :]
        wanted = jnp.concatenate([first, second], axis=1)
        found = jnp.zeros((96, 256), f32)
        for tile in range(8):
            onehot = (iota((256, 256), 0) + 256 * tile == wanted).astype(f32).astype(bf16)
            found = found + dot(packed[tile], onehot)
        value = found[0:48] + found[48:96]
        pushes[2 * index] = value[:, 0:128]
        pushes[2 * index + 1] = value[:, 128:256]
        return carry

    lax.fori_loop(0, 6, one_gather, 0)
    total[...] = jnp.zeros_like(total)

    def one_block(index, carry):
        mid = [mids[a, pl.ds(index, 1), :] for a in range(3)]
        for g in range(EQUIV // 8):
            at = slice(8 * g, 8 * g + 8)
            check = [mid[a] + inner_radius * surf_ref[at, a : a + 1] for a in range(3)]
            sums = [total[EQUIV * a + 8 * g : EQUIV * a + 8 * g + 8, :] for a in range(3)]
            for j in range(14):
                f = [pushes[index, 16 * a + j : 16 * a + j + 1, :] for a in range(3)]
                r = [check[a] - points[3 * (14 * portion + j) + a] for a in range(3)]
                even, along = pull(r, f)
                sums = [sums[a] + (even * f[a] + along * r[a]) for a in range(3)]
            for a in range(3):
                total[EQUIV * a + 8 * g : EQUIV * a + 8 * g + 8, :] = sums[a]
        return carry

    lax.fori_loop(0, 12, one_block, 0)
    value = total[...] * inv_eight_pi
    value = value + pltpu.roll(value, 64, 1)
    value = value + pltpu.roll(value, 32, 1)
    local_ref[...] = dot_wide(inverse_ref[...], value)


def last_kernel(
    points,
    gat_ref,
    far_ref,
    surf_ref,
    inverse_ref,
    comp_ref,
    near_ref,
    out_ref,
    far4,
    sources,
    packed,
    pushes,
    mids,
    total,
    local_ref,
    held_local,
    factors,
    spread_ref,
    part_ref,
    held_part,
    send_local,
    recv_local,
    send_part,
    recv_part,
):
    sides = beside("cells", (1, -1))
    mates = beside("leaf", (1, 2, 3))
    barrier = pltpu.get_barrier_semaphore()
    for target in (*sides, *mates):
        pl.semaphore_signal(barrier, inc=1, device_id=target, device_id_type=MESH)
    far_part(
        points, gat_ref, far_ref, surf_ref, inverse_ref, local_ref, far4, sources, packed, pushes, mids, total
    )
    pl.semaphore_wait(barrier, 5)
    copies = [
        remote(local_ref, held_local.at[k], send_local.at[k], recv_local.at[k], target)
        for k, target in enumerate(sides)
    ]
    for copy in copies:
        copy.start()
    for copy in copies:
        copy.wait()
    lane = iota((ROWS, 128), 1) // PER_OWNER
    value = jnp.where(
        lane == 0, held_local[0], jnp.where(lane == 1, local_ref[...], held_local[1])
    )
    top, low = halves(value)
    factors[0:ROWS, :] = top
    factors[ROWS : 2 * ROWS, :] = low

    def one_cell(t, carry):
        rel = comp_ref[REL, pl.ds(t, 1), :].astype(i32) - 3 * PER_OWNER
        member = (iota((128, WIDE), 0) == rel).astype(f32).astype(bf16)
        both = dot(factors[...], member)
        spread_ref[t] = both[0:ROWS] + both[ROWS : 2 * ROWS]
        return carry

    lax.fori_loop(0, CPD, one_cell, 0)
    for t in range(CPD):
        d = [comp_ref[DX + a, t : t + 1, :] for a in range(3)]
        sums = [jnp.zeros((8, WIDE), f32) for _ in range(3)]
        for g in range(EQUIV // 8):
            at = slice(8 * g, 8 * g + 8)
            r = [d[a] - outer_radius * surf_ref[at, a : a + 1] for a in range(3)]
            f = [spread_ref[t, EQUIV * a + 8 * g : EQUIV * a + 8 * g + 8, :] for a in range(3)]
            even, along = pull(r, f)
            sums = [sums[a] + (even * f[a] + along * r[a]) for a in range(3)]
        for a in range(3):
            row = jnp.sum(sums[a], axis=0, keepdims=True) * inv_eight_pi + near_ref[a, t : t + 1, :]
            part_ref[a : a + 1, NPT * t : NPT * (t + 1)] = row[:, 0:NPT]
    copies = [
        remote(part_ref, held_part.at[k], send_part.at[k], recv_part.at[k], target)
        for k, target in enumerate(mates)
    ]
    for copy in copies:
        copy.start()
    for copy in copies:
        copy.wait()
    out_ref[...] = (part_ref[...] + held_part[1]) + (held_part[0] + held_part[2])


def last(points, gathered, far_list, surf, down_inverse, comp, near, npoints):
    dma = pltpu.SemaphoreType.DMA
    return pl.pallas_call(
        last_kernel,
        out_shape=jax.ShapeDtypeStruct((3, npoints), f32),
        in_specs=[SMEM] + [VMEM] * 6,
        out_specs=VMEM,
        scratch_shapes=[
            pltpu.VMEM((4, FAR, 128), i32),
            pltpu.VMEM((16, 128), i32),
            pltpu.VMEM((8, 96, 256), bf16),
            pltpu.VMEM((12, FAR, 128), f32),
            pltpu.VMEM((3, 16, 128), f32),
            pltpu.VMEM((ROWS, 128), f32),
            pltpu.VMEM((ROWS, 128), f32),
            pltpu.VMEM((2, ROWS, 128), f32),
            pltpu.VMEM((2 * ROWS, 128), bf16),
            pltpu.VMEM((CPD, ROWS, WIDE), f32),
            pltpu.VMEM((3, npoints), f32),
            pltpu.VMEM((3, 3, npoints), f32),
            dma((2,)),
            dma((2,)),
            dma((3,)),
            dma((3,)),
        ],
        compiler_params=pltpu.CompilerParams(collective_id=1, has_side_effects=True),
        name="last",
    )(points, gathered, far_list, surf, down_inverse, comp, near)


def body(displacement, point_leaf, near_list, far_list, stiffness, up_inverse, down_inverse):
    table = surface_table()
    surf = jnp.asarray(np.pad(table, ((0, 0), (0, 5))))
    points = jnp.asarray((inner_radius * table).astype(np.float32).reshape(-1))
    comp, lists, gathered, wanted, lefts, spots = first(
        displacement, point_leaf[None, :], near_list, stiffness, surf, up_inverse
    )
    near = near_field(lists, comp, wanted, lefts, spots)
    return last(
        points, gathered, far_list, surf, down_inverse, comp, near, displacement.shape[1]
    )


def solution(mesh):
    in_specs = (P(None, "cells"), P("cells"), P(), P(), P(), P(), P())
    out_specs = P(None, "cells")
    return jax.shard_map(body, mesh=mesh, in_specs=in_specs, out_specs=out_specs, check_vma=False)
```

```python
import math

import jax
import jax.numpy as jnp
import numpy as np
from jax import lax
from jax.experimental import pallas as pl
from jax.experimental.pallas import tpu as pltpu
from jax.sharding import PartitionSpec as P

NPT = 312
CPD = 6
SLICE = 16
EQUIV = 56
FAR = 48
ROWS = 3 * EQUIV
PER_OWNER = 2 * SLICE
WIDE = 384
OFFSETS = (1, -1, 2, -2, 3, -3)
CELLS = CPD * (len(OFFSETS) + 1)
OWNABLE = 3 * CPD
SHARE = NPT // 4
SHARE_PAD = 80
COUNT = 127

inv_eight_pi = 1.0 / (8.0 * math.pi)
smooth_sq = 0.0625
inner_radius = 1.05
outer_radius = 2.95
MESH = pl.DeviceIdType.MESH
VMEM = pl.BlockSpec(memory_space=pltpu.VMEM)
SMEM = pl.BlockSpec(memory_space=pltpu.SMEM)
f32 = jnp.float32
bf16 = jnp.bfloat16
i32 = jnp.int32


def surface_table():
    ladder = [-1.0, -1.0 / 3.0, 1.0 / 3.0, 1.0]
    corners = [
        (a, b, c)
        for a in ladder
        for b in ladder
        for c in ladder
        if max(abs(a), abs(b), abs(c)) == 1.0
    ]
    return np.array(corners, dtype=np.float32)


def iota(shape, dim):
    return lax.broadcasted_iota(i32, shape, dim)


def dot(a, b):
    return jnp.dot(a, b, preferred_element_type=f32)


def dot_nt(a, b):
    return lax.dot_general(a, b, (((1,), (1,)), ((), ())), preferred_element_type=f32)


def halves(value):
    top = value.astype(bf16)
    return top, (value - top.astype(f32)).astype(bf16)


def dot_wide(a, b):
    a_top, a_low = halves(a)
    b_top, b_low = halves(b)
    return dot(a_top, b_top) + (dot(a_top, b_low) + dot(a_low, b_top))


DX, DY, DZ, FX, FY, FZ, PX, PY, PZ, REL = range(10)
FEATURES = 24
DEPTH = FEATURES + 8 * CPD
FAR_AWAY = 1e30
LIMIT = 20 << 20
HBM = pl.BlockSpec(memory_space=pltpu.HBM)
DUMMY = CELLS
BATCH = 3
EARLY = 7


def thirds(value):
    top = value.astype(bf16).astype(f32)
    rest = value - top
    middle = rest.astype(bf16).astype(f32)
    return top, middle, rest - middle


def pull(offset, strength):
    dx, dy, dz = offset
    fx, fy, fz = strength
    shifted = (dx * dx + dy * dy) + (dz * dz + smooth_sq)
    inner = (dx * fx + dy * fy) + dz * fz
    root = lax.rsqrt(shifted)
    cube = root * root * root
    return root + smooth_sq * cube, cube * inner


def in_hbm(array):
    return pltpu.with_memory_space_constraint(array, pltpu.HBM)


def remote(src, dst, send_sem, recv_sem, target):
    return pltpu.make_async_remote_copy(
        src_ref=src,
        dst_ref=dst,
        send_sem=send_sem,
        recv_sem=recv_sem,
        device_id=target,
        device_id_type=MESH,
    )


def greet(targets):
    barrier = pltpu.get_barrier_semaphore()
    for target in targets:
        pl.semaphore_signal(barrier, inc=1, device_id=target, device_id_type=MESH)
    pl.semaphore_wait(barrier, len(targets))


def beside(axis, offsets):
    count = lax.axis_size(axis)
    me = lax.axis_index(axis)
    return [{axis: lax.rem(me + (off + count), count)} for off in offsets]


def first_kernel(
    disp_hbm,
    leaf_hbm,
    near_hbm,
    stiff_hbm,
    surf_hbm,
    inverse_hbm,
    comp_ref,
    lists_ref,
    gat_ref,
    lefts_ref,
    spots_ref,
    rights_ref,
    held_disp,
    held_leaf,
    disp_ref,
    surf_ref,
    leaf_ref,
    near_ref,
    stiff_ref,
    inverse_ref,
    disp,
    leaves,
    force,
    listed_ref,
    relation,
    wanted_ref,
    wide,
    terms_top,
    terms_low,
    member_ref,
    total,
    density,
    block_ref,
    send_disp,
    recv_disp,
    send_leaf,
    recv_leaf,
    load_sem,
    own_sem,
    z_send,
    z_recv,
    y_send,
    y_recv,
    c_send,
    c_recv,
):
    me = lax.axis_index("cells")
    portion = lax.axis_index("leaf")
    start = lax.rem(me + 63, 64)
    block = start // 4
    leaf_load = pltpu.make_async_copy(leaf_hbm, leaf_ref.at[0], load_sem.at[0])
    loads = [
        pltpu.make_async_copy(
            near_hbm.at[:, pl.ds(pl.multiple_of(lax.rem(block + k, 16) * 128, 128), 128)],
            near_ref.at[k],
            load_sem.at[1 + k],
        )
        for k in range(2)
    ]
    loads.append(pltpu.make_async_copy(stiff_hbm, stiff_ref, load_sem.at[3]))
    loads.append(pltpu.make_async_copy(inverse_hbm, inverse_ref, load_sem.at[4]))
    loads.append(pltpu.make_async_copy(surf_hbm, surf_ref, load_sem.at[5]))
    disp_load = pltpu.make_async_copy(disp_hbm, disp_ref, load_sem.at[6])
    disp_load.start()
    leaf_load.start()
    for load in loads:
        load.start()
    core = lax.rem(me, 2)
    z = lax.rem(me // 2, 8)
    y = me // 16

    def device(y_at, z_at, core_at):
        return {"cells": (y_at * 8 + z_at) * 2 + core_at}

    sides = beside("cells", OFFSETS)
    z_targets = [device(y, lax.rem(z + k, 8), core) for k in range(1, 8)]
    y_targets = [device(lax.rem(y + k, 4), z, core) for k in range(1, 4)]
    c_target = device(y, z, 1 - core)
    greet([*sides, *z_targets, *y_targets, c_target])
    disp_load.wait()
    leaf_load.wait()
    copies = []
    for slot, target in enumerate(sides):
        copies.append(
            remote(disp_ref, held_disp.at[slot], send_disp.at[slot], recv_disp.at[slot], target)
        )
        copies.append(
            remote(leaf_ref, held_leaf.at[slot], send_leaf.at[slot], recv_leaf.at[slot], target)
        )
    for copy in copies:
        copy.start()

    comp_ref[...] = jnp.zeros_like(comp_ref)
    disp[...] = jnp.zeros_like(disp)
    leaves[...] = jnp.zeros_like(leaves)

    def place_cells(home, points, leaf_row):
        for k in range(CPD):
            at = slice(NPT * k, NPT * (k + 1))
            row = home * CPD + k
            for a in range(3):
                disp[48 * a + row : 48 * a + row + 1, 0:NPT] = points[a : a + 1, at]
            leaves[row : row + 1, 0:NPT] = leaf_row[:, at]

    def fill_table(rows):
        live = iota((rows, WIDE), 1) < NPT
        rel = jnp.where(live, (leaves[0:rows, :] - PER_OWNER * (me - 4)) & 2047, -1)
        for a in range(3):
            comp_ref[DX + a, 0:rows, :] = disp[48 * a : 48 * a + rows, :]
        comp_ref[REL, 0:rows, :] = rel.astype(f32)
        comp_ref[PX, 0:rows, :] = comp_ref[DX, 0:rows, :] + (2 * (rel >> 4) + 1).astype(f32)
        comp_ref[PY, 0:rows, :] = comp_ref[DY, 0:rows, :] + (2 * ((rel >> 2) & 3) + 1).astype(f32)
        comp_ref[PZ, 0:rows, :] = comp_ref[DZ, 0:rows, :] + (2 * (rel & 3) + 1).astype(f32)
        relf = rel.astype(f32)
        first = jnp.min(jnp.where(live, relf, 1e9), axis=1, keepdims=True)
        last = jnp.max(relf, axis=1, keepdims=True)
        return first, last

    place_cells(0, disp_ref[...], leaf_ref[...])
    first, last = fill_table(8)

    for load in loads:
        load.wait()
    both = jnp.concatenate([near_ref[0], near_ref[1]], axis=1)
    listed = both[:, 0:128]
    for k in range(1, 4):
        listed = jnp.where(lax.rem(start, 4) == k, both[:, 32 * k : 32 * k + 128], listed)
    listed_ref[...] = jnp.where(listed >= 0, (listed - PER_OWNER * (me - 2)) & 2047, -1)
    source_leaf = iota((160, 128), 0)

    def eight_entries(index, near):
        rows = listed_ref[pl.ds(pl.multiple_of(8 * index, 8), 8), :]
        for k in range(8):
            near = near + jnp.where(rows[k : k + 1, :] == source_leaf, 1.0, 0.0)
        return near

    near = lax.fori_loop(0, 6, eight_entries, jnp.zeros((160, 128), f32))
    relation[...] = near.astype(bf16)
    row8, lane8 = iota((8, 128), 0).astype(f32), iota((8, 128), 1).astype(f32)
    leaf_rows = [
        jnp.where((lane8 == first[t : t + 1] - 3.0 * PER_OWNER + row8) & (row8 < 3.0), 1.0, 0.0)
        for t in range(CPD)
    ]
    wanted_ref[...] = dot_nt(
        jnp.concatenate(leaf_rows, axis=0).astype(bf16), relation[...]
    ).astype(bf16)

    pick_row, pick_lane = iota((SHARE_PAD, WIDE), 0), iota((SHARE_PAD, WIDE), 1)
    pick16 = ((pick_lane == pick_row + SHARE * portion) & (pick_row < SHARE)).astype(f32).astype(bf16)
    slot = iota((SHARE_PAD, 128), 1)
    slot_turn = lax.rem(slot, 6)
    left_first = (slot < 18) & (slot_turn < 3) | (slot == 18)
    left_second = (slot < 18) & (slot_turn >= 3) & (slot_turn < 5) | (slot == 19)
    row32 = iota((32, WIDE), 0)

    def one_own(t, carry):
        rel = comp_ref[REL, pl.ds(t, 1), :]
        px, py, pz = [comp_ref[PX + a, pl.ds(t, 1), :] for a in range(3)]
        lowest = jnp.min(jnp.where(rel >= 0.0, rel, 1e9), axis=1, keepdims=True)
        owner = jnp.floor(lowest * (1.0 / PER_OWNER))
        py4, pz4 = py - 4.0, pz - 4.0
        extra = iota((8, WIDE), 0)
        place = jnp.where(extra == 0, px, jnp.where(extra == 1, py, jnp.where(extra == 2, pz, rel)))
        top, middle, low = thirds(place)
        spot = dot_nt(pick16, top.astype(bf16)) + (
            dot_nt(pick16, middle.astype(bf16)) + dot_nt(pick16, low.astype(bf16))
        )
        for a in range(3):
            spots_ref[t, a] = jnp.broadcast_to(spot[:, a : a + 1], (SHARE_PAD, 128))
        leaf_at = (spot[:, 3:4] - lowest).astype(i32)
        matched = (slot - (FEATURES + 8 * t) == leaf_at) & (leaf_at >= 0) & (leaf_at < 3)
        for w in range(3):
            px4 = px - (4.0 * (owner + float(w - 1)) + 2.0)
            square = (px4 * px4 + py4 * py4) + pz4 * pz4
            rows = jnp.where(
                row32 < 6,
                px4,
                jnp.where(row32 < 12, py4, jnp.where(row32 < 18, pz4, square)),
            )
            rows = jnp.concatenate([rows, jnp.zeros((96, WIDE), f32)], axis=0)
            top, middle, low = thirds(rows)
            value = dot_nt(pick16, top.astype(bf16)) + (
                dot_nt(pick16, middle.astype(bf16)) + dot_nt(pick16, low.astype(bf16))
            )
            top, middle, low = thirds(value)
            chosen = jnp.where(left_first, top, jnp.where(left_second, middle, low))
            chosen = jnp.where((slot >= 21) & (slot < 24), 1.0, chosen)
            chosen = jnp.where(slot >= FEATURES, jnp.where(matched, 1.0, 0.0), chosen)
            lefts_ref[3 * t + w] = chosen[:, 0:DEPTH].astype(bf16)
        return carry

    lax.fori_loop(0, CPD, one_own, 0)
    for a in range(3):
        wide[a] = jnp.broadcast_to(outer_radius * surf_ref[:, a : a + 1], (EQUIV, 128))

    for copy in copies:
        copy.wait()
    for home in range(1, len(OFFSETS) + 1):
        place_cells(home, held_disp[home - 1], held_leaf[home - 1])
    first, last = fill_table(48)
    force[...] = dot_wide(disp[0:144, 0:NPT], stiff_ref[...])
    for a in range(3):
        comp_ref[FX + a, 0:48, 0:NPT] = force[48 * a : 48 * a + 48, :]

    total[...] = jnp.zeros_like(total)

    def one_home(home, carry):
        for k in range(CPD):
            c = CPD * home + k
            d = [comp_ref[DX + a, pl.ds(c, 1), :] for a in range(3)]
            f = [comp_ref[FX + a, pl.ds(c, 1), :] for a in range(3)]
            rel = comp_ref[REL, pl.ds(c, 1), :].astype(i32) - 4 * PER_OWNER
            member = (iota((PER_OWNER, WIDE), 0) == rel).astype(f32).astype(bf16)
            member_ref[:, WIDE * k : WIDE * (k + 1)] = member
            for b in range(WIDE // 128):
                lanes = slice(128 * b, 128 * b + 128)
                out = slice(WIDE * k + 128 * b, WIDE * k + 128 * b + 128)
                for g in range(EQUIV // 8):
                    at = slice(8 * g, 8 * g + 8)
                    r = [wide[a, at, :] - d[a][:, lanes] for a in range(3)]
                    fb = [f[a][:, lanes] for a in range(3)]
                    even, along = pull(r, fb)
                    for a in range(3):
                        row = EQUIV * a + 8 * g
                        top, low = halves(even * fb[a] + along * r[a])
                        terms_top[row : row + 8, out] = top
                        terms_low[row : row + 8, out] = low
        total[...] += dot_nt(terms_top[...], member_ref[...]) + dot_nt(terms_low[...], member_ref[...])
        return carry

    lax.fori_loop(0, 3, one_home, 0)
    density[...] = dot_wide(inverse_ref[...], total[...] * inv_eight_pi)
    block_ref[...] = jnp.zeros_like(block_ref)
    for part in range(4):

        @pl.when(portion == part)
        def _():
            for a in range(3):
                rows = density[EQUIV * a + 14 * part : EQUIV * a + 14 * part + 14, :]
                block_ref[0:14, PER_OWNER * a : PER_OWNER * (a + 1)] = rows

    row = core * 4 + y
    own = pltpu.make_async_copy(block_ref, gat_ref.at[row, z], own_sem)
    own.start()
    z_copies = [
        remote(block_ref, gat_ref.at[row, z], z_send.at[k], z_recv.at[k], target)
        for k, target in enumerate(z_targets)
    ]
    for copy in z_copies:
        copy.start()

    low = jnp.floor(first * (1.0 / 16.0))
    high = jnp.floor(last * (1.0 / 16.0))
    lane = iota((48, 128), 1)
    which = iota((48, 1), 0).astype(f32)
    real = which < float(CELLS)
    flags = []
    for t in range(CPD):
        low_t, high_t = low[t : t + 1], high[t : t + 1]
        flags.append(jnp.where((high >= low_t - 1.0) & (low <= high_t + 1.0) & real, 1.0, 0.0))
    owner = jnp.floor(low * 0.5)
    union = flags[0]
    for t in range(1, CPD):
        union = jnp.maximum(union, flags[t])
    flags.append(union)
    table = jnp.zeros((48, 128), f32)
    for t, flag in enumerate(flags):
        table = table + jnp.where(lane == t, flag, 0.0)
    before = (iota((48, 48), 0) > iota((48, 48), 1)).astype(f32)
    rank = dot(before, table)
    count = jnp.sum(table, axis=0, keepdims=True)
    lane_row = iota((1, 128), 1)
    lists_ref[...] = jnp.zeros_like(lists_ref)
    for t, flag in enumerate(flags):
        hit = (rank[:, t : t + 1] == lane.astype(f32)) & (flag > 0.0)
        line = jnp.sum(jnp.where(hit, which, 0.0), axis=0, keepdims=True)
        line = jnp.where(lane_row.astype(f32) >= count[:, t : t + 1], float(DUMMY), line)
        line = jnp.where(lane_row == COUNT, count[:, t : t + 1], line)
        lists_ref[t : t + 1, :] = line.astype(i32)
    square = iota((48, 128), 0) == lane
    line = jnp.sum(jnp.where(square, owner, 0.0), axis=0, keepdims=True)
    lists_ref[7:8, :] = line.astype(i32)

    feature = iota((FEATURES, WIDE), 0)
    turn = lax.rem(feature, 6)
    use_top = (feature < 18) & ((turn == 0) | (turn == 3) | (turn == 5)) | (feature == 21)
    use_middle = (feature < 18) & ((turn == 1) | (turn == 4)) | (feature == 22)

    def factors(x, y, z, last):
        value = jnp.where(
            feature < 6, x, jnp.where(feature < 12, y, jnp.where(feature < 18, z, last))
        )
        top, middle, low = thirds(value)
        return jnp.where(use_top, top, jnp.where(use_middle, middle, low))

    def some_sources(index, carry):
        cells = [BATCH * index + k for k in range(BATCH)]
        rels = [comp_ref[REL, pl.ds(c, 1), :].astype(i32) for c in cells]
        hits = [
            (iota((160, WIDE), 0) == rel - 2 * PER_OWNER).astype(f32).astype(bf16) for rel in rels
        ]
        reaches = [dot(wanted_ref[...], hit) for hit in hits]
        for k, c in enumerate(cells):
            rel = rels[k]
            px = comp_ref[PX, pl.ds(c, 1), :] - (4 * (rel >> 5) + 2).astype(f32)
            py = comp_ref[PY, pl.ds(c, 1), :] - 4.0
            pz = comp_ref[PZ, pl.ds(c, 1), :] - 4.0
            fx, fy, fz = [comp_ref[FX + a, pl.ds(c, 1), :] for a in range(3)]
            square = (px * px + py * py) + (pz * pz + smooth_sq)
            along = (px * fx + py * fy) + pz * fz
            near_rows = factors(-2.0 * px, -2.0 * py, -2.0 * pz, square)
            near_rows = jnp.where((feature >= 18) & (feature < 21), 1.0, near_rows)
            push_rows = factors(fx, fy, fz, -along)
            push_rows = jnp.where((feature >= 18) & (feature < 21), 0.0, push_rows)
            mask_rows = FAR_AWAY - FAR_AWAY * reaches[k]
            rights_ref[c, :, 0:WIDE] = jnp.concatenate([near_rows, mask_rows], axis=0).astype(bf16)
            rights_ref[c, :, WIDE : 2 * WIDE] = jnp.concatenate(
                [push_rows, jnp.zeros((8 * CPD, WIDE), f32)], axis=0
            ).astype(bf16)
        return carry

    rights_ref[DUMMY] = jnp.where(iota((DEPTH, 2 * WIDE), 0) == 21, FAR_AWAY, 0.0).astype(bf16)
    lax.fori_loop(0, EARLY, some_sources, 0)

    own.wait()
    y_copies, c_copies = [], []

    def pass_on(at, where, index):
        place = gat_ref.at[at, where]
        copy = remote(place, place, c_send.at[index], c_recv.at[index], c_target)
        copy.start()
        c_copies.append(copy)

    for order, k in enumerate((0, 1, 7, 2, 6, 3, 5, 4)):
        where = lax.rem(z - k + 8, 8)
        if k:
            z_copies[k - 1].wait_recv()
        place = gat_ref.at[row, where]
        for side, target in enumerate(y_targets):
            index = 3 * order + side
            copy = remote(place, place, y_send.at[index], y_recv.at[index], target)
            copy.start()
            y_copies.append(copy)
        pass_on(row, where, order)
    lax.fori_loop(EARLY, CELLS // BATCH, some_sources, 0)
    for order, k in enumerate((0, 1, 7, 2, 6, 3, 5, 4)):
        where = lax.rem(z - k + 8, 8)
        for side in range(3):
            index = 3 * order + side
            y_copies[index].wait_recv()
            pass_on(core * 4 + lax.rem(y - side + 3, 4), where, 8 + index)
    for copy in (*z_copies, *y_copies):
        copy.wait_send()
    for copy in c_copies:
        copy.wait()


def first(displacement, point_leaf, near_list, stiffness, surf, up_inverse):
    npoints = displacement.shape[1]
    sides = len(OFFSETS)
    dma = pltpu.SemaphoreType.DMA
    return pl.pallas_call(
        first_kernel,
        out_shape=(
            jax.ShapeDtypeStruct((10, 48, WIDE), f32),
            jax.ShapeDtypeStruct((8, 128), i32),
            jax.ShapeDtypeStruct((8, 8, 16, 128), f32),
            jax.ShapeDtypeStruct((3 * CPD, SHARE_PAD, DEPTH), bf16),
            jax.ShapeDtypeStruct((CPD, 3, SHARE_PAD, 128), f32),
            jax.ShapeDtypeStruct((CELLS + 1, DEPTH, 2 * WIDE), bf16),
        ),
        in_specs=[HBM] * 6,
        out_specs=(VMEM,) * 6,
        scratch_shapes=[
            pltpu.VMEM((sides, 3, npoints), f32),
            pltpu.VMEM((sides, 1, npoints), i32),
            pltpu.VMEM((3, npoints), f32),
            pltpu.VMEM((EQUIV, 8), f32),
            pltpu.VMEM((1, npoints), i32),
            pltpu.VMEM((2, FAR, 128), i32),
            pltpu.VMEM((NPT, NPT), f32),
            pltpu.VMEM((ROWS, ROWS), f32),
            pltpu.VMEM((144, WIDE), f32),
            pltpu.VMEM((48, WIDE), i32),
            pltpu.VMEM((144, NPT), f32),
            pltpu.VMEM((FAR, 128), i32),
            pltpu.VMEM((160, 128), bf16),
            pltpu.VMEM((8 * CPD, 160), bf16),
            pltpu.VMEM((3, EQUIV, 128), f32),
            pltpu.VMEM((ROWS, CPD * WIDE), bf16),
            pltpu.VMEM((ROWS, CPD * WIDE), bf16),
            pltpu.VMEM((PER_OWNER, CPD * WIDE), bf16),
            pltpu.VMEM((ROWS, PER_OWNER), f32),
            pltpu.VMEM((ROWS, PER_OWNER), f32),
            pltpu.VMEM((16, 128), f32),
            dma((sides,)),
            dma((sides,)),
            dma((sides,)),
            dma((sides,)),
            dma((7,)),
            dma,
            dma((7,)),
            dma((7,)),
            dma((24,)),
            dma((24,)),
            dma((32,)),
            dma((32,)),
        ],
        compiler_params=pltpu.CompilerParams(
            collective_id=0, has_side_effects=True, vmem_limit_bytes=LIMIT
        ),
        name="first",
    )(*(in_hbm(x) for x in (displacement, point_leaf, near_list, stiffness, surf, up_inverse)))


def near_kernel(lists, comp_ref, lefts, spots, rights, out_ref, even_pairs, odd_pairs, sums):
    portion = lax.axis_index("leaf")

    def multiply(t, index, products):
        c = lists[t, index]
        w = jnp.clip(lists[7, c] - lists[7, t] + 1, 0, 2)
        products[...] = dot(lefts[3 * t + w], rights[c])

    def add_pair(t, index, products):
        c = lists[t, index]
        p = [comp_ref[PX + a, pl.ds(c, 1), :] for a in range(3)]
        f = [comp_ref[FX + a, pl.ds(c, 1), :] for a in range(3)]
        for g in range(SHARE_PAD // 8):
            at = slice(8 * g, 8 * g + 8)
            added = None
            for b in range(WIDE // 128):
                lanes = slice(128 * b, 128 * b + 128)
                shifted = products[at, lanes]
                inner = products[at, WIDE + 128 * b : WIDE + 128 * b + 128]
                root = lax.rsqrt(shifted)
                cube = root * root * root
                even = root + smooth_sq * cube
                along = cube * inner
                part = [even * f[a][:, lanes] - along * p[a][:, lanes] for a in range(3)]
                part.append(along)
                if added is None:
                    added = part
                else:
                    added = [u + v for u, v in zip(added, part)]
            for a in range(4):
                sums[t, a, at, :] += added[a]

    sums[...] = jnp.zeros_like(sums)
    multiply(0, 0, even_pairs)

    def one_target(t, carry):
        steps = (lists[t, COUNT] + 1) // 2

        def two_pairs(index, carry):
            multiply(t, 2 * index + 1, odd_pairs)
            add_pair(t, 2 * index, even_pairs)
            ends = index + 1 == steps
            after = jnp.where(ends, jnp.minimum(t + 1, CPD - 1), t)
            multiply(after, jnp.where(ends, 0, 2 * index + 2), even_pairs)
            add_pair(t, 2 * index + 1, odd_pairs)
            return carry

        lax.fori_loop(0, steps, two_pairs, 0)
        return carry

    lax.fori_loop(0, CPD, one_target, 0)
    pick_row, pick_lane = iota((SHARE_PAD, WIDE), 0), iota((SHARE_PAD, WIDE), 1)
    pick = (pick_lane == pick_row + SHARE * portion) & (pick_row < SHARE)

    def finish(index, carry):
        for t in (2 * index, 2 * index + 1):
            for a in range(3):
                total = sums[t, a] + spots[t, a] * sums[t, 3]
                column = jnp.sum(total, axis=1, keepdims=True) * inv_eight_pi
                row = jnp.sum(jnp.where(pick, column, 0.0), axis=0, keepdims=True)
                out_ref[a, pl.ds(t, 1), :] = row
        return carry

    lax.fori_loop(0, CPD // 2, finish, 0)


def near_field(lists, comp, lefts, spots, rights):
    return pl.pallas_call(
        near_kernel,
        out_shape=jax.ShapeDtypeStruct((3, 8, WIDE), f32),
        in_specs=[SMEM] + [VMEM] * 4,
        out_specs=VMEM,
        scratch_shapes=[
            pltpu.VMEM((SHARE_PAD, 2 * WIDE), f32),
            pltpu.VMEM((SHARE_PAD, 2 * WIDE), f32),
            pltpu.VMEM((CPD, 4, SHARE_PAD, 128), f32),
        ],
        compiler_params=pltpu.CompilerParams(vmem_limit_bytes=LIMIT),
        name="near_field",
    )(lists, comp, lefts, spots, rights)


def far_part(
    points, gat_ref, far_ref, far_load, surf_ref, inverse_ref, local_ref, far4, sources, packed, pushes, mids, total
):
    me = lax.axis_index("cells")
    portion = lax.axis_index("leaf")
    lane = iota((16, 128), 1)

    def one_tile(tile, carry):
        for half in range(2):
            rows = [jnp.zeros((16, 128), f32) for _ in range(3)]
            for v in range(4):
                at = 8 * tile + 4 * half + v
                value = gat_ref[at // 8, at - at // 8 * 8]
                for a in range(3):
                    shift = (PER_OWNER * (v - a)) % 128
                    moved = pltpu.roll(value, shift, 1) if shift else value
                    rows[a] = jnp.where(lane // PER_OWNER == v, moved, rows[a])
            top, low = halves(jnp.concatenate(rows, axis=0))
            packed[tile, 0:48, 128 * half : 128 * half + 128] = top
            packed[tile, 48:96, 128 * half : 128 * half + 128] = low
        return carry

    lax.fori_loop(0, 8, one_tile, 0)

    far_load.wait()
    entries = far_ref[...]
    mine = lax.rem(me, 4)
    lane48 = iota((FAR, 128), 1) // PER_OWNER
    picked = jnp.zeros((FAR, 128), i32)
    for place in range(4):
        moved = entries
        for k in range(1, 4):
            turned = pltpu.roll(entries, PER_OWNER * k, 1)
            moved = jnp.where(lax.rem(mine + k, 4) == place, turned, moved)
        far4[place] = moved
    for place in range(4):
        rows = far4[place, pl.ds(place, FAR // 4, stride=4), :]
        chosen = iota((FAR // 4, 128), 1) // PER_OWNER == place
        if place == 0:
            merged = rows
        else:
            merged = jnp.where(chosen, rows, merged)
    owner = merged >> 5
    spot = (((owner & 1) << 5) + (owner >> 1)) * PER_OWNER + (merged & 31)
    sources[0:12, :] = jnp.where(merged >= 0, spot, -1)
    target = me * PER_OWNER + (iota((12, 128), 1) & 31)
    mids[0, 0:12, :] = (2 * ((target >> 4) - (merged >> 4))).astype(f32)
    mids[1, 0:12, :] = (2 * (((target >> 2) & 3) - ((merged >> 2) & 3))).astype(f32)
    mids[2, 0:12, :] = (2 * ((target & 3) - (merged & 3))).astype(f32)

    def one_gather(index, carry):
        first = sources[pl.ds(2 * index, 1), :]
        second = sources[pl.ds(2 * index + 1, 1), :]
        wanted = jnp.concatenate([first, second], axis=1)
        found = jnp.zeros((96, 256), f32)
        for tile in range(8):
            onehot = (iota((256, 256), 0) + 256 * tile == wanted).astype(f32).astype(bf16)
            found = found + dot(packed[tile], onehot)
        value = found[0:48] + found[48:96]
        pushes[2 * index] = value[:, 0:128]
        pushes[2 * index + 1] = value[:, 128:256]
        return carry

    lax.fori_loop(0, 6, one_gather, 0)
    total[...] = jnp.zeros_like(total)

    def one_block(index, carry):
        mid = [mids[a, pl.ds(index, 1), :] for a in range(3)]
        for g in range(EQUIV // 8):
            at = slice(8 * g, 8 * g + 8)
            check = [mid[a] + inner_radius * surf_ref[at, a : a + 1] for a in range(3)]
            sums = [total[EQUIV * a + 8 * g : EQUIV * a + 8 * g + 8, :] for a in range(3)]
            for j in range(14):
                f = [pushes[index, 16 * a + j : 16 * a + j + 1, :] for a in range(3)]
                r = [check[a] - points[3 * (14 * portion + j) + a] for a in range(3)]
                even, along = pull(r, f)
                sums = [sums[a] + (even * f[a] + along * r[a]) for a in range(3)]
            for a in range(3):
                total[EQUIV * a + 8 * g : EQUIV * a + 8 * g + 8, :] = sums[a]
        return carry

    lax.fori_loop(0, 12, one_block, 0)
    value = total[...] * inv_eight_pi
    value = value + pltpu.roll(value, 64, 1)
    value = value + pltpu.roll(value, 32, 1)
    local_ref[...] = dot_wide(inverse_ref[...], value)


def last_kernel(
    points,
    gat_ref,
    far_hbm,
    surf_ref,
    inverse_ref,
    comp_ref,
    near_ref,
    out_ref,
    far_ref,
    load_sem,
    far4,
    sources,
    packed,
    pushes,
    mids,
    total,
    local_ref,
    held_local,
    factors,
    spread_ref,
    part_ref,
    held_part,
    send_local,
    recv_local,
    send_part,
    recv_part,
):
    block = pl.multiple_of(lax.axis_index("cells") // 4 * 128, 128)
    far_load = pltpu.make_async_copy(far_hbm.at[:, pl.ds(block, 128)], far_ref, load_sem)
    far_load.start()
    sides = beside("cells", (1, -1))
    mates = beside("leaf", (1, 2, 3))
    barrier = pltpu.get_barrier_semaphore()
    for target in (*sides, *mates):
        pl.semaphore_signal(barrier, inc=1, device_id=target, device_id_type=MESH)
    far_part(
        points, gat_ref, far_ref, far_load, surf_ref, inverse_ref, local_ref, far4, sources, packed, pushes, mids, total
    )
    pl.semaphore_wait(barrier, 5)
    copies = [
        remote(local_ref, held_local.at[k], send_local.at[k], recv_local.at[k], target)
        for k, target in enumerate(sides)
    ]
    for copy in copies:
        copy.start()
    for copy in copies:
        copy.wait()
    lane = iota((ROWS, 128), 1) // PER_OWNER
    value = jnp.where(
        lane == 0, held_local[0], jnp.where(lane == 1, local_ref[...], held_local[1])
    )
    top, low = halves(value)
    factors[0:ROWS, :] = top
    factors[ROWS : 2 * ROWS, :] = low

    def one_cell(t, carry):
        rel = comp_ref[REL, pl.ds(t, 1), :].astype(i32) - 3 * PER_OWNER
        member = (iota((128, WIDE), 0) == rel).astype(f32).astype(bf16)
        both = dot(factors[...], member)
        spread_ref[t] = both[0:ROWS] + both[ROWS : 2 * ROWS]
        return carry

    lax.fori_loop(0, CPD, one_cell, 0)
    for t in range(CPD):
        d = [comp_ref[DX + a, t : t + 1, :] for a in range(3)]
        sums = [jnp.zeros((8, WIDE), f32) for _ in range(3)]
        for g in range(EQUIV // 8):
            at = slice(8 * g, 8 * g + 8)
            r = [d[a] - outer_radius * surf_ref[at, a : a + 1] for a in range(3)]
            f = [spread_ref[t, EQUIV * a + 8 * g : EQUIV * a + 8 * g + 8, :] for a in range(3)]
            even, along = pull(r, f)
            sums = [sums[a] + (even * f[a] + along * r[a]) for a in range(3)]
        for a in range(3):
            row = jnp.sum(sums[a], axis=0, keepdims=True) * inv_eight_pi + near_ref[a, t : t + 1, :]
            part_ref[a : a + 1, NPT * t : NPT * (t + 1)] = row[:, 0:NPT]
    copies = [
        remote(part_ref, held_part.at[k], send_part.at[k], recv_part.at[k], target)
        for k, target in enumerate(mates)
    ]
    for copy in copies:
        copy.start()
    for copy in copies:
        copy.wait()
    out_ref[...] = (part_ref[...] + held_part[1]) + (held_part[0] + held_part[2])


def last(points, gathered, far_list, surf, down_inverse, comp, near, npoints):
    dma = pltpu.SemaphoreType.DMA
    return pl.pallas_call(
        last_kernel,
        out_shape=jax.ShapeDtypeStruct((3, npoints), f32),
        in_specs=[SMEM, VMEM, HBM] + [VMEM] * 4,
        out_specs=VMEM,
        scratch_shapes=[
            pltpu.VMEM((FAR, 128), i32),
            dma,
            pltpu.VMEM((4, FAR, 128), i32),
            pltpu.VMEM((16, 128), i32),
            pltpu.VMEM((8, 96, 256), bf16),
            pltpu.VMEM((12, FAR, 128), f32),
            pltpu.VMEM((3, 16, 128), f32),
            pltpu.VMEM((ROWS, 128), f32),
            pltpu.VMEM((ROWS, 128), f32),
            pltpu.VMEM((2, ROWS, 128), f32),
            pltpu.VMEM((2 * ROWS, 128), bf16),
            pltpu.VMEM((CPD, ROWS, WIDE), f32),
            pltpu.VMEM((3, npoints), f32),
            pltpu.VMEM((3, 3, npoints), f32),
            dma((2,)),
            dma((2,)),
            dma((3,)),
            dma((3,)),
        ],
        compiler_params=pltpu.CompilerParams(
            collective_id=1, has_side_effects=True, vmem_limit_bytes=LIMIT
        ),
        name="last",
    )(points, gathered, in_hbm(far_list), surf, down_inverse, comp, near)


def body(displacement, point_leaf, near_list, far_list, stiffness, up_inverse, down_inverse):
    table = surface_table()
    surf = jnp.asarray(np.pad(table, ((0, 0), (0, 5))))
    points = jnp.asarray((inner_radius * table).astype(np.float32).reshape(-1))
    comp, lists, gathered, lefts, spots, rights = first(
        displacement, point_leaf, near_list, stiffness, surf, up_inverse
    )
    near = near_field(lists, comp, lefts, spots, rights)
    return last(
        points, gathered, far_list, surf, down_inverse, comp, near, displacement.shape[1]
    )


def solution(mesh):
    in_specs = (P(None, "cells"), P("cells"), P(), P(), P(), P(), P())
    out_specs = P(None, "cells")
    return jax.shard_map(body, mesh=mesh, in_specs=in_specs, out_specs=out_specs, check_vma=False)
```

```python
import math

import jax
import jax.numpy as jnp
import numpy as np
from jax import lax
from jax.experimental import pallas as pl
from jax.experimental.pallas import tpu as pltpu
from jax.sharding import PartitionSpec as P

NPT = 312
CPD = 6
SLICE = 16
EQUIV = 56
FAR = 48
ROWS = 3 * EQUIV
PER_OWNER = 2 * SLICE
WIDE = 384
OFFSETS = (1, -1, 2, -2, 3, -3)
CELLS = CPD * (len(OFFSETS) + 1)
OWNABLE = 3 * CPD
SHARE = NPT // 4
SHARE_PAD = 80
COUNT = 127

inv_eight_pi = 1.0 / (8.0 * math.pi)
smooth_sq = 0.0625
inner_radius = 1.05
outer_radius = 2.95
MESH = pl.DeviceIdType.MESH
VMEM = pl.BlockSpec(memory_space=pltpu.VMEM)
SMEM = pl.BlockSpec(memory_space=pltpu.SMEM)
f32 = jnp.float32
bf16 = jnp.bfloat16
i32 = jnp.int32


def surface_table():
    ladder = [-1.0, -1.0 / 3.0, 1.0 / 3.0, 1.0]
    corners = [
        (a, b, c)
        for a in ladder
        for b in ladder
        for c in ladder
        if max(abs(a), abs(b), abs(c)) == 1.0
    ]
    return np.array(corners, dtype=np.float32)


def iota(shape, dim):
    return lax.broadcasted_iota(i32, shape, dim)


def dot(a, b):
    return jnp.dot(a, b, preferred_element_type=f32)


def dot_nt(a, b):
    return lax.dot_general(a, b, (((1,), (1,)), ((), ())), preferred_element_type=f32)


def halves(value):
    top = value.astype(bf16)
    return top, (value - top.astype(f32)).astype(bf16)


def dot_wide(a, b):
    a_top, a_low = halves(a)
    b_top, b_low = halves(b)
    return dot(a_top, b_top) + (dot(a_top, b_low) + dot(a_low, b_top))


DX, DY, DZ, FX, FY, FZ, PX, PY, PZ, REL = range(10)
FEATURES = 24
DEPTH = FEATURES + 8 * CPD
FAR_AWAY = 1e30
LIMIT = 20 << 20
HBM = pl.BlockSpec(memory_space=pltpu.HBM)
DUMMY = CELLS
BATCH = 6
PARTS = 2
EARLY = 5
MIDDLE = 3


def thirds(value):
    top = value.astype(bf16).astype(f32)
    rest = value - top
    middle = rest.astype(bf16).astype(f32)
    return top, middle, rest - middle


def pull(offset, strength):
    dx, dy, dz = offset
    fx, fy, fz = strength
    shifted = (dx * dx + dy * dy) + (dz * dz + smooth_sq)
    inner = (dx * fx + dy * fy) + dz * fz
    root = lax.rsqrt(shifted)
    cube = root * root * root
    return root + smooth_sq * cube, cube * inner


def in_hbm(array):
    return pltpu.with_memory_space_constraint(array, pltpu.HBM)


def remote(src, dst, send_sem, recv_sem, target):
    return pltpu.make_async_remote_copy(
        src_ref=src,
        dst_ref=dst,
        send_sem=send_sem,
        recv_sem=recv_sem,
        device_id=target,
        device_id_type=MESH,
    )


def greet(targets):
    barrier = pltpu.get_barrier_semaphore()
    for target in targets:
        pl.semaphore_signal(barrier, inc=1, device_id=target, device_id_type=MESH)
    pl.semaphore_wait(barrier, len(targets))


def beside(axis, offsets):
    count = lax.axis_size(axis)
    me = lax.axis_index(axis)
    return [{axis: lax.rem(me + (off + count), count)} for off in offsets]


def add_pair(comp_ref, sums, t, c, products):
    p = [comp_ref[PX + a, pl.ds(c, 1), :] for a in range(3)]
    f = [comp_ref[FX + a, pl.ds(c, 1), :] for a in range(3)]
    for part in range(PARTS):
        groups = range(part * 10 // PARTS, (part + 1) * 10 // PARTS)
        added = {}
        for b in range(WIDE // 128):
            lanes = slice(128 * b, 128 * b + 128)
            pb = [value[:, lanes] for value in p]
            fb = [value[:, lanes] for value in f]
            for g in groups:
                at = slice(8 * g, 8 * g + 8)
                shifted = products[at, lanes]
                inner = products[at, WIDE + 128 * b : WIDE + 128 * b + 128]
                root = lax.rsqrt(shifted)
                cube = root * root * root
                even = root + smooth_sq * cube
                along = cube * inner
                one = [even * fb[a] - along * pb[a] for a in range(3)] + [along]
                added[g] = [u + v for u, v in zip(added[g], one)] if b else one
        for g in groups:
            at = slice(8 * g, 8 * g + 8)
            for a in range(4):
                sums[t, a, at, :] += added[g][a]


def first_kernel(
    disp_hbm,
    leaf_hbm,
    near_hbm,
    stiff_hbm,
    surf_hbm,
    inverse_hbm,
    comp_ref,
    lists_ref,
    gat_ref,
    lefts_ref,
    spots_ref,
    rights_ref,
    sums_ref,
    held_disp,
    held_leaf,
    disp_ref,
    surf_ref,
    leaf_ref,
    near_ref,
    stiff_ref,
    inverse_ref,
    disp,
    leaves,
    force,
    listed_ref,
    relation,
    wanted_ref,
    wide,
    owned_ref,
    terms_top,
    terms_low,
    member_ref,
    total,
    density,
    block_ref,
    even_pairs,
    odd_pairs,
    owners_ref,
    send_disp,
    recv_disp,
    send_leaf,
    recv_leaf,
    load_sem,
    own_sem,
    z_send,
    z_recv,
    y_send,
    y_recv,
    c_send,
    c_recv,
):
    me = lax.axis_index("cells")
    portion = lax.axis_index("leaf")
    start = lax.rem(me + 63, 64)
    block = start // 4
    leaf_load = pltpu.make_async_copy(leaf_hbm, leaf_ref.at[0], load_sem.at[0])
    loads = [
        pltpu.make_async_copy(
            near_hbm.at[:, pl.ds(pl.multiple_of(lax.rem(block + k, 16) * 128, 128), 128)],
            near_ref.at[k],
            load_sem.at[1 + k],
        )
        for k in range(2)
    ]
    loads.append(pltpu.make_async_copy(stiff_hbm, stiff_ref, load_sem.at[3]))
    loads.append(pltpu.make_async_copy(inverse_hbm, inverse_ref, load_sem.at[4]))
    loads.append(pltpu.make_async_copy(surf_hbm, surf_ref, load_sem.at[5]))
    disp_load = pltpu.make_async_copy(disp_hbm, disp_ref, load_sem.at[6])
    disp_load.start()
    leaf_load.start()
    for load in loads:
        load.start()
    core = lax.rem(me, 2)
    z = lax.rem(me // 2, 8)
    y = me // 16

    def device(y_at, z_at, core_at):
        return {"cells": (y_at * 8 + z_at) * 2 + core_at}

    sides = beside("cells", OFFSETS)
    z_targets = [device(y, lax.rem(z + k, 8), core) for k in range(1, 8)]
    y_targets = [device(lax.rem(y + k, 4), z, core) for k in range(1, 4)]
    c_target = device(y, z, 1 - core)
    greet([*sides, *z_targets, *y_targets, c_target])
    disp_load.wait()
    leaf_load.wait()
    copies = []
    for slot, target in enumerate(sides):
        copies.append(
            remote(disp_ref, held_disp.at[slot], send_disp.at[slot], recv_disp.at[slot], target)
        )
        copies.append(
            remote(leaf_ref, held_leaf.at[slot], send_leaf.at[slot], recv_leaf.at[slot], target)
        )
    for copy in copies:
        copy.start()

    comp_ref[...] = jnp.zeros_like(comp_ref)
    disp[...] = jnp.zeros_like(disp)
    leaves[...] = jnp.zeros_like(leaves)

    def place_cells(home, points, leaf_row):
        for k in range(CPD):
            at = slice(NPT * k, NPT * (k + 1))
            row = home * CPD + k
            for a in range(3):
                disp[48 * a + row : 48 * a + row + 1, 0:NPT] = points[a : a + 1, at]
            leaves[row : row + 1, 0:NPT] = leaf_row[:, at]

    def fill_table(rows):
        live = iota((rows, WIDE), 1) < NPT
        rel = jnp.where(live, (leaves[0:rows, :] - PER_OWNER * (me - 4)) & 2047, -1)
        for a in range(3):
            comp_ref[DX + a, 0:rows, :] = disp[48 * a : 48 * a + rows, :]
        comp_ref[REL, 0:rows, :] = rel.astype(f32)
        comp_ref[PX, 0:rows, :] = comp_ref[DX, 0:rows, :] + (2 * (rel >> 4) + 1).astype(f32)
        comp_ref[PY, 0:rows, :] = comp_ref[DY, 0:rows, :] + (2 * ((rel >> 2) & 3) + 1).astype(f32)
        comp_ref[PZ, 0:rows, :] = comp_ref[DZ, 0:rows, :] + (2 * (rel & 3) + 1).astype(f32)
        relf = rel.astype(f32)
        first = jnp.min(jnp.where(live, relf, 1e9), axis=1, keepdims=True)
        last = jnp.max(relf, axis=1, keepdims=True)
        return first, last

    place_cells(0, disp_ref[...], leaf_ref[...])
    first, last = fill_table(8)

    for load in loads:
        load.wait()
    both = jnp.concatenate([near_ref[0], near_ref[1]], axis=1)
    listed = both[:, 0:128]
    for k in range(1, 4):
        listed = jnp.where(lax.rem(start, 4) == k, both[:, 32 * k : 32 * k + 128], listed)
    listed_ref[...] = jnp.where(listed >= 0, (listed - PER_OWNER * (me - 2)) & 2047, -1)
    source_leaf = iota((160, 128), 0)

    def eight_entries(index, near):
        rows = listed_ref[pl.ds(pl.multiple_of(8 * index, 8), 8), :]
        for k in range(8):
            near = near + jnp.where(rows[k : k + 1, :] == source_leaf, 1.0, 0.0)
        return near

    near = lax.fori_loop(0, 6, eight_entries, jnp.zeros((160, 128), f32))
    relation[...] = near.astype(bf16)
    row8, lane8 = iota((8, 128), 0).astype(f32), iota((8, 128), 1).astype(f32)
    leaf_rows = [
        jnp.where((lane8 == first[t : t + 1] - 3.0 * PER_OWNER + row8) & (row8 < 3.0), 1.0, 0.0)
        for t in range(CPD)
    ]
    wanted_ref[...] = dot_nt(
        jnp.concatenate(leaf_rows, axis=0).astype(bf16), relation[...]
    ).astype(bf16)

    pick_row, pick_lane = iota((SHARE_PAD, WIDE), 0), iota((SHARE_PAD, WIDE), 1)
    pick16 = ((pick_lane == pick_row + SHARE * portion) & (pick_row < SHARE)).astype(f32).astype(bf16)
    slot = iota((SHARE_PAD, 128), 1)
    slot_turn = lax.rem(slot, 6)
    left_first = (slot < 18) & (slot_turn < 3) | (slot == 18)
    left_second = (slot < 18) & (slot_turn >= 3) & (slot_turn < 5) | (slot == 19)
    row32 = iota((32, WIDE), 0)

    def one_own(t, carry):
        rel = comp_ref[REL, pl.ds(t, 1), :]
        px, py, pz = [comp_ref[PX + a, pl.ds(t, 1), :] for a in range(3)]
        lowest = jnp.min(jnp.where(rel >= 0.0, rel, 1e9), axis=1, keepdims=True)
        owner = jnp.floor(lowest * (1.0 / PER_OWNER))
        py4, pz4 = py - 4.0, pz - 4.0
        extra = iota((8, WIDE), 0)
        place = jnp.where(extra == 0, px, jnp.where(extra == 1, py, jnp.where(extra == 2, pz, rel)))
        top, middle, low = thirds(place)
        spot = dot_nt(pick16, top.astype(bf16)) + (
            dot_nt(pick16, middle.astype(bf16)) + dot_nt(pick16, low.astype(bf16))
        )
        for a in range(3):
            spots_ref[t, a] = jnp.broadcast_to(spot[:, a : a + 1], (SHARE_PAD, 128))
        leaf_at = (spot[:, 3:4] - lowest).astype(i32)
        matched = (slot - (FEATURES + 8 * t) == leaf_at) & (leaf_at >= 0) & (leaf_at < 3)
        for w in range(3):
            px4 = px - (4.0 * (owner + float(w - 1)) + 2.0)
            square = (px4 * px4 + py4 * py4) + pz4 * pz4
            rows = jnp.where(
                row32 < 6,
                px4,
                jnp.where(row32 < 12, py4, jnp.where(row32 < 18, pz4, square)),
            )
            rows = jnp.concatenate([rows, jnp.zeros((96, WIDE), f32)], axis=0)
            top, middle, low = thirds(rows)
            value = dot_nt(pick16, top.astype(bf16)) + (
                dot_nt(pick16, middle.astype(bf16)) + dot_nt(pick16, low.astype(bf16))
            )
            top, middle, low = thirds(value)
            chosen = jnp.where(left_first, top, jnp.where(left_second, middle, low))
            chosen = jnp.where((slot >= 21) & (slot < 24), 1.0, chosen)
            chosen = jnp.where(slot >= FEATURES, jnp.where(matched, 1.0, 0.0), chosen)
            lefts_ref[3 * t + w] = chosen[:, 0:DEPTH].astype(bf16)
        return carry

    lax.fori_loop(0, CPD, one_own, 0)
    for a in range(3):
        wide[a] = jnp.broadcast_to(outer_radius * surf_ref[:, a : a + 1], (EQUIV, 128))

    for copy in copies:
        copy.wait()
    for home in range(1, len(OFFSETS) + 1):
        place_cells(home, held_disp[home - 1], held_leaf[home - 1])
    first, last = fill_table(48)
    force[...] = dot_wide(disp[0:144, 0:NPT], stiff_ref[...])
    for a in range(3):
        comp_ref[FX + a, 0:48, 0:NPT] = force[48 * a : 48 * a + 48, :]

    cell = iota((48, 1), 0)
    mine = (jnp.floor(first * (1.0 / PER_OWNER)) == 4.0) & (cell < OWNABLE)
    mine = jnp.where(mine, 1.0, 0.0)
    before = (iota((48, 48), 0) > iota((48, 48), 1)).astype(f32)
    rank = dot(before, jnp.broadcast_to(mine, (48, 128)))
    chosen = jnp.where((rank == iota((48, 128), 1).astype(f32)) & (mine > 0.0), 1.0, 0.0)
    chosen = jnp.concatenate([chosen] * 3, axis=0).astype(bf16)
    for k, part in enumerate((DX, DY, DZ, FX, FY, FZ, REL)):
        pieces = jnp.concatenate(thirds(comp_ref[part]), axis=0).astype(bf16)
        found = lax.dot_general(
            chosen, pieces, (((0,), (0,)), ((), ())), preferred_element_type=f32
        )
        owned_ref[k] = found[0:16]
    total[...] = jnp.zeros_like(total)

    def one_home(home, carry):
        for k in range(3):
            c = 3 * home + k
            d = [owned_ref[a, pl.ds(c, 1), :] for a in range(3)]
            f = [owned_ref[3 + a, pl.ds(c, 1), :] for a in range(3)]
            rel = owned_ref[6, pl.ds(c, 1), :].astype(i32) - 4 * PER_OWNER
            member = (iota((PER_OWNER, WIDE), 0) == rel).astype(f32).astype(bf16)
            member_ref[:, WIDE * k : WIDE * (k + 1)] = member
            for b in range(WIDE // 128):
                lanes = slice(128 * b, 128 * b + 128)
                out = slice(WIDE * k + 128 * b, WIDE * k + 128 * b + 128)
                for g in range(EQUIV // 8):
                    at = slice(8 * g, 8 * g + 8)
                    r = [wide[a, at, :] - d[a][:, lanes] for a in range(3)]
                    fb = [f[a][:, lanes] for a in range(3)]
                    even, along = pull(r, fb)
                    for a in range(3):
                        row = EQUIV * a + 8 * g
                        top, low = halves(even * fb[a] + along * r[a])
                        terms_top[row : row + 8, out] = top
                        terms_low[row : row + 8, out] = low
        total[...] += dot_nt(terms_top[...], member_ref[...]) + dot_nt(terms_low[...], member_ref[...])
        return carry

    lax.fori_loop(0, 3, one_home, 0)
    density[...] = dot_wide(inverse_ref[...], total[...] * inv_eight_pi)
    block_ref[...] = jnp.zeros_like(block_ref)
    for part in range(4):

        @pl.when(portion == part)
        def _():
            for a in range(3):
                rows = density[EQUIV * a + 14 * part : EQUIV * a + 14 * part + 14, :]
                block_ref[0:14, PER_OWNER * a : PER_OWNER * (a + 1)] = rows

    row = core * 4 + y
    own = pltpu.make_async_copy(block_ref, gat_ref.at[row, z], own_sem)
    own.start()
    z_copies = [
        remote(block_ref, gat_ref.at[row, z], z_send.at[k], z_recv.at[k], target)
        for k, target in enumerate(z_targets)
    ]
    for copy in z_copies:
        copy.start()

    low = jnp.floor(first * (1.0 / 16.0))
    high = jnp.floor(last * (1.0 / 16.0))
    lane = iota((48, 128), 1)
    which = iota((48, 1), 0).astype(f32)
    real = (which < float(CELLS)) & (which >= float(CPD))
    flags = []
    for t in range(CPD):
        low_t, high_t = low[t : t + 1], high[t : t + 1]
        flags.append(jnp.where((high >= low_t - 1.0) & (low <= high_t + 1.0) & real, 1.0, 0.0))
    owner = jnp.floor(low * 0.5)
    table = jnp.zeros((48, 128), f32)
    for t, flag in enumerate(flags):
        table = table + jnp.where(lane == t, flag, 0.0)
    rank = dot(before, table)
    count = jnp.sum(table, axis=0, keepdims=True)
    lane_row = iota((1, 128), 1)
    lists_ref[...] = jnp.zeros_like(lists_ref)
    for t, flag in enumerate(flags):
        hit = (rank[:, t : t + 1] == lane.astype(f32)) & (flag > 0.0)
        line = jnp.sum(jnp.where(hit, which, 0.0), axis=0, keepdims=True)
        line = jnp.where(lane_row.astype(f32) >= count[:, t : t + 1], float(DUMMY), line)
        line = jnp.where(lane_row == COUNT, count[:, t : t + 1], line)
        lists_ref[t : t + 1, :] = line.astype(i32)
    square = iota((48, 128), 0) == lane
    line = jnp.sum(jnp.where(square, owner, 0.0), axis=0, keepdims=True)
    lists_ref[7:8, :] = line.astype(i32)

    feature = iota((FEATURES, WIDE), 0)
    turn = lax.rem(feature, 6)
    use_top = (feature < 18) & ((turn == 0) | (turn == 3) | (turn == 5)) | (feature == 21)
    use_middle = (feature < 18) & ((turn == 1) | (turn == 4)) | (feature == 22)

    def factors(x, y, z, last):
        value = jnp.where(
            feature < 6, x, jnp.where(feature < 12, y, jnp.where(feature < 18, z, last))
        )
        top, middle, low = thirds(value)
        return jnp.where(use_top, top, jnp.where(use_middle, middle, low))

    def some_sources(index, carry):
        cells = [BATCH * index + k for k in range(BATCH)]
        rels = [comp_ref[REL, pl.ds(c, 1), :].astype(i32) for c in cells]
        hits = [
            (iota((160, WIDE), 0) == rel - 2 * PER_OWNER).astype(f32).astype(bf16) for rel in rels
        ]
        reaches = [dot(wanted_ref[...], hit) for hit in hits]
        for k, c in enumerate(cells):
            rel = rels[k]
            px = comp_ref[PX, pl.ds(c, 1), :] - (4 * (rel >> 5) + 2).astype(f32)
            py = comp_ref[PY, pl.ds(c, 1), :] - 4.0
            pz = comp_ref[PZ, pl.ds(c, 1), :] - 4.0
            fx, fy, fz = [comp_ref[FX + a, pl.ds(c, 1), :] for a in range(3)]
            square = (px * px + py * py) + (pz * pz + smooth_sq)
            along = (px * fx + py * fy) + pz * fz
            near_rows = factors(-2.0 * px, -2.0 * py, -2.0 * pz, square)
            near_rows = jnp.where((feature >= 18) & (feature < 21), 1.0, near_rows)
            push_rows = factors(fx, fy, fz, -along)
            push_rows = jnp.where((feature >= 18) & (feature < 21), 0.0, push_rows)
            mask_rows = FAR_AWAY - FAR_AWAY * reaches[k]
            rights_ref[c, :, 0:WIDE] = jnp.concatenate([near_rows, mask_rows], axis=0).astype(bf16)
            rights_ref[c, :, WIDE : 2 * WIDE] = jnp.concatenate(
                [push_rows, jnp.zeros((8 * CPD, WIDE), f32)], axis=0
            ).astype(bf16)
        return carry

    owners_ref[...] = jnp.broadcast_to(owner[0:8], (8, 128))

    def multiply_own(t, c, products):
        apart = owners_ref[pl.ds(c, 1), 0:1] - owners_ref[pl.ds(t, 1), 0:1]
        left = [lefts_ref[3 * t + w].astype(f32) for w in range(3)]
        left = jnp.where(apart < -0.5, left[0], jnp.where(apart > 0.5, left[2], left[1]))
        products[...] = dot(left.astype(bf16), rights_ref[c])

    def own_target(t, carry):
        for k in range(CPD // 2):
            multiply_own(t, 2 * k + 1, odd_pairs)
            add_pair(comp_ref, sums_ref, t, 2 * k, even_pairs)
            if k + 1 < CPD // 2:
                multiply_own(t, 2 * k + 2, even_pairs)
            else:
                multiply_own(jnp.minimum(t + 1, CPD - 1), 0, even_pairs)
            add_pair(comp_ref, sums_ref, t, 2 * k + 1, odd_pairs)
        return carry

    sums_ref[...] = jnp.zeros_like(sums_ref)
    rights_ref[DUMMY] = jnp.where(iota((DEPTH, 2 * WIDE), 0) == 21, FAR_AWAY, 0.0).astype(bf16)
    lax.fori_loop(0, EARLY, some_sources, 0)

    own.wait()
    y_copies, c_copies = [], []

    def pass_on(at, where, index):
        place = gat_ref.at[at, where]
        copy = remote(place, place, c_send.at[index], c_recv.at[index], c_target)
        copy.start()
        c_copies.append(copy)

    for order, k in enumerate((0, 1, 7, 2, 6, 3, 5, 4)):
        where = lax.rem(z - k + 8, 8)
        if k:
            z_copies[k - 1].wait_recv()
        place = gat_ref.at[row, where]
        for side, target in enumerate(y_targets):
            index = 3 * order + side
            copy = remote(place, place, y_send.at[index], y_recv.at[index], target)
            copy.start()
            y_copies.append(copy)
        pass_on(row, where, order)
    lax.fori_loop(EARLY, CELLS // BATCH, some_sources, 0)
    multiply_own(0, 0, even_pairs)
    lax.fori_loop(0, MIDDLE, own_target, 0)
    for order, k in enumerate((0, 1, 7, 2, 6, 3, 5, 4)):
        where = lax.rem(z - k + 8, 8)
        for side in range(3):
            index = 3 * order + side
            y_copies[index].wait_recv()
            pass_on(core * 4 + lax.rem(y - side + 3, 4), where, 8 + index)
    lax.fori_loop(MIDDLE, CPD, own_target, 0)
    for copy in (*z_copies, *y_copies):
        copy.wait_send()
    for copy in c_copies:
        copy.wait()


def first(displacement, point_leaf, near_list, stiffness, surf, up_inverse):
    npoints = displacement.shape[1]
    sides = len(OFFSETS)
    dma = pltpu.SemaphoreType.DMA
    return pl.pallas_call(
        first_kernel,
        out_shape=(
            jax.ShapeDtypeStruct((10, 48, WIDE), f32),
            jax.ShapeDtypeStruct((8, 128), i32),
            jax.ShapeDtypeStruct((8, 8, 16, 128), f32),
            jax.ShapeDtypeStruct((3 * CPD, SHARE_PAD, DEPTH), bf16),
            jax.ShapeDtypeStruct((CPD, 3, SHARE_PAD, 128), f32),
            jax.ShapeDtypeStruct((CELLS + 1, DEPTH, 2 * WIDE), bf16),
            jax.ShapeDtypeStruct((CPD, 4, SHARE_PAD, 128), f32),
        ),
        in_specs=[HBM] * 6,
        out_specs=(VMEM,) * 7,
        scratch_shapes=[
            pltpu.VMEM((sides, 3, npoints), f32),
            pltpu.VMEM((sides, 1, npoints), i32),
            pltpu.VMEM((3, npoints), f32),
            pltpu.VMEM((EQUIV, 8), f32),
            pltpu.VMEM((1, npoints), i32),
            pltpu.VMEM((2, FAR, 128), i32),
            pltpu.VMEM((NPT, NPT), f32),
            pltpu.VMEM((ROWS, ROWS), f32),
            pltpu.VMEM((144, WIDE), f32),
            pltpu.VMEM((48, WIDE), i32),
            pltpu.VMEM((144, NPT), f32),
            pltpu.VMEM((FAR, 128), i32),
            pltpu.VMEM((160, 128), bf16),
            pltpu.VMEM((8 * CPD, 160), bf16),
            pltpu.VMEM((3, EQUIV, 128), f32),
            pltpu.VMEM((7, 16, WIDE), f32),
            pltpu.VMEM((ROWS, 3 * WIDE), bf16),
            pltpu.VMEM((ROWS, 3 * WIDE), bf16),
            pltpu.VMEM((PER_OWNER, 3 * WIDE), bf16),
            pltpu.VMEM((ROWS, PER_OWNER), f32),
            pltpu.VMEM((ROWS, PER_OWNER), f32),
            pltpu.VMEM((16, 128), f32),
            pltpu.VMEM((SHARE_PAD, 2 * WIDE), f32),
            pltpu.VMEM((SHARE_PAD, 2 * WIDE), f32),
            pltpu.VMEM((8, 128), f32),
            dma((sides,)),
            dma((sides,)),
            dma((sides,)),
            dma((sides,)),
            dma((7,)),
            dma,
            dma((7,)),
            dma((7,)),
            dma((24,)),
            dma((24,)),
            dma((32,)),
            dma((32,)),
        ],
        compiler_params=pltpu.CompilerParams(
            collective_id=0, has_side_effects=True, vmem_limit_bytes=LIMIT
        ),
        name="first",
    )(*(in_hbm(x) for x in (displacement, point_leaf, near_list, stiffness, surf, up_inverse)))


def near_kernel(lists, comp_ref, lefts, spots, rights, own_sums, out_ref, even_pairs, odd_pairs, sums):
    portion = lax.axis_index("leaf")

    def multiply(t, index, products):
        c = lists[t, index]
        w = jnp.clip(lists[7, c] - lists[7, t] + 1, 0, 2)
        products[...] = dot(lefts[3 * t + w], rights[c])

    sums[...] = own_sums[...]
    multiply(0, 0, even_pairs)

    def one_target(t, carry):
        steps = jnp.maximum((lists[t, COUNT] + 1) // 2, 1)

        def two_pairs(index, carry):
            multiply(t, 2 * index + 1, odd_pairs)
            add_pair(comp_ref, sums, t, lists[t, 2 * index], even_pairs)
            ends = index + 1 == steps
            after = jnp.where(ends, jnp.minimum(t + 1, CPD - 1), t)
            multiply(after, jnp.where(ends, 0, 2 * index + 2), even_pairs)
            add_pair(comp_ref, sums, t, lists[t, 2 * index + 1], odd_pairs)
            return carry

        lax.fori_loop(0, steps, two_pairs, 0)
        return carry

    lax.fori_loop(0, CPD, one_target, 0)
    pick_row, pick_lane = iota((SHARE_PAD, WIDE), 0), iota((SHARE_PAD, WIDE), 1)
    pick = (pick_lane == pick_row + SHARE * portion) & (pick_row < SHARE)

    def finish(index, carry):
        for t in (2 * index, 2 * index + 1):
            for a in range(3):
                total = sums[t, a] + spots[t, a] * sums[t, 3]
                column = jnp.sum(total, axis=1, keepdims=True) * inv_eight_pi
                row = jnp.sum(jnp.where(pick, column, 0.0), axis=0, keepdims=True)
                out_ref[a, pl.ds(t, 1), :] = row
        return carry

    lax.fori_loop(0, CPD // 2, finish, 0)


def near_field(lists, comp, lefts, spots, rights, own_sums):
    return pl.pallas_call(
        near_kernel,
        out_shape=jax.ShapeDtypeStruct((3, 8, WIDE), f32),
        in_specs=[SMEM] + [VMEM] * 5,
        out_specs=VMEM,
        scratch_shapes=[
            pltpu.VMEM((SHARE_PAD, 2 * WIDE), f32),
            pltpu.VMEM((SHARE_PAD, 2 * WIDE), f32),
            pltpu.VMEM((CPD, 4, SHARE_PAD, 128), f32),
        ],
        compiler_params=pltpu.CompilerParams(vmem_limit_bytes=LIMIT),
        name="near_field",
    )(lists, comp, lefts, spots, rights, own_sums)


def far_part(
    left_ref,
    quarter_ref,
    points,
    gat_ref,
    far_ref,
    far_load,
    surf_ref,
    inverse_ref,
    local_ref,
    far4,
    sources,
    packed,
    pushes,
    mids,
    total,
    quarter,
    even_rows,
    odd_rows,
    even_blocks,
    odd_blocks,
):
    me = lax.axis_index("cells")
    portion = lax.axis_index("leaf")
    lane = iota((16, 128), 1)

    def one_tile(tile, carry):
        for half in range(2):
            rows = [jnp.zeros((16, 128), f32) for _ in range(3)]
            for v in range(4):
                at = 8 * tile + 4 * half + v
                value = gat_ref[at // 8, at - at // 8 * 8]
                for a in range(3):
                    shift = (PER_OWNER * (v - a)) % 128
                    moved = pltpu.roll(value, shift, 1) if shift else value
                    rows[a] = jnp.where(lane // PER_OWNER == v, moved, rows[a])
            top, low = halves(jnp.concatenate(rows, axis=0))
            packed[tile, 0:48, 128 * half : 128 * half + 128] = top
            packed[tile, 48:96, 128 * half : 128 * half + 128] = low
        return carry

    lax.fori_loop(0, 8, one_tile, 0)

    far_load.wait()
    entries = far_ref[...]
    mine = lax.rem(me, 4)
    lane48 = iota((FAR, 128), 1) // PER_OWNER
    picked = jnp.zeros((FAR, 128), i32)
    for place in range(4):
        moved = entries
        for k in range(1, 4):
            turned = pltpu.roll(entries, PER_OWNER * k, 1)
            moved = jnp.where(lax.rem(mine + k, 4) == place, turned, moved)
        far4[place] = moved
    for place in range(4):
        rows = far4[place, pl.ds(place, FAR // 4, stride=4), :]
        chosen = iota((FAR // 4, 128), 1) // PER_OWNER == place
        if place == 0:
            merged = rows
        else:
            merged = jnp.where(chosen, rows, merged)
    owner = merged >> 5
    spot = (((owner & 1) << 5) + (owner >> 1)) * PER_OWNER + (merged & 31)
    sources[0:12, :] = jnp.where(merged >= 0, spot, -1)
    target = me * PER_OWNER + (iota((12, 128), 1) & 31)
    mids[0, 0:12, :] = (2 * ((target >> 4) - (merged >> 4))).astype(f32)
    mids[1, 0:12, :] = (2 * (((target >> 2) & 3) - ((merged >> 2) & 3))).astype(f32)
    mids[2, 0:12, :] = (2 * ((target & 3) - (merged & 3))).astype(f32)

    def one_gather(index, carry):
        first = sources[pl.ds(2 * index, 1), :]
        second = sources[pl.ds(2 * index + 1, 1), :]
        wanted = jnp.concatenate([first, second], axis=1)
        found = jnp.zeros((96, 256), f32)
        for tile in range(8):
            onehot = (iota((256, 256), 0) + 256 * tile == wanted).astype(f32).astype(bf16)
            found = found + dot(packed[tile], onehot)
        value = found[0:48] + found[48:96]
        pushes[2 * index] = value[:, 0:128]
        pushes[2 * index + 1] = value[:, 128:256]
        return carry

    lax.fori_loop(0, 6, one_gather, 0)
    total[...] = jnp.zeros_like(total)

    left = left_ref[...].astype(bf16)
    for a in range(3):
        quarter[a] = jnp.broadcast_to(quarter_ref[portion, :, a : a + 1], (16, 128))
    steps = thirds(jnp.full((16, 128), (inner_radius / 3.0) ** 2, f32))
    for rows in (even_rows, odd_rows):
        rows[...] = jnp.zeros_like(rows)
        for k in range(3):
            rows[pl.ds(12 + k, 16, stride=32), :] = steps[k]

    def prepare_block(index, rows, blocks):
        push = [pushes[index, 16 * a : 16 * a + 16, :] for a in range(3)]
        gap = [mids[a, pl.ds(index, 1), :] - quarter[a] for a in range(3)]
        square = (gap[0] * gap[0] + gap[1] * gap[1]) + (gap[2] * gap[2] + smooth_sq)
        inner = (gap[0] * push[0] + gap[1] * push[1]) + gap[2] * push[2]
        scale = inner_radius / 3.0
        for a in range(3):
            for k, third in enumerate(thirds((2.0 * scale) * gap[a])):
                rows[pl.ds(3 * a + k, 16, stride=32), :] = third
            for k, third in enumerate(thirds(scale * push[a])):
                rows[pl.ds(16 + 3 * a + k, 16, stride=32), :] = third
        for k, third in enumerate(thirds(square)):
            rows[pl.ds(9 + k, 16, stride=32), :] = third
        for k, third in enumerate(thirds(inner)):
            rows[pl.ds(25 + k, 16, stride=32), :] = third
        for j in range(14):
            right = jnp.concatenate(
                [rows[32 * j : 32 * j + 16, :], rows[32 * j + 16 : 32 * j + 32, :]], axis=1
            )
            blocks[j] = dot(left, right.astype(bf16))

    def add_block(index, blocks):
        groups = EQUIV // 8
        sums = [[jnp.zeros((8, 128), f32) for _ in range(4)] for _ in range(groups)]
        for j in range(14):
            f = [pushes[index, 16 * a + j : 16 * a + j + 1, :] for a in range(3)]
            shift = [points[3 * (14 * portion + j) + a] for a in range(3)]
            for g in range(groups):
                at = slice(8 * g, 8 * g + 8)
                shifted = blocks[j, at, 0:128]
                inner = blocks[j, at, 128:256]
                root = lax.rsqrt(shifted)
                cube = root * root * root
                even = root + smooth_sq * cube
                along = cube * inner
                for a in range(3):
                    sums[g][a] = sums[g][a] + (even * f[a] - along * shift[a])
                sums[g][3] = sums[g][3] + along
        mid = [mids[a, pl.ds(index, 1), :] for a in range(3)]
        for g in range(groups):
            at = slice(8 * g, 8 * g + 8)
            for a in range(3):
                check = mid[a] + inner_radius * surf_ref[at, a : a + 1]
                row = EQUIV * a + 8 * g
                total[row : row + 8, :] += sums[g][a] + check * sums[g][3]

    prepare_block(0, even_rows, even_blocks)

    def two_blocks(index, carry):
        prepare_block(2 * index + 1, odd_rows, odd_blocks)
        add_block(2 * index, even_blocks)
        prepare_block(jnp.minimum(2 * index + 2, 11), even_rows, even_blocks)
        add_block(2 * index + 1, odd_blocks)
        return carry

    lax.fori_loop(0, 6, two_blocks, 0)
    value = total[...] * inv_eight_pi
    value = value + pltpu.roll(value, 64, 1)
    value = value + pltpu.roll(value, 32, 1)
    local_ref[...] = dot_wide(inverse_ref[...], value)


def last_kernel(
    points,
    left_ref,
    quarter_ref,
    gat_ref,
    far_hbm,
    surf_ref,
    inverse_ref,
    comp_ref,
    near_ref,
    out_ref,
    far_ref,
    load_sem,
    far4,
    sources,
    packed,
    pushes,
    mids,
    total,
    quarter,
    even_rows,
    odd_rows,
    even_blocks,
    odd_blocks,
    local_ref,
    packed_local,
    held_local,
    factors,
    spread_ref,
    cell_ref,
    part_ref,
    held_part,
    send_local,
    recv_local,
    send_part,
    recv_part,
):
    block = pl.multiple_of(lax.axis_index("cells") // 4 * 128, 128)
    far_load = pltpu.make_async_copy(far_hbm.at[:, pl.ds(block, 128)], far_ref, load_sem)
    far_load.start()
    packed_local[...] = jnp.zeros_like(packed_local)
    sides = beside("cells", (1, -1))
    mates = beside("leaf", (1, 2, 3))
    barrier = pltpu.get_barrier_semaphore()
    for target in (*sides, *mates):
        pl.semaphore_signal(barrier, inc=1, device_id=target, device_id_type=MESH)
    far_part(
        left_ref,
        quarter_ref,
        points,
        gat_ref,
        far_ref,
        far_load,
        surf_ref,
        inverse_ref,
        local_ref,
        far4,
        sources,
        packed,
        pushes,
        mids,
        total,
        quarter,
        even_rows,
        odd_rows,
        even_blocks,
        odd_blocks,
    )
    pl.semaphore_wait(barrier, 5)
    lane = iota((48, 128), 1) // PER_OWNER
    for k in range(4):
        rows = min(48, ROWS - 48 * k)
        piece = local_ref[48 * k : 48 * k + rows, :]
        here = lane[0:rows] == k
        packed_local[0:rows, :] = jnp.where(here, piece, packed_local[0:rows, :])
    copies = [
        remote(packed_local, held_local.at[k], send_local.at[k], recv_local.at[k], target)
        for k, target in enumerate(sides)
    ]
    for copy in copies:
        copy.start()
    for copy in copies:
        copy.wait()
    lane = iota((48, 128), 1) // PER_OWNER
    for k in range(4):
        rows = min(48, ROWS - 48 * k)
        value = local_ref[48 * k : 48 * k + rows, :]
        for side in range(2):
            place = 2 * side
            moved = held_local[side, 0:rows, :]
            if place != k:
                moved = pltpu.roll(moved, (PER_OWNER * (place - k)) % 128, 1)
            value = jnp.where(lane[0:rows] == place, moved, value)
        top, low = halves(value)
        factors[48 * k : 48 * k + rows, 0:128] = top
        factors[48 * k : 48 * k + rows, 128:256] = low

    def spread_out(t):
        rel = comp_ref[REL, pl.ds(t, 1), :].astype(i32) - 3 * PER_OWNER
        member = (iota((128, WIDE), 0) == rel).astype(f32).astype(bf16)
        spread_ref[t] = dot(factors[...], jnp.concatenate([member, member], axis=0))

    def three_cells(index, carry):
        for k in range(3):
            spread_out(3 * index + k)
        return carry

    lax.fori_loop(0, 2, three_cells, 0)

    def one_cell(t, carry):
        d = [comp_ref[DX + a, pl.ds(t, 1), :] for a in range(3)]
        sums = [jnp.zeros((8, WIDE), f32) for _ in range(3)]
        for g in range(EQUIV // 8):
            at = slice(8 * g, 8 * g + 8)
            r = [d[a] - outer_radius * surf_ref[at, a : a + 1] for a in range(3)]
            f = [spread_ref[t, EQUIV * a + 8 * g : EQUIV * a + 8 * g + 8, :] for a in range(3)]
            even, along = pull(r, f)
            sums = [sums[a] + (even * f[a] + along * r[a]) for a in range(3)]
        for a in range(3):
            row = jnp.sum(sums[a], axis=0, keepdims=True) * inv_eight_pi
            cell_ref[a, pl.ds(t, 1), :] = row + near_ref[a, pl.ds(t, 1), :]
        return carry

    lax.fori_loop(0, CPD, one_cell, 0)
    for t in range(CPD):
        for a in range(3):
            part_ref[a : a + 1, NPT * t : NPT * (t + 1)] = cell_ref[a, t : t + 1, 0:NPT]
    copies = [
        remote(part_ref, held_part.at[k], send_part.at[k], recv_part.at[k], target)
        for k, target in enumerate(mates)
    ]
    for copy in copies:
        copy.start()
    for copy in copies:
        copy.wait()
    out_ref[...] = (part_ref[...] + held_part[1]) + (held_part[0] + held_part[2])


def last(points, left, quarter, gathered, far_list, surf, down_inverse, comp, near, npoints):
    dma = pltpu.SemaphoreType.DMA
    return pl.pallas_call(
        last_kernel,
        out_shape=jax.ShapeDtypeStruct((3, npoints), f32),
        in_specs=[SMEM, VMEM, VMEM, VMEM, HBM] + [VMEM] * 4,
        out_specs=VMEM,
        scratch_shapes=[
            pltpu.VMEM((FAR, 128), i32),
            dma,
            pltpu.VMEM((4, FAR, 128), i32),
            pltpu.VMEM((16, 128), i32),
            pltpu.VMEM((8, 96, 256), bf16),
            pltpu.VMEM((12, FAR, 128), f32),
            pltpu.VMEM((3, 16, 128), f32),
            pltpu.VMEM((ROWS, 128), f32),
            pltpu.VMEM((3, 16, 128), f32),
            pltpu.VMEM((512, 128), f32),
            pltpu.VMEM((512, 128), f32),
            pltpu.VMEM((14, EQUIV, 256), f32),
            pltpu.VMEM((14, EQUIV, 256), f32),
            pltpu.VMEM((ROWS, 128), f32),
            pltpu.VMEM((48, 128), f32),
            pltpu.VMEM((2, 48, 128), f32),
            pltpu.VMEM((ROWS, 256), bf16),
            pltpu.VMEM((CPD, ROWS, WIDE), f32),
            pltpu.VMEM((3, 8, WIDE), f32),
            pltpu.VMEM((3, npoints), f32),
            pltpu.VMEM((3, 3, npoints), f32),
            dma((2,)),
            dma((2,)),
            dma((3,)),
            dma((3,)),
        ],
        compiler_params=pltpu.CompilerParams(
            collective_id=1, has_side_effects=True, vmem_limit_bytes=LIMIT
        ),
        name="last",
    )(points, left, quarter, gathered, in_hbm(far_list), surf, down_inverse, comp, near)


def body(displacement, point_leaf, near_list, far_list, stiffness, up_inverse, down_inverse):
    table = surface_table()
    surf = jnp.asarray(np.pad(table, ((0, 0), (0, 5))))
    points = jnp.asarray((inner_radius * table).astype(np.float32).reshape(-1))
    whole = np.round(3.0 * table)
    ones = np.ones((EQUIV, 3), np.float32)
    square = np.sum(whole * whole, axis=1, keepdims=True)
    left = np.concatenate([np.repeat(whole, 3, axis=1), ones, ones * square, 0.0 * square], axis=1)
    left = jnp.asarray(left.astype(np.float32))
    quarter = inner_radius * table.reshape(4, 14, 3)
    quarter = jnp.asarray(np.pad(quarter, ((0, 0), (0, 2), (0, 5))).astype(np.float32))
    comp, lists, gathered, lefts, spots, rights, own_sums = first(
        displacement, point_leaf, near_list, stiffness, surf, up_inverse
    )
    near = near_field(lists, comp, lefts, spots, rights, own_sums)
    return last(
        points, left, quarter, gathered, far_list, surf, down_inverse, comp, near, displacement.shape[1]
    )


def solution(mesh):
    in_specs = (P(None, "cells"), P("cells"), P(), P(), P(), P(), P())
    out_specs = P(None, "cells")
    return jax.shard_map(body, mesh=mesh, in_specs=in_specs, out_specs=out_specs, check_vma=False)
```

```python
import math

import jax
import jax.numpy as jnp
import numpy as np
from jax import lax
from jax.experimental import pallas as pl
from jax.experimental.pallas import tpu as pltpu
from jax.sharding import PartitionSpec as P

NPT = 312
CPD = 6
SLICE = 16
EQUIV = 56
FAR = 48
ROWS = 3 * EQUIV
PER_OWNER = 2 * SLICE
WIDE = 384
OFFSETS = (1, -1, 2, -2, 3, -3)
CELLS = CPD * (len(OFFSETS) + 1)
OWNABLE = 3 * CPD
SHARE = NPT // 4
SHARE_PAD = 80

inv_eight_pi = 1.0 / (8.0 * math.pi)
smooth_sq = 0.0625
inner_radius = 1.05
outer_radius = 2.95
MESH = pl.DeviceIdType.MESH
VMEM = pl.BlockSpec(memory_space=pltpu.VMEM)
SMEM = pl.BlockSpec(memory_space=pltpu.SMEM)
f32 = jnp.float32
bf16 = jnp.bfloat16
i32 = jnp.int32


def surface_table():
    ladder = [-1.0, -1.0 / 3.0, 1.0 / 3.0, 1.0]
    corners = [
        (a, b, c)
        for a in ladder
        for b in ladder
        for c in ladder
        if max(abs(a), abs(b), abs(c)) == 1.0
    ]
    return np.array(corners, dtype=np.float32)


def iota(shape, dim):
    return lax.broadcasted_iota(i32, shape, dim)


def dot(a, b):
    return jnp.dot(a, b, preferred_element_type=f32)


def dot_nt(a, b):
    return lax.dot_general(a, b, (((1,), (1,)), ((), ())), preferred_element_type=f32)


def halves(value):
    top = value.astype(bf16)
    return top, (value - top.astype(f32)).astype(bf16)


def dot_wide(a, b):
    a_top, a_low = halves(a)
    b_top, b_low = halves(b)
    return dot(a_top, b_top) + (dot(a_top, b_low) + dot(a_low, b_top))


DX, DY, DZ, FX, FY, FZ, PX, PY, PZ, REL = range(10)
FEATURES = 24
DEPTH = FEATURES + 8 * CPD
FAR_AWAY = 1e30
LIMIT = 20 << 20
HBM = pl.BlockSpec(memory_space=pltpu.HBM)
DUMMY = CELLS
TOGETHER = 4
BATCH = 6
PARTS = 2
EARLY = 5
MIDDLE = 3


def thirds(value):
    top = value.astype(bf16).astype(f32)
    rest = value - top
    middle = rest.astype(bf16).astype(f32)
    return top, middle, rest - middle


def pull(offset, strength):
    dx, dy, dz = offset
    fx, fy, fz = strength
    shifted = (dx * dx + dy * dy) + (dz * dz + smooth_sq)
    inner = (dx * fx + dy * fy) + dz * fz
    root = lax.rsqrt(shifted)
    cube = root * root * root
    return root + smooth_sq * cube, cube * inner


def in_hbm(array):
    return pltpu.with_memory_space_constraint(array, pltpu.HBM)


def remote(src, dst, send_sem, recv_sem, target):
    return pltpu.make_async_remote_copy(
        src_ref=src,
        dst_ref=dst,
        send_sem=send_sem,
        recv_sem=recv_sem,
        device_id=target,
        device_id_type=MESH,
    )


def greet(targets):
    barrier = pltpu.get_barrier_semaphore()
    for target in targets:
        pl.semaphore_signal(barrier, inc=1, device_id=target, device_id_type=MESH)
    pl.semaphore_wait(barrier, len(targets))


def beside(axis, offsets):
    count = lax.axis_size(axis)
    me = lax.axis_index(axis)
    return [{axis: lax.rem(me + (off + count), count)} for off in offsets]


def add_pair(comp_ref, sums, t, c, products):
    p = [comp_ref[PX + a, pl.ds(c, 1), :] for a in range(3)]
    f = [comp_ref[FX + a, pl.ds(c, 1), :] for a in range(3)]
    for part in range(PARTS):
        groups = range(part * 10 // PARTS, (part + 1) * 10 // PARTS)
        added = {}
        for b in range(WIDE // 128):
            lanes = slice(128 * b, 128 * b + 128)
            pb = [value[:, lanes] for value in p]
            fb = [value[:, lanes] for value in f]
            for g in groups:
                at = slice(8 * g, 8 * g + 8)
                shifted = products[at, lanes]
                inner = products[at, WIDE + 128 * b : WIDE + 128 * b + 128]
                root = lax.rsqrt(shifted)
                cube = root * root * root
                even = root + smooth_sq * cube
                along = cube * inner
                one = [even * fb[a] - along * pb[a] for a in range(3)] + [along]
                added[g] = [u + v for u, v in zip(added[g], one)] if b else one
        for g in groups:
            at = slice(8 * g, 8 * g + 8)
            for a in range(4):
                sums[t, a, at, :] += added[g][a]


def first_kernel(
    disp_hbm,
    leaf_hbm,
    near_hbm,
    stiff_hbm,
    surf_hbm,
    inverse_hbm,
    comp_ref,
    lists_ref,
    gat_ref,
    lefts_ref,
    spots_ref,
    rights_ref,
    sums_ref,
    held_disp,
    held_leaf,
    disp_ref,
    surf_ref,
    leaf_ref,
    near_ref,
    stiff_ref,
    inverse_ref,
    disp,
    leaves,
    force,
    listed_ref,
    relation,
    wanted_ref,
    wide,
    owned_ref,
    terms_top,
    terms_low,
    member_ref,
    total,
    density,
    block_ref,
    even_pairs,
    odd_pairs,
    owners_ref,
    send_disp,
    recv_disp,
    send_leaf,
    recv_leaf,
    load_sem,
    own_sem,
    z_send,
    z_recv,
    y_send,
    y_recv,
    c_send,
    c_recv,
):
    me = lax.axis_index("cells")
    portion = lax.axis_index("leaf")
    start = lax.rem(me + 63, 64)
    block = start // 4
    leaf_load = pltpu.make_async_copy(leaf_hbm, leaf_ref.at[0], load_sem.at[0])
    loads = [
        pltpu.make_async_copy(
            near_hbm.at[:, pl.ds(pl.multiple_of(lax.rem(block + k, 16) * 128, 128), 128)],
            near_ref.at[k],
            load_sem.at[1 + k],
        )
        for k in range(2)
    ]
    loads.append(pltpu.make_async_copy(stiff_hbm, stiff_ref, load_sem.at[3]))
    loads.append(pltpu.make_async_copy(inverse_hbm, inverse_ref, load_sem.at[4]))
    loads.append(pltpu.make_async_copy(surf_hbm, surf_ref, load_sem.at[5]))
    disp_load = pltpu.make_async_copy(disp_hbm, disp_ref, load_sem.at[6])
    disp_load.start()
    leaf_load.start()
    for load in loads:
        load.start()
    core = lax.rem(me, 2)
    z = lax.rem(me // 2, 8)
    y = me // 16

    def device(y_at, z_at, core_at):
        return {"cells": (y_at * 8 + z_at) * 2 + core_at}

    sides = beside("cells", OFFSETS)
    z_targets = [device(y, lax.rem(z + k, 8), core) for k in range(1, 8)]
    y_targets = [device(lax.rem(y + k, 4), z, core) for k in range(1, 4)]
    c_target = device(y, z, 1 - core)
    greet([*sides, *z_targets, *y_targets, c_target])
    disp_load.wait()
    leaf_load.wait()
    copies = []
    for slot, target in enumerate(sides):
        copies.append(
            remote(disp_ref, held_disp.at[slot], send_disp.at[slot], recv_disp.at[slot], target)
        )
        copies.append(
            remote(leaf_ref, held_leaf.at[slot], send_leaf.at[slot], recv_leaf.at[slot], target)
        )
    for copy in copies:
        copy.start()

    comp_ref[...] = jnp.zeros_like(comp_ref)
    disp[...] = jnp.zeros_like(disp)
    leaves[...] = jnp.zeros_like(leaves)

    def place_cells(home, points, leaf_row):
        for k in range(CPD):
            at = slice(NPT * k, NPT * (k + 1))
            row = home * CPD + k
            for a in range(3):
                disp[48 * a + row : 48 * a + row + 1, 0:NPT] = points[a : a + 1, at]
            leaves[row : row + 1, 0:NPT] = leaf_row[:, at]

    def fill_table(rows):
        live = iota((rows, WIDE), 1) < NPT
        rel = jnp.where(live, (leaves[0:rows, :] - PER_OWNER * (me - 4)) & 2047, -1)
        for a in range(3):
            comp_ref[DX + a, 0:rows, :] = disp[48 * a : 48 * a + rows, :]
        comp_ref[REL, 0:rows, :] = rel.astype(f32)
        comp_ref[PX, 0:rows, :] = comp_ref[DX, 0:rows, :] + (2 * (rel >> 4) + 1).astype(f32)
        comp_ref[PY, 0:rows, :] = comp_ref[DY, 0:rows, :] + (2 * ((rel >> 2) & 3) + 1).astype(f32)
        comp_ref[PZ, 0:rows, :] = comp_ref[DZ, 0:rows, :] + (2 * (rel & 3) + 1).astype(f32)
        relf = rel.astype(f32)
        first = jnp.min(jnp.where(live, relf, 1e9), axis=1, keepdims=True)
        last = jnp.max(relf, axis=1, keepdims=True)
        return first, last

    place_cells(0, disp_ref[...], leaf_ref[...])
    first, last = fill_table(8)

    for load in loads:
        load.wait()
    both = jnp.concatenate([near_ref[0], near_ref[1]], axis=1)
    listed = both[:, 0:128]
    for k in range(1, 4):
        listed = jnp.where(lax.rem(start, 4) == k, both[:, 32 * k : 32 * k + 128], listed)
    listed_ref[...] = jnp.where(listed >= 0, (listed - PER_OWNER * (me - 2)) & 2047, -1)
    source_leaf = iota((160, 128), 0)

    def eight_entries(index, near):
        rows = listed_ref[pl.ds(pl.multiple_of(8 * index, 8), 8), :]
        for k in range(8):
            near = near + jnp.where(rows[k : k + 1, :] == source_leaf, 1.0, 0.0)
        return near

    near = lax.fori_loop(0, 6, eight_entries, jnp.zeros((160, 128), f32))
    relation[...] = near.astype(bf16)
    row8, lane8 = iota((8, 128), 0).astype(f32), iota((8, 128), 1).astype(f32)
    leaf_rows = [
        jnp.where((lane8 == first[t : t + 1] - 3.0 * PER_OWNER + row8) & (row8 < 3.0), 1.0, 0.0)
        for t in range(CPD)
    ]
    wanted_ref[...] = dot_nt(
        jnp.concatenate(leaf_rows, axis=0).astype(bf16), relation[...]
    ).astype(bf16)

    pick_row, pick_lane = iota((SHARE_PAD, WIDE), 0), iota((SHARE_PAD, WIDE), 1)
    pick16 = ((pick_lane == pick_row + SHARE * portion) & (pick_row < SHARE)).astype(f32).astype(bf16)
    slot = iota((SHARE_PAD, 128), 1)
    slot_turn = lax.rem(slot, 6)
    left_first = (slot < 18) & (slot_turn < 3) | (slot == 18)
    left_second = (slot < 18) & (slot_turn >= 3) & (slot_turn < 5) | (slot == 19)
    row32 = iota((32, WIDE), 0)

    def one_own(t):
        rel = comp_ref[REL, pl.ds(t, 1), :]
        px, py, pz = [comp_ref[PX + a, pl.ds(t, 1), :] for a in range(3)]
        lowest = jnp.min(jnp.where(rel >= 0.0, rel, 1e9), axis=1, keepdims=True)
        owner = jnp.floor(lowest * (1.0 / PER_OWNER))
        py4, pz4 = py - 4.0, pz - 4.0
        rows = []
        for w in range(3):
            px4 = px - (4.0 * (owner + float(w - 1)) + 2.0)
            square = (px4 * px4 + py4 * py4) + pz4 * pz4
            rows.append(
                jnp.where(
                    row32 < 6,
                    px4,
                    jnp.where(row32 < 12, py4, jnp.where(row32 < 18, pz4, square)),
                )
            )
        place = jnp.where(row32 == 0, px, jnp.where(row32 == 1, py, jnp.where(row32 == 2, pz, rel)))
        top, middle, low = thirds(jnp.concatenate([*rows, place], axis=0))
        found = dot_nt(pick16, top.astype(bf16)) + (
            dot_nt(pick16, middle.astype(bf16)) + dot_nt(pick16, low.astype(bf16))
        )
        for a in range(3):
            spots_ref[t, a] = jnp.broadcast_to(found[:, 96 + a : 97 + a], (SHARE_PAD, 128))
        leaf_at = (found[:, 99:100] - lowest).astype(i32)
        matched = (slot - (FEATURES + 8 * t) == leaf_at) & (leaf_at >= 0) & (leaf_at < 3)
        for w in range(3):
            value = pltpu.roll(found, 128 - 32 * w, 1) if w else found
            top, middle, low = thirds(value)
            chosen = jnp.where(left_first, top, jnp.where(left_second, middle, low))
            chosen = jnp.where((slot >= 21) & (slot < 24), 1.0, chosen)
            chosen = jnp.where(slot >= FEATURES, jnp.where(matched, 1.0, 0.0), chosen)
            lefts_ref[3 * t + w] = chosen[:, 0:DEPTH].astype(bf16)

    def two_own(index, carry):
        one_own(2 * index)
        one_own(2 * index + 1)
        return carry

    lax.fori_loop(0, CPD // 2, two_own, 0)
    for a in range(3):
        wide[a] = jnp.broadcast_to(outer_radius * surf_ref[:, a : a + 1], (EQUIV, 128))

    for copy in copies:
        copy.wait()
    for home in range(1, len(OFFSETS) + 1):
        place_cells(home, held_disp[home - 1], held_leaf[home - 1])
    first, last = fill_table(48)
    force[...] = dot_wide(disp[0:144, 0:NPT], stiff_ref[...])
    for a in range(3):
        comp_ref[FX + a, 0:48, 0:NPT] = force[48 * a : 48 * a + 48, :]

    cell = iota((48, 1), 0)
    mine = (jnp.floor(first * (1.0 / PER_OWNER)) == 4.0) & (cell < OWNABLE)
    mine = jnp.where(mine, 1.0, 0.0)
    before = (iota((48, 48), 0) > iota((48, 48), 1)).astype(f32)
    rank = dot(before, jnp.broadcast_to(mine, (48, 128)))
    chosen = jnp.where((rank == iota((48, 128), 1).astype(f32)) & (mine > 0.0), 1.0, 0.0)
    chosen = jnp.concatenate([chosen] * 3, axis=0).astype(bf16)
    for k, part in enumerate((DX, DY, DZ, FX, FY, FZ, REL)):
        pieces = jnp.concatenate(thirds(comp_ref[part]), axis=0).astype(bf16)
        found = lax.dot_general(
            chosen, pieces, (((0,), (0,)), ((), ())), preferred_element_type=f32
        )
        owned_ref[k] = found[0:16]
    total[...] = jnp.zeros_like(total)

    def one_home(home, carry):
        for k in range(3):
            c = 3 * home + k
            d = [owned_ref[a, pl.ds(c, 1), :] for a in range(3)]
            f = [owned_ref[3 + a, pl.ds(c, 1), :] for a in range(3)]
            rel = owned_ref[6, pl.ds(c, 1), :].astype(i32) - 4 * PER_OWNER
            member = (iota((PER_OWNER, WIDE), 0) == rel).astype(f32).astype(bf16)
            member_ref[:, WIDE * k : WIDE * (k + 1)] = member
            for b in range(WIDE // 128):
                lanes = slice(128 * b, 128 * b + 128)
                out = slice(WIDE * k + 128 * b, WIDE * k + 128 * b + 128)
                for g in range(EQUIV // 8):
                    at = slice(8 * g, 8 * g + 8)
                    r = [wide[a, at, :] - d[a][:, lanes] for a in range(3)]
                    fb = [f[a][:, lanes] for a in range(3)]
                    even, along = pull(r, fb)
                    for a in range(3):
                        row = EQUIV * a + 8 * g
                        top, low = halves(even * fb[a] + along * r[a])
                        terms_top[row : row + 8, out] = top
                        terms_low[row : row + 8, out] = low
        total[...] += dot_nt(terms_top[...], member_ref[...]) + dot_nt(terms_low[...], member_ref[...])
        return carry

    lax.fori_loop(0, 3, one_home, 0)
    density[...] = dot_wide(inverse_ref[...], total[...] * inv_eight_pi)
    block_ref[...] = jnp.zeros_like(block_ref)
    for part in range(4):

        @pl.when(portion == part)
        def _():
            for a in range(3):
                rows = density[EQUIV * a + 14 * part : EQUIV * a + 14 * part + 14, :]
                block_ref[0:14, PER_OWNER * a : PER_OWNER * (a + 1)] = rows

    row = core * 4 + y
    own = pltpu.make_async_copy(block_ref, gat_ref.at[row, z], own_sem)
    own.start()
    z_copies = [
        remote(block_ref, gat_ref.at[row, z], z_send.at[k], z_recv.at[k], target)
        for k, target in enumerate(z_targets)
    ]
    for copy in z_copies:
        copy.start()

    low = jnp.floor(first * (1.0 / 16.0))
    high = jnp.floor(last * (1.0 / 16.0))
    lane = iota((48, 128), 1)
    which = iota((48, 1), 0).astype(f32)
    real = (which < float(CELLS)) & (which >= float(CPD))
    flags = []
    for t in range(CPD):
        low_t, high_t = low[t : t + 1], high[t : t + 1]
        flags.append(jnp.where((high >= low_t - 1.0) & (low <= high_t + 1.0) & real, 1.0, 0.0))
    owner = jnp.floor(low * 0.5)
    table = jnp.zeros((48, 128), f32)
    for t, flag in enumerate(flags):
        table = table + jnp.where(lane == t, flag, 0.0)
    rank = dot(before, table)
    count = jnp.sum(table, axis=0, keepdims=True)
    lane_row = iota((1, 128), 1).astype(f32)
    lists_ref[...] = jnp.zeros_like(lists_ref)
    lines = [jnp.zeros((1, 128), f32) for _ in range(2)]
    ahead = jnp.zeros((1, 1), f32)
    for t, flag in enumerate(flags):
        spot = rank[:, t : t + 1] + ahead
        for half in range(2):
            hit = (spot == lane.astype(f32) + 128.0 * half) & (flag > 0.0)
            lines[half] = lines[half] + jnp.sum(
                jnp.where(hit, which + 64.0 * t, 0.0), axis=0, keepdims=True
            )
        ahead = ahead + count[:, t : t + 1]
    for half in range(2):
        line = jnp.where(lane_row + 128.0 * half >= ahead, float(DUMMY), lines[half])
        lists_ref[half : half + 1, :] = line.astype(i32)
    lists_ref[2:3, :] = jnp.broadcast_to(ahead, (1, 128)).astype(i32)
    square = iota((48, 128), 0) == lane
    line = jnp.sum(jnp.where(square, owner, 0.0), axis=0, keepdims=True)
    lists_ref[7:8, :] = line.astype(i32)

    feature = iota((FEATURES, WIDE), 0)
    turn = lax.rem(feature, 6)
    use_top = (feature < 18) & ((turn == 0) | (turn == 3) | (turn == 5)) | (feature == 21)
    use_middle = (feature < 18) & ((turn == 1) | (turn == 4)) | (feature == 22)

    def factors(x, y, z, last):
        value = jnp.where(
            feature < 6, x, jnp.where(feature < 12, y, jnp.where(feature < 18, z, last))
        )
        top, middle, low = thirds(value)
        return jnp.where(use_top, top, jnp.where(use_middle, middle, low))

    def some_sources(index, carry):
        cells = [BATCH * index + k for k in range(BATCH)]
        rels = [comp_ref[REL, pl.ds(c, 1), :].astype(i32) for c in cells]
        hits = [
            (iota((160, WIDE), 0) == rel - 2 * PER_OWNER).astype(f32).astype(bf16) for rel in rels
        ]
        reaches = [dot(wanted_ref[...], hit) for hit in hits]
        for k, c in enumerate(cells):
            rel = rels[k]
            px = comp_ref[PX, pl.ds(c, 1), :] - (4 * (rel >> 5) + 2).astype(f32)
            py = comp_ref[PY, pl.ds(c, 1), :] - 4.0
            pz = comp_ref[PZ, pl.ds(c, 1), :] - 4.0
            fx, fy, fz = [comp_ref[FX + a, pl.ds(c, 1), :] for a in range(3)]
            square = (px * px + py * py) + (pz * pz + smooth_sq)
            along = (px * fx + py * fy) + pz * fz
            near_rows = factors(-2.0 * px, -2.0 * py, -2.0 * pz, square)
            near_rows = jnp.where((feature >= 18) & (feature < 21), 1.0, near_rows)
            push_rows = factors(fx, fy, fz, -along)
            push_rows = jnp.where((feature >= 18) & (feature < 21), 0.0, push_rows)
            mask_rows = FAR_AWAY - FAR_AWAY * reaches[k]
            rights_ref[c, :, 0:WIDE] = jnp.concatenate([near_rows, mask_rows], axis=0).astype(bf16)
            rights_ref[c, :, WIDE : 2 * WIDE] = jnp.concatenate(
                [push_rows, jnp.zeros((8 * CPD, WIDE), f32)], axis=0
            ).astype(bf16)
        return carry

    owners_ref[...] = jnp.broadcast_to(owner[0:8], (8, 128))

    def multiply_own(t, c, products):
        apart = owners_ref[pl.ds(c, 1), 0:1] - owners_ref[pl.ds(t, 1), 0:1]
        left = [lefts_ref[3 * t + w].astype(f32) for w in range(3)]
        left = jnp.where(apart < -0.5, left[0], jnp.where(apart > 0.5, left[2], left[1]))
        products[...] = dot(left.astype(bf16), rights_ref[c])

    def own_target(t, carry):
        for k in range(CPD // 2):
            multiply_own(t, 2 * k + 1, odd_pairs)
            add_pair(comp_ref, sums_ref, t, 2 * k, even_pairs)
            if k + 1 < CPD // 2:
                multiply_own(t, 2 * k + 2, even_pairs)
            else:
                multiply_own(jnp.minimum(t + 1, CPD - 1), 0, even_pairs)
            add_pair(comp_ref, sums_ref, t, 2 * k + 1, odd_pairs)
        return carry

    sums_ref[...] = jnp.zeros_like(sums_ref)
    rights_ref[DUMMY] = jnp.where(iota((DEPTH, 2 * WIDE), 0) == 21, FAR_AWAY, 0.0).astype(bf16)
    lax.fori_loop(0, EARLY, some_sources, 0)

    own.wait()
    y_copies, c_copies = [], []

    def pass_on(at, where, index):
        place = gat_ref.at[at, where]
        copy = remote(place, place, c_send.at[index], c_recv.at[index], c_target)
        copy.start()
        c_copies.append(copy)

    for order, k in enumerate((0, 1, 7, 2, 6, 3, 5, 4)):
        where = lax.rem(z - k + 8, 8)
        if k:
            z_copies[k - 1].wait_recv()
        place = gat_ref.at[row, where]
        for side, target in enumerate(y_targets):
            index = 3 * order + side
            copy = remote(place, place, y_send.at[index], y_recv.at[index], target)
            copy.start()
            y_copies.append(copy)
        pass_on(row, where, order)
    lax.fori_loop(EARLY, CELLS // BATCH, some_sources, 0)
    multiply_own(0, 0, even_pairs)
    lax.fori_loop(0, MIDDLE, own_target, 0)
    for order, k in enumerate((0, 1, 7, 2, 6, 3, 5, 4)):
        where = lax.rem(z - k + 8, 8)
        for side in range(3):
            index = 3 * order + side
            y_copies[index].wait_recv()
            pass_on(core * 4 + lax.rem(y - side + 3, 4), where, 8 + index)
    lax.fori_loop(MIDDLE, CPD, own_target, 0)
    for copy in (*z_copies, *y_copies):
        copy.wait_send()
    for copy in c_copies:
        copy.wait()


def first(displacement, point_leaf, near_list, stiffness, surf, up_inverse):
    npoints = displacement.shape[1]
    sides = len(OFFSETS)
    dma = pltpu.SemaphoreType.DMA
    return pl.pallas_call(
        first_kernel,
        out_shape=(
            jax.ShapeDtypeStruct((10, 48, WIDE), f32),
            jax.ShapeDtypeStruct((8, 128), i32),
            jax.ShapeDtypeStruct((8, 8, 16, 128), f32),
            jax.ShapeDtypeStruct((3 * CPD, SHARE_PAD, DEPTH), bf16),
            jax.ShapeDtypeStruct((CPD, 3, SHARE_PAD, 128), f32),
            jax.ShapeDtypeStruct((CELLS + 1, DEPTH, 2 * WIDE), bf16),
            jax.ShapeDtypeStruct((CPD, 4, SHARE_PAD, 128), f32),
        ),
        in_specs=[HBM] * 6,
        out_specs=(VMEM,) * 7,
        scratch_shapes=[
            pltpu.VMEM((sides, 3, npoints), f32),
            pltpu.VMEM((sides, 1, npoints), i32),
            pltpu.VMEM((3, npoints), f32),
            pltpu.VMEM((EQUIV, 8), f32),
            pltpu.VMEM((1, npoints), i32),
            pltpu.VMEM((2, FAR, 128), i32),
            pltpu.VMEM((NPT, NPT), f32),
            pltpu.VMEM((ROWS, ROWS), f32),
            pltpu.VMEM((144, WIDE), f32),
            pltpu.VMEM((48, WIDE), i32),
            pltpu.VMEM((144, NPT), f32),
            pltpu.VMEM((FAR, 128), i32),
            pltpu.VMEM((160, 128), bf16),
            pltpu.VMEM((8 * CPD, 160), bf16),
            pltpu.VMEM((3, EQUIV, 128), f32),
            pltpu.VMEM((7, 16, WIDE), f32),
            pltpu.VMEM((ROWS, 3 * WIDE), bf16),
            pltpu.VMEM((ROWS, 3 * WIDE), bf16),
            pltpu.VMEM((PER_OWNER, 3 * WIDE), bf16),
            pltpu.VMEM((ROWS, PER_OWNER), f32),
            pltpu.VMEM((ROWS, PER_OWNER), f32),
            pltpu.VMEM((16, 128), f32),
            pltpu.VMEM((SHARE_PAD, 2 * WIDE), f32),
            pltpu.VMEM((SHARE_PAD, 2 * WIDE), f32),
            pltpu.VMEM((8, 128), f32),
            dma((sides,)),
            dma((sides,)),
            dma((sides,)),
            dma((sides,)),
            dma((7,)),
            dma,
            dma((7,)),
            dma((7,)),
            dma((24,)),
            dma((24,)),
            dma((32,)),
            dma((32,)),
        ],
        compiler_params=pltpu.CompilerParams(
            collective_id=0, has_side_effects=True, vmem_limit_bytes=LIMIT
        ),
        name="first",
    )(*(in_hbm(x) for x in (displacement, point_leaf, near_list, stiffness, surf, up_inverse)))


def near_kernel(lists, comp_ref, lefts, spots, rights, own_sums, out_ref, even_pairs, odd_pairs, sums):
    portion = lax.axis_index("leaf")

    def pair(index):
        code = lists[index >> 7, index & 127]
        return code >> 6, code & 63

    def multiply(index, products):
        t, c = pair(index)
        w = jnp.clip(lists[7, c] - lists[7, t] + 1, 0, 2)
        products[...] = dot(lefts[3 * t + w], rights[c])

    sums[...] = own_sums[...]
    multiply(0, even_pairs)

    def some_pairs(index, carry):
        for k in range(TOGETHER):
            now, after = (odd_pairs, even_pairs) if k % 2 else (even_pairs, odd_pairs)
            at = TOGETHER * index + k
            multiply(at + 1, after)
            add_pair(comp_ref, sums, *pair(at), now)
        return carry

    lax.fori_loop(0, (lists[2, 0] + (TOGETHER - 1)) // TOGETHER, some_pairs, 0)
    pick_row, pick_lane = iota((SHARE_PAD, WIDE), 0), iota((SHARE_PAD, WIDE), 1)
    pick = (pick_lane == pick_row + SHARE * portion) & (pick_row < SHARE)

    def finish(index, carry):
        for t in (2 * index, 2 * index + 1):
            for a in range(3):
                total = sums[t, a] + spots[t, a] * sums[t, 3]
                column = jnp.sum(total, axis=1, keepdims=True) * inv_eight_pi
                row = jnp.sum(jnp.where(pick, column, 0.0), axis=0, keepdims=True)
                out_ref[a, pl.ds(t, 1), :] = row
        return carry

    lax.fori_loop(0, CPD // 2, finish, 0)


def near_field(lists, comp, lefts, spots, rights, own_sums):
    return pl.pallas_call(
        near_kernel,
        out_shape=jax.ShapeDtypeStruct((3, 8, WIDE), f32),
        in_specs=[SMEM] + [VMEM] * 5,
        out_specs=VMEM,
        scratch_shapes=[
            pltpu.VMEM((SHARE_PAD, 2 * WIDE), f32),
            pltpu.VMEM((SHARE_PAD, 2 * WIDE), f32),
            pltpu.VMEM((CPD, 4, SHARE_PAD, 128), f32),
        ],
        compiler_params=pltpu.CompilerParams(vmem_limit_bytes=LIMIT),
        name="near_field",
    )(lists, comp, lefts, spots, rights, own_sums)


def far_part(
    left_ref,
    quarter_ref,
    gat_ref,
    far_ref,
    far_load,
    surf_ref,
    inverse_ref,
    local_ref,
    far4,
    sources,
    packed,
    pushes,
    mids,
    total,
    quarter,
    even_rows,
    odd_rows,
    even_blocks,
    odd_blocks,
):
    me = lax.axis_index("cells")
    portion = lax.axis_index("leaf")
    lane = iota((16, 128), 1)

    def one_tile(tile, carry):
        for half in range(2):
            rows = [jnp.zeros((16, 128), f32) for _ in range(3)]
            for v in range(4):
                at = 8 * tile + 4 * half + v
                value = gat_ref[at // 8, at - at // 8 * 8]
                for a in range(3):
                    shift = (PER_OWNER * (v - a)) % 128
                    moved = pltpu.roll(value, shift, 1) if shift else value
                    rows[a] = jnp.where(lane // PER_OWNER == v, moved, rows[a])
            top, low = halves(jnp.concatenate(rows, axis=0))
            packed[tile, 0:48, 128 * half : 128 * half + 128] = top
            packed[tile, 48:96, 128 * half : 128 * half + 128] = low
        return carry

    lax.fori_loop(0, 8, one_tile, 0)

    far_load.wait()
    entries = far_ref[...]
    mine = lax.rem(me, 4)
    lane48 = iota((FAR, 128), 1) // PER_OWNER
    picked = jnp.zeros((FAR, 128), i32)
    for place in range(4):
        moved = entries
        for k in range(1, 4):
            turned = pltpu.roll(entries, PER_OWNER * k, 1)
            moved = jnp.where(lax.rem(mine + k, 4) == place, turned, moved)
        far4[place] = moved
    for place in range(4):
        rows = far4[place, pl.ds(place, FAR // 4, stride=4), :]
        chosen = iota((FAR // 4, 128), 1) // PER_OWNER == place
        if place == 0:
            merged = rows
        else:
            merged = jnp.where(chosen, rows, merged)
    owner = merged >> 5
    spot = (((owner & 1) << 5) + (owner >> 1)) * PER_OWNER + (merged & 31)
    sources[0:12, :] = jnp.where(merged >= 0, spot, -1)
    target = me * PER_OWNER + (iota((12, 128), 1) & 31)
    mids[0, 0:12, :] = (2 * ((target >> 4) - (merged >> 4))).astype(f32)
    mids[1, 0:12, :] = (2 * (((target >> 2) & 3) - ((merged >> 2) & 3))).astype(f32)
    mids[2, 0:12, :] = (2 * ((target & 3) - (merged & 3))).astype(f32)

    def gather_two(index):
        first = sources[pl.ds(2 * index, 1), :]
        second = sources[pl.ds(2 * index + 1, 1), :]
        wanted = jnp.concatenate([first, second], axis=1)
        found = jnp.zeros((96, 256), f32)
        for tile in range(8):
            onehot = (iota((256, 256), 0) + 256 * tile == wanted).astype(f32).astype(bf16)
            found = found + dot(packed[tile], onehot)
        value = found[0:48] + found[48:96]
        pushes[2 * index] = value[:, 0:128]
        pushes[2 * index + 1] = value[:, 128:256]

    def some_gathers(index, carry):
        for k in range(3):
            gather_two(3 * index + k)
        return carry

    lax.fori_loop(0, 2, some_gathers, 0)
    total[...] = jnp.zeros_like(total)

    left = left_ref[...].astype(bf16)
    for a in range(3):
        quarter[a] = jnp.broadcast_to(quarter_ref[portion, :, a : a + 1], (16, 128))
    steps = thirds(jnp.full((16, 128), (inner_radius / 3.0) ** 2, f32))
    for rows in (even_rows, odd_rows):
        rows[...] = jnp.zeros_like(rows)
        for k in range(3):
            rows[pl.ds(12 + k, 16, stride=32), :] = steps[k]

    def prepare_block(index, rows, blocks):
        push = [pushes[index, 16 * a : 16 * a + 16, :] for a in range(3)]
        gap = [mids[a, pl.ds(index, 1), :] - quarter[a] for a in range(3)]
        square = (gap[0] * gap[0] + gap[1] * gap[1]) + (gap[2] * gap[2] + smooth_sq)
        inner = (gap[0] * push[0] + gap[1] * push[1]) + gap[2] * push[2]
        scale = inner_radius / 3.0
        for a in range(3):
            for k, third in enumerate(thirds((2.0 * scale) * gap[a])):
                rows[pl.ds(3 * a + k, 16, stride=32), :] = third
            for k, third in enumerate(thirds(scale * push[a])):
                rows[pl.ds(16 + 3 * a + k, 16, stride=32), :] = third
        for k, third in enumerate(thirds(square)):
            rows[pl.ds(9 + k, 16, stride=32), :] = third
        for k, third in enumerate(thirds(inner)):
            rows[pl.ds(25 + k, 16, stride=32), :] = third
        for j in range(14):
            right = jnp.concatenate(
                [rows[32 * j : 32 * j + 16, :], rows[32 * j + 16 : 32 * j + 32, :]], axis=1
            )
            blocks[j] = dot(left, right.astype(bf16))

    def add_block(index, blocks):
        groups = EQUIV // 8
        sums = [[jnp.zeros((8, 128), f32) for _ in range(4)] for _ in range(groups)]
        for j in range(14):
            f = [pushes[index, 16 * a + j : 16 * a + j + 1, :] for a in range(3)]
            shift = [quarter[a, j : j + 1, :] for a in range(3)]
            for g in range(groups):
                at = slice(8 * g, 8 * g + 8)
                shifted = blocks[j, at, 0:128]
                inner = blocks[j, at, 128:256]
                root = lax.rsqrt(shifted)
                cube = root * root * root
                even = root + smooth_sq * cube
                along = cube * inner
                for a in range(3):
                    sums[g][a] = sums[g][a] + (even * f[a] - along * shift[a])
                sums[g][3] = sums[g][3] + along
        mid = [mids[a, pl.ds(index, 1), :] for a in range(3)]
        for g in range(groups):
            at = slice(8 * g, 8 * g + 8)
            for a in range(3):
                check = mid[a] + inner_radius * surf_ref[at, a : a + 1]
                row = EQUIV * a + 8 * g
                total[row : row + 8, :] += sums[g][a] + check * sums[g][3]

    prepare_block(0, even_rows, even_blocks)

    def two_blocks(index, carry):
        prepare_block(2 * index + 1, odd_rows, odd_blocks)
        add_block(2 * index, even_blocks)
        prepare_block(jnp.minimum(2 * index + 2, 11), even_rows, even_blocks)
        add_block(2 * index + 1, odd_blocks)
        return carry

    lax.fori_loop(0, 6, two_blocks, 0)
    value = total[...] * inv_eight_pi
    value = value + pltpu.roll(value, 64, 1)
    value = value + pltpu.roll(value, 32, 1)
    local_ref[...] = dot_wide(inverse_ref[...], value)


def last_kernel(
    left_ref,
    quarter_ref,
    gat_ref,
    far_hbm,
    surf_ref,
    inverse_ref,
    comp_ref,
    near_ref,
    out_ref,
    far_ref,
    load_sem,
    far4,
    sources,
    packed,
    pushes,
    mids,
    total,
    quarter,
    even_rows,
    odd_rows,
    even_blocks,
    odd_blocks,
    local_ref,
    packed_local,
    held_local,
    factors,
    spread_ref,
    cell_ref,
    part_ref,
    held_part,
    send_local,
    recv_local,
    send_part,
    recv_part,
):
    block = pl.multiple_of(lax.axis_index("cells") // 4 * 128, 128)
    far_load = pltpu.make_async_copy(far_hbm.at[:, pl.ds(block, 128)], far_ref, load_sem)
    far_load.start()
    packed_local[...] = jnp.zeros_like(packed_local)
    sides = beside("cells", (1, -1))
    mates = beside("leaf", (1, 2, 3))
    barrier = pltpu.get_barrier_semaphore()
    for target in (*sides, *mates):
        pl.semaphore_signal(barrier, inc=1, device_id=target, device_id_type=MESH)
    far_part(
        left_ref,
        quarter_ref,
        gat_ref,
        far_ref,
        far_load,
        surf_ref,
        inverse_ref,
        local_ref,
        far4,
        sources,
        packed,
        pushes,
        mids,
        total,
        quarter,
        even_rows,
        odd_rows,
        even_blocks,
        odd_blocks,
    )
    pl.semaphore_wait(barrier, 5)
    lane = iota((48, 128), 1) // PER_OWNER
    for k in range(4):
        rows = min(48, ROWS - 48 * k)
        piece = local_ref[48 * k : 48 * k + rows, :]
        here = lane[0:rows] == k
        packed_local[0:rows, :] = jnp.where(here, piece, packed_local[0:rows, :])
    copies = [
        remote(packed_local, held_local.at[k], send_local.at[k], recv_local.at[k], target)
        for k, target in enumerate(sides)
    ]
    for copy in copies:
        copy.start()
    for copy in copies:
        copy.wait()
    lane = iota((48, 128), 1) // PER_OWNER
    for k in range(4):
        rows = min(48, ROWS - 48 * k)
        value = local_ref[48 * k : 48 * k + rows, :]
        for side in range(2):
            place = 2 * side
            moved = held_local[side, 0:rows, :]
            if place != k:
                moved = pltpu.roll(moved, (PER_OWNER * (place - k)) % 128, 1)
            value = jnp.where(lane[0:rows] == place, moved, value)
        top, low = halves(value)
        factors[48 * k : 48 * k + rows, 0:128] = top
        factors[48 * k : 48 * k + rows, 128:256] = low

    def spread_out(t):
        rel = comp_ref[REL, pl.ds(t, 1), :].astype(i32) - 3 * PER_OWNER
        member = (iota((128, WIDE), 0) == rel).astype(f32).astype(bf16)
        spread_ref[t] = dot(factors[...], jnp.concatenate([member, member], axis=0))

    def three_cells(index, carry):
        for k in range(3):
            spread_out(3 * index + k)
        return carry

    lax.fori_loop(0, 2, three_cells, 0)

    def one_cell(t):
        d = [comp_ref[DX + a, pl.ds(t, 1), :] for a in range(3)]
        sums = [jnp.zeros((8, WIDE), f32) for _ in range(3)]
        for g in range(EQUIV // 8):
            at = slice(8 * g, 8 * g + 8)
            r = [d[a] - outer_radius * surf_ref[at, a : a + 1] for a in range(3)]
            f = [spread_ref[t, EQUIV * a + 8 * g : EQUIV * a + 8 * g + 8, :] for a in range(3)]
            even, along = pull(r, f)
            sums = [sums[a] + (even * f[a] + along * r[a]) for a in range(3)]
        for a in range(3):
            row = jnp.sum(sums[a], axis=0, keepdims=True) * inv_eight_pi
            cell_ref[a, pl.ds(t, 1), :] = row + near_ref[a, pl.ds(t, 1), :]

    def two_cells(index, carry):
        one_cell(2 * index)
        one_cell(2 * index + 1)
        return carry

    lax.fori_loop(0, CPD // 2, two_cells, 0)
    for t in range(CPD):
        for a in range(3):
            part_ref[a : a + 1, NPT * t : NPT * (t + 1)] = cell_ref[a, t : t + 1, 0:NPT]
    copies = [
        remote(part_ref, held_part.at[k], send_part.at[k], recv_part.at[k], target)
        for k, target in enumerate(mates)
    ]
    for copy in copies:
        copy.start()
    for copy in copies:
        copy.wait()
    out_ref[...] = (part_ref[...] + held_part[1]) + (held_part[0] + held_part[2])


def last(left, quarter, gathered, far_list, surf, down_inverse, comp, near, npoints):
    dma = pltpu.SemaphoreType.DMA
    return pl.pallas_call(
        last_kernel,
        out_shape=jax.ShapeDtypeStruct((3, npoints), f32),
        in_specs=[VMEM, VMEM, VMEM, HBM] + [VMEM] * 4,
        out_specs=VMEM,
        scratch_shapes=[
            pltpu.VMEM((FAR, 128), i32),
            dma,
            pltpu.VMEM((4, FAR, 128), i32),
            pltpu.VMEM((16, 128), i32),
            pltpu.VMEM((8, 96, 256), bf16),
            pltpu.VMEM((12, FAR, 128), f32),
            pltpu.VMEM((3, 16, 128), f32),
            pltpu.VMEM((ROWS, 128), f32),
            pltpu.VMEM((3, 16, 128), f32),
            pltpu.VMEM((512, 128), f32),
            pltpu.VMEM((512, 128), f32),
            pltpu.VMEM((14, EQUIV, 256), f32),
            pltpu.VMEM((14, EQUIV, 256), f32),
            pltpu.VMEM((ROWS, 128), f32),
            pltpu.VMEM((48, 128), f32),
            pltpu.VMEM((2, 48, 128), f32),
            pltpu.VMEM((ROWS, 256), bf16),
            pltpu.VMEM((CPD, ROWS, WIDE), f32),
            pltpu.VMEM((3, 8, WIDE), f32),
            pltpu.VMEM((3, npoints), f32),
            pltpu.VMEM((3, 3, npoints), f32),
            dma((2,)),
            dma((2,)),
            dma((3,)),
            dma((3,)),
        ],
        compiler_params=pltpu.CompilerParams(
            collective_id=1, has_side_effects=True, vmem_limit_bytes=LIMIT
        ),
        name="last",
    )(left, quarter, gathered, in_hbm(far_list), surf, down_inverse, comp, near)


def body(displacement, point_leaf, near_list, far_list, stiffness, up_inverse, down_inverse):
    table = surface_table()
    surf = jnp.asarray(np.pad(table, ((0, 0), (0, 5))))
    whole = np.round(3.0 * table)
    ones = np.ones((EQUIV, 3), np.float32)
    square = np.sum(whole * whole, axis=1, keepdims=True)
    left = np.concatenate([np.repeat(whole, 3, axis=1), ones, ones * square, 0.0 * square], axis=1)
    left = jnp.asarray(left.astype(np.float32))
    quarter = inner_radius * table.reshape(4, 14, 3)
    quarter = jnp.asarray(np.pad(quarter, ((0, 0), (0, 2), (0, 5))).astype(np.float32))
    comp, lists, gathered, lefts, spots, rights, own_sums = first(
        displacement, point_leaf, near_list, stiffness, surf, up_inverse
    )
    near = near_field(lists, comp, lefts, spots, rights, own_sums)
    return last(
        left, quarter, gathered, far_list, surf, down_inverse, comp, near, displacement.shape[1]
    )


def solution(mesh):
    in_specs = (P(None, "cells"), P("cells"), P(), P(), P(), P(), P())
    out_specs = P(None, "cells")
    return jax.shard_map(body, mesh=mesh, in_specs=in_specs, out_specs=out_specs, check_vma=False)
```

```python
import math

import jax
import jax.numpy as jnp
import numpy as np
from jax import lax
from jax.experimental import pallas as pl
from jax.experimental.pallas import tpu as pltpu
from jax.sharding import PartitionSpec as P

NPT = 312
CPD = 6
SLICE = 16
EQUIV = 56
FAR = 48
ROWS = 3 * EQUIV
PER_OWNER = 2 * SLICE
WIDE = 384
OFFSETS = (1, -1, 2, -2, 3, -3)
CELLS = CPD * (len(OFFSETS) + 1)
OWNABLE = 3 * CPD
SHARE = NPT // 4
SHARE_PAD = 80

inv_eight_pi = 1.0 / (8.0 * math.pi)
smooth_sq = 0.0625
inner_radius = 1.05
outer_radius = 2.95
MESH = pl.DeviceIdType.MESH
VMEM = pl.BlockSpec(memory_space=pltpu.VMEM)
SMEM = pl.BlockSpec(memory_space=pltpu.SMEM)
f32 = jnp.float32
bf16 = jnp.bfloat16
i32 = jnp.int32


def surface_table():
    ladder = [-1.0, -1.0 / 3.0, 1.0 / 3.0, 1.0]
    corners = [
        (a, b, c)
        for a in ladder
        for b in ladder
        for c in ladder
        if max(abs(a), abs(b), abs(c)) == 1.0
    ]
    return np.array(corners, dtype=np.float32)


def iota(shape, dim):
    return lax.broadcasted_iota(i32, shape, dim)


def dot(a, b):
    return jnp.dot(a, b, preferred_element_type=f32)


def dot_nt(a, b):
    return lax.dot_general(a, b, (((1,), (1,)), ((), ())), preferred_element_type=f32)


def halves(value):
    top = value.astype(bf16)
    return top, (value - top.astype(f32)).astype(bf16)


def dot_wide(a, b):
    a_top, a_low = halves(a)
    b_top, b_low = halves(b)
    return dot(a_top, b_top) + (dot(a_top, b_low) + dot(a_low, b_top))


DX, DY, DZ, FX, FY, FZ, PX, PY, PZ, REL = range(10)
FEATURES = 24
DEPTH = FEATURES + 8 * CPD
FAR_AWAY = 1e30
LIMIT = 20 << 20
HBM = pl.BlockSpec(memory_space=pltpu.HBM)
DUMMY = CELLS
TOGETHER = 4
BATCH = 6
PARTS = 2
STEPS = (0, 1, 7, 2, 6, 3, 5, 4)


def thirds(value):
    top = value.astype(bf16).astype(f32)
    rest = value - top
    middle = rest.astype(bf16).astype(f32)
    return top, middle, rest - middle


def pull(offset, strength):
    dx, dy, dz = offset
    fx, fy, fz = strength
    shifted = (dx * dx + dy * dy) + (dz * dz + smooth_sq)
    inner = (dx * fx + dy * fy) + dz * fz
    root = lax.rsqrt(shifted)
    cube = root * root * root
    return root + smooth_sq * cube, cube * inner


def in_hbm(array):
    return pltpu.with_memory_space_constraint(array, pltpu.HBM)


def remote(src, dst, send_sem, recv_sem, target):
    return pltpu.make_async_remote_copy(
        src_ref=src,
        dst_ref=dst,
        send_sem=send_sem,
        recv_sem=recv_sem,
        device_id=target,
        device_id_type=MESH,
    )


def greet(targets):
    barrier = pltpu.get_barrier_semaphore()
    for target in targets:
        pl.semaphore_signal(barrier, inc=1, device_id=target, device_id_type=MESH)
    pl.semaphore_wait(barrier, len(targets))


def beside(axis, offsets):
    count = lax.axis_size(axis)
    me = lax.axis_index(axis)
    return [{axis: lax.rem(me + (off + count), count)} for off in offsets]


def add_pair(comp_ref, sums, t, c, products):
    p = [comp_ref[PX + a, pl.ds(c, 1), :] for a in range(3)]
    f = [comp_ref[FX + a, pl.ds(c, 1), :] for a in range(3)]
    for part in range(PARTS):
        groups = range(part * 10 // PARTS, (part + 1) * 10 // PARTS)
        added = {}
        for b in range(WIDE // 128):
            lanes = slice(128 * b, 128 * b + 128)
            pb = [value[:, lanes] for value in p]
            fb = [value[:, lanes] for value in f]
            for g in groups:
                at = slice(8 * g, 8 * g + 8)
                shifted = products[at, lanes]
                inner = products[at, WIDE + 128 * b : WIDE + 128 * b + 128]
                root = lax.rsqrt(shifted)
                cube = root * root * root
                even = root + smooth_sq * cube
                along = cube * inner
                one = [even * fb[a] - along * pb[a] for a in range(3)] + [along]
                added[g] = [u + v for u, v in zip(added[g], one)] if b else one
        for g in groups:
            at = slice(8 * g, 8 * g + 8)
            for a in range(4):
                sums[t, a, at, :] += added[g][a]


def first_kernel(
    disp_hbm,
    leaf_hbm,
    near_hbm,
    stiff_hbm,
    surf_hbm,
    inverse_hbm,
    comp_ref,
    lists_ref,
    gat_ref,
    lefts_ref,
    spots_ref,
    rights_ref,
    sums_ref,
    held_disp,
    held_leaf,
    disp_ref,
    surf_ref,
    leaf_ref,
    near_ref,
    stiff_ref,
    inverse_ref,
    disp,
    leaves,
    force,
    listed_ref,
    relation,
    wanted_ref,
    wide,
    owned_ref,
    terms_top,
    terms_low,
    member_ref,
    total,
    density,
    block_ref,
    even_pairs,
    odd_pairs,
    owners_ref,
    send_disp,
    recv_disp,
    send_leaf,
    recv_leaf,
    load_sem,
    own_sem,
    z_send,
    z_recv,
    y_send,
    y_recv,
    c_send,
    c_recv,
):
    me = lax.axis_index("cells")
    portion = lax.axis_index("leaf")
    start = lax.rem(me + 63, 64)
    block = start // 4
    leaf_load = pltpu.make_async_copy(leaf_hbm, leaf_ref.at[0], load_sem.at[0])
    loads = [
        pltpu.make_async_copy(
            near_hbm.at[:, pl.ds(pl.multiple_of(lax.rem(block + k, 16) * 128, 128), 128)],
            near_ref.at[k],
            load_sem.at[1 + k],
        )
        for k in range(2)
    ]
    loads.append(pltpu.make_async_copy(stiff_hbm, stiff_ref, load_sem.at[3]))
    loads.append(pltpu.make_async_copy(inverse_hbm, inverse_ref, load_sem.at[4]))
    loads.append(pltpu.make_async_copy(surf_hbm, surf_ref, load_sem.at[5]))
    disp_load = pltpu.make_async_copy(disp_hbm, disp_ref, load_sem.at[6])
    disp_load.start()
    leaf_load.start()
    for load in loads:
        load.start()
    core = lax.rem(me, 2)
    z = lax.rem(me // 2, 8)
    y = me // 16

    def device(y_at, z_at, core_at):
        return {"cells": (y_at * 8 + z_at) * 2 + core_at}

    sides = beside("cells", OFFSETS)
    z_targets = [device(y, lax.rem(z + k, 8), core) for k in range(1, 8)]
    y_targets = [device(lax.rem(y + k, 4), z, core) for k in range(1, 4)]
    c_target = device(y, z, 1 - core)
    greet([*sides, *z_targets, *y_targets, c_target])
    disp_load.wait()
    leaf_load.wait()
    copies = []
    for slot, target in enumerate(sides):
        copies.append(
            remote(disp_ref, held_disp.at[slot], send_disp.at[slot], recv_disp.at[slot], target)
        )
        copies.append(
            remote(leaf_ref, held_leaf.at[slot], send_leaf.at[slot], recv_leaf.at[slot], target)
        )
    for copy in copies:
        copy.start()

    comp_ref[...] = jnp.zeros_like(comp_ref)
    disp[...] = jnp.zeros_like(disp)
    leaves[...] = jnp.zeros_like(leaves)

    def place_cells(home, points, leaf_row):
        for k in range(CPD):
            at = slice(NPT * k, NPT * (k + 1))
            row = home * CPD + k
            for a in range(3):
                disp[48 * a + row : 48 * a + row + 1, 0:NPT] = points[a : a + 1, at]
            leaves[row : row + 1, 0:NPT] = leaf_row[:, at]

    def fill_table(rows):
        live = iota((rows, WIDE), 1) < NPT
        rel = jnp.where(live, (leaves[0:rows, :] - PER_OWNER * (me - 4)) & 2047, -1)
        for a in range(3):
            comp_ref[DX + a, 0:rows, :] = disp[48 * a : 48 * a + rows, :]
        comp_ref[REL, 0:rows, :] = rel.astype(f32)
        comp_ref[PX, 0:rows, :] = comp_ref[DX, 0:rows, :] + (2 * (rel >> 4) + 1).astype(f32)
        comp_ref[PY, 0:rows, :] = comp_ref[DY, 0:rows, :] + (2 * ((rel >> 2) & 3) + 1).astype(f32)
        comp_ref[PZ, 0:rows, :] = comp_ref[DZ, 0:rows, :] + (2 * (rel & 3) + 1).astype(f32)
        relf = rel.astype(f32)
        first = jnp.min(jnp.where(live, relf, 1e9), axis=1, keepdims=True)
        last = jnp.max(relf, axis=1, keepdims=True)
        return first, last

    place_cells(0, disp_ref[...], leaf_ref[...])
    first, last = fill_table(8)

    for load in loads:
        load.wait()
    both = jnp.concatenate([near_ref[0], near_ref[1]], axis=1)
    listed = both[:, 0:128]
    for k in range(1, 4):
        listed = jnp.where(lax.rem(start, 4) == k, both[:, 32 * k : 32 * k + 128], listed)
    listed_ref[...] = jnp.where(listed >= 0, (listed - PER_OWNER * (me - 2)) & 2047, -1)
    source_leaf = iota((160, 128), 0)

    def eight_entries(index, near):
        rows = listed_ref[pl.ds(pl.multiple_of(8 * index, 8), 8), :]
        for k in range(8):
            near = near + jnp.where(rows[k : k + 1, :] == source_leaf, 1.0, 0.0)
        return near

    near = lax.fori_loop(0, 6, eight_entries, jnp.zeros((160, 128), f32))
    relation[...] = near.astype(bf16)
    row8, lane8 = iota((8, 128), 0).astype(f32), iota((8, 128), 1).astype(f32)
    leaf_rows = [
        jnp.where((lane8 == first[t : t + 1] - 3.0 * PER_OWNER + row8) & (row8 < 3.0), 1.0, 0.0)
        for t in range(CPD)
    ]
    wanted_ref[...] = dot_nt(
        jnp.concatenate(leaf_rows, axis=0).astype(bf16), relation[...]
    ).astype(bf16)

    pick_row, pick_lane = iota((SHARE_PAD, WIDE), 0), iota((SHARE_PAD, WIDE), 1)
    pick16 = ((pick_lane == pick_row + SHARE * portion) & (pick_row < SHARE)).astype(f32).astype(bf16)
    slot = iota((SHARE_PAD, 128), 1)
    slot_turn = lax.rem(slot, 6)
    left_first = (slot < 18) & (slot_turn < 3) | (slot == 18)
    left_second = (slot < 18) & (slot_turn >= 3) & (slot_turn < 5) | (slot == 19)
    row32 = iota((32, WIDE), 0)

    def one_own(t):
        rel = comp_ref[REL, pl.ds(t, 1), :]
        px, py, pz = [comp_ref[PX + a, pl.ds(t, 1), :] for a in range(3)]
        lowest = jnp.min(jnp.where(rel >= 0.0, rel, 1e9), axis=1, keepdims=True)
        owner = jnp.floor(lowest * (1.0 / PER_OWNER))
        py4, pz4 = py - 4.0, pz - 4.0
        rows = []
        for w in range(3):
            px4 = px - (4.0 * (owner + float(w - 1)) + 2.0)
            square = (px4 * px4 + py4 * py4) + pz4 * pz4
            rows.append(
                jnp.where(
                    row32 < 6,
                    px4,
                    jnp.where(row32 < 12, py4, jnp.where(row32 < 18, pz4, square)),
                )
            )
        place = jnp.where(row32 == 0, px, jnp.where(row32 == 1, py, jnp.where(row32 == 2, pz, rel)))
        top, middle, low = thirds(jnp.concatenate([*rows, place], axis=0))
        found = dot_nt(pick16, top.astype(bf16)) + (
            dot_nt(pick16, middle.astype(bf16)) + dot_nt(pick16, low.astype(bf16))
        )
        for a in range(3):
            spots_ref[t, a] = jnp.broadcast_to(found[:, 96 + a : 97 + a], (SHARE_PAD, 128))
        leaf_at = (found[:, 99:100] - lowest).astype(i32)
        matched = (slot - (FEATURES + 8 * t) == leaf_at) & (leaf_at >= 0) & (leaf_at < 3)
        for w in range(3):
            value = pltpu.roll(found, 128 - 32 * w, 1) if w else found
            top, middle, low = thirds(value)
            chosen = jnp.where(left_first, top, jnp.where(left_second, middle, low))
            chosen = jnp.where((slot >= 21) & (slot < 24), 1.0, chosen)
            chosen = jnp.where(slot >= FEATURES, jnp.where(matched, 1.0, 0.0), chosen)
            lefts_ref[3 * t + w] = chosen[:, 0:DEPTH].astype(bf16)

    def two_own(index, carry):
        one_own(2 * index)
        one_own(2 * index + 1)
        return carry

    lax.fori_loop(0, CPD // 2, two_own, 0)
    for a in range(3):
        wide[a] = jnp.broadcast_to(outer_radius * surf_ref[:, a : a + 1], (EQUIV, 128))

    for copy in copies:
        copy.wait()
    for home in range(1, len(OFFSETS) + 1):
        place_cells(home, held_disp[home - 1], held_leaf[home - 1])
    first, last = fill_table(48)
    force[...] = dot_wide(disp[0:144, 0:NPT], stiff_ref[...])
    for a in range(3):
        comp_ref[FX + a, 0:48, 0:NPT] = force[48 * a : 48 * a + 48, :]

    cell = iota((48, 1), 0)
    mine = (jnp.floor(first * (1.0 / PER_OWNER)) == 4.0) & (cell < OWNABLE)
    mine = jnp.where(mine, 1.0, 0.0)
    before = (iota((48, 48), 0) > iota((48, 48), 1)).astype(f32)
    rank = dot(before, jnp.broadcast_to(mine, (48, 128)))
    chosen = jnp.where((rank == iota((48, 128), 1).astype(f32)) & (mine > 0.0), 1.0, 0.0)
    chosen = jnp.concatenate([chosen] * 3, axis=0).astype(bf16)
    for k, part in enumerate((DX, DY, DZ, FX, FY, FZ, REL)):
        pieces = jnp.concatenate(thirds(comp_ref[part]), axis=0).astype(bf16)
        found = lax.dot_general(
            chosen, pieces, (((0,), (0,)), ((), ())), preferred_element_type=f32
        )
        owned_ref[k] = found[0:16]
    total[...] = jnp.zeros_like(total)

    def one_home(home, carry):
        for k in range(3):
            c = 3 * home + k
            d = [owned_ref[a, pl.ds(c, 1), :] for a in range(3)]
            f = [owned_ref[3 + a, pl.ds(c, 1), :] for a in range(3)]
            rel = owned_ref[6, pl.ds(c, 1), :].astype(i32) - 4 * PER_OWNER
            member = (iota((PER_OWNER, WIDE), 0) == rel).astype(f32).astype(bf16)
            member_ref[:, WIDE * k : WIDE * (k + 1)] = member
            for b in range(WIDE // 128):
                lanes = slice(128 * b, 128 * b + 128)
                out = slice(WIDE * k + 128 * b, WIDE * k + 128 * b + 128)
                for g in range(EQUIV // 8):
                    at = slice(8 * g, 8 * g + 8)
                    r = [wide[a, at, :] - d[a][:, lanes] for a in range(3)]
                    fb = [f[a][:, lanes] for a in range(3)]
                    even, along = pull(r, fb)
                    for a in range(3):
                        row = EQUIV * a + 8 * g
                        top, low = halves(even * fb[a] + along * r[a])
                        terms_top[row : row + 8, out] = top
                        terms_low[row : row + 8, out] = low
        total[...] += dot_nt(terms_top[...], member_ref[...]) + dot_nt(terms_low[...], member_ref[...])
        return carry

    lax.fori_loop(0, 3, one_home, 0)
    density[...] = dot_wide(inverse_ref[...], total[...] * inv_eight_pi)
    block_ref[...] = jnp.zeros_like(block_ref)
    for part in range(4):

        @pl.when(portion == part)
        def _():
            for a in range(3):
                rows = density[EQUIV * a + 14 * part : EQUIV * a + 14 * part + 14, :]
                block_ref[0:14, PER_OWNER * a : PER_OWNER * (a + 1)] = rows

    row = core * 4 + y
    own = pltpu.make_async_copy(block_ref, gat_ref.at[row, z], own_sem)
    own.start()
    z_copies = [
        remote(block_ref, gat_ref.at[row, z], z_send.at[k], z_recv.at[k], target)
        for k, target in enumerate(z_targets)
    ]
    for copy in z_copies:
        copy.start()
    y_copies, c_copies = [], []

    def send_along_y(source, where, order):
        for side, target in enumerate(y_targets):
            index = 3 * order + side
            copy = remote(source, gat_ref.at[row, where], y_send.at[index], y_recv.at[index], target)
            copy.start()
            y_copies.append(copy)

    def pass_on(source, at, where, index):
        copy = remote(source, gat_ref.at[at, where], c_send.at[index], c_recv.at[index], c_target)
        copy.start()
        c_copies.append(copy)

    def take_z(orders):
        for order in orders:
            k = STEPS[order]
            where = lax.rem(z - k + 8, 8)
            z_copies[k - 1].wait_recv()
            place = gat_ref.at[row, where]
            send_along_y(place, where, order)
            pass_on(place, row, where, order)

    def take_y(orders):
        for order in orders:
            where = lax.rem(z - STEPS[order] + 8, 8)
            for side in range(3):
                index = 3 * order + side
                y_copies[index].wait_recv()
                at = core * 4 + lax.rem(y - side + 3, 4)
                pass_on(gat_ref.at[at, where], at, where, 8 + index)

    send_along_y(block_ref, z, 0)
    pass_on(block_ref, row, z, 0)

    low = jnp.floor(first * (1.0 / 16.0))
    high = jnp.floor(last * (1.0 / 16.0))
    lane = iota((48, 128), 1)
    which = iota((48, 1), 0).astype(f32)
    real = (which < float(CELLS)) & (which >= float(CPD))
    flags = []
    for t in range(CPD):
        low_t, high_t = low[t : t + 1], high[t : t + 1]
        flags.append(jnp.where((high >= low_t - 1.0) & (low <= high_t + 1.0) & real, 1.0, 0.0))
    owner = jnp.floor(low * 0.5)
    table = jnp.zeros((48, 128), f32)
    for t, flag in enumerate(flags):
        table = table + jnp.where(lane == t, flag, 0.0)
    rank = dot(before, table)
    count = jnp.sum(table, axis=0, keepdims=True)
    lane_row = iota((1, 128), 1).astype(f32)
    lists_ref[...] = jnp.zeros_like(lists_ref)
    lines = [jnp.zeros((1, 128), f32) for _ in range(2)]
    ahead = jnp.zeros((1, 1), f32)
    for t, flag in enumerate(flags):
        spot = rank[:, t : t + 1] + ahead
        for half in range(2):
            hit = (spot == lane.astype(f32) + 128.0 * half) & (flag > 0.0)
            lines[half] = lines[half] + jnp.sum(
                jnp.where(hit, which + 64.0 * t, 0.0), axis=0, keepdims=True
            )
        ahead = ahead + count[:, t : t + 1]
    for half in range(2):
        line = jnp.where(lane_row + 128.0 * half >= ahead, float(DUMMY), lines[half])
        lists_ref[half : half + 1, :] = line.astype(i32)
    lists_ref[2:3, :] = jnp.broadcast_to(ahead, (1, 128)).astype(i32)
    square = iota((48, 128), 0) == lane
    line = jnp.sum(jnp.where(square, owner, 0.0), axis=0, keepdims=True)
    lists_ref[7:8, :] = line.astype(i32)

    feature = iota((FEATURES, WIDE), 0)
    turn = lax.rem(feature, 6)
    use_top = (feature < 18) & ((turn == 0) | (turn == 3) | (turn == 5)) | (feature == 21)
    use_middle = (feature < 18) & ((turn == 1) | (turn == 4)) | (feature == 22)

    def factors(x, y, z, last):
        value = jnp.where(
            feature < 6, x, jnp.where(feature < 12, y, jnp.where(feature < 18, z, last))
        )
        top, middle, low = thirds(value)
        return jnp.where(use_top, top, jnp.where(use_middle, middle, low))

    def some_sources(index, carry):
        cells = [BATCH * index + k for k in range(BATCH)]
        rels = [comp_ref[REL, pl.ds(c, 1), :].astype(i32) for c in cells]
        hits = [
            (iota((160, WIDE), 0) == rel - 2 * PER_OWNER).astype(f32).astype(bf16) for rel in rels
        ]
        reaches = [dot(wanted_ref[...], hit) for hit in hits]
        for k, c in enumerate(cells):
            rel = rels[k]
            px = comp_ref[PX, pl.ds(c, 1), :] - (4 * (rel >> 5) + 2).astype(f32)
            py = comp_ref[PY, pl.ds(c, 1), :] - 4.0
            pz = comp_ref[PZ, pl.ds(c, 1), :] - 4.0
            fx, fy, fz = [comp_ref[FX + a, pl.ds(c, 1), :] for a in range(3)]
            square = (px * px + py * py) + (pz * pz + smooth_sq)
            along = (px * fx + py * fy) + pz * fz
            near_rows = factors(-2.0 * px, -2.0 * py, -2.0 * pz, square)
            near_rows = jnp.where((feature >= 18) & (feature < 21), 1.0, near_rows)
            push_rows = factors(fx, fy, fz, -along)
            push_rows = jnp.where((feature >= 18) & (feature < 21), 0.0, push_rows)
            mask_rows = FAR_AWAY - FAR_AWAY * reaches[k]
            rights_ref[c, :, 0:WIDE] = jnp.concatenate([near_rows, mask_rows], axis=0).astype(bf16)
            rights_ref[c, :, WIDE : 2 * WIDE] = jnp.concatenate(
                [push_rows, jnp.zeros((8 * CPD, WIDE), f32)], axis=0
            ).astype(bf16)
        return carry

    owners_ref[...] = jnp.broadcast_to(owner[0:8], (8, 128))

    def multiply_own(t, c, products):
        apart = owners_ref[pl.ds(c, 1), 0:1] - owners_ref[pl.ds(t, 1), 0:1]
        left = [lefts_ref[3 * t + w].astype(f32) for w in range(3)]
        left = jnp.where(apart < -0.5, left[0], jnp.where(apart > 0.5, left[2], left[1]))
        products[...] = dot(left.astype(bf16), rights_ref[c])

    def own_target(t, carry):
        for k in range(CPD // 2):
            multiply_own(t, 2 * k + 1, odd_pairs)
            add_pair(comp_ref, sums_ref, t, 2 * k, even_pairs)
            if k + 1 < CPD // 2:
                multiply_own(t, 2 * k + 2, even_pairs)
            else:
                multiply_own(jnp.minimum(t + 1, CPD - 1), 0, even_pairs)
            add_pair(comp_ref, sums_ref, t, 2 * k + 1, odd_pairs)
        return carry

    sums_ref[...] = jnp.zeros_like(sums_ref)
    rights_ref[DUMMY] = jnp.where(iota((DEPTH, 2 * WIDE), 0) == 21, FAR_AWAY, 0.0).astype(bf16)
    lax.fori_loop(0, 3, some_sources, 0)
    take_z((1, 2))
    lax.fori_loop(3, 5, some_sources, 0)
    own.wait()
    take_z(range(3, 8))
    lax.fori_loop(5, CELLS // BATCH, some_sources, 0)
    multiply_own(0, 0, even_pairs)
    lax.fori_loop(0, 2, own_target, 0)
    take_y(range(3))
    lax.fori_loop(2, 4, own_target, 0)
    take_y(range(3, 8))
    lax.fori_loop(4, CPD, own_target, 0)
    for copy in (*z_copies, *y_copies):
        copy.wait_send()
    for copy in c_copies:
        copy.wait()


def first(displacement, point_leaf, near_list, stiffness, surf, up_inverse):
    npoints = displacement.shape[1]
    sides = len(OFFSETS)
    dma = pltpu.SemaphoreType.DMA
    return pl.pallas_call(
        first_kernel,
        out_shape=(
            jax.ShapeDtypeStruct((10, 48, WIDE), f32),
            jax.ShapeDtypeStruct((8, 128), i32),
            jax.ShapeDtypeStruct((8, 8, 16, 128), f32),
            jax.ShapeDtypeStruct((3 * CPD, SHARE_PAD, DEPTH), bf16),
            jax.ShapeDtypeStruct((CPD, 3, SHARE_PAD, 128), f32),
            jax.ShapeDtypeStruct((CELLS + 1, DEPTH, 2 * WIDE), bf16),
            jax.ShapeDtypeStruct((CPD, 4, SHARE_PAD, 128), f32),
        ),
        in_specs=[HBM] * 6,
        out_specs=(VMEM,) * 7,
        scratch_shapes=[
            pltpu.VMEM((sides, 3, npoints), f32),
            pltpu.VMEM((sides, 1, npoints), i32),
            pltpu.VMEM((3, npoints), f32),
            pltpu.VMEM((EQUIV, 8), f32),
            pltpu.VMEM((1, npoints), i32),
            pltpu.VMEM((2, FAR, 128), i32),
            pltpu.VMEM((NPT, NPT), f32),
            pltpu.VMEM((ROWS, ROWS), f32),
            pltpu.VMEM((144, WIDE), f32),
            pltpu.VMEM((48, WIDE), i32),
            pltpu.VMEM((144, NPT), f32),
            pltpu.VMEM((FAR, 128), i32),
            pltpu.VMEM((160, 128), bf16),
            pltpu.VMEM((8 * CPD, 160), bf16),
            pltpu.VMEM((3, EQUIV, 128), f32),
            pltpu.VMEM((7, 16, WIDE), f32),
            pltpu.VMEM((ROWS, 3 * WIDE), bf16),
            pltpu.VMEM((ROWS, 3 * WIDE), bf16),
            pltpu.VMEM((PER_OWNER, 3 * WIDE), bf16),
            pltpu.VMEM((ROWS, PER_OWNER), f32),
            pltpu.VMEM((ROWS, PER_OWNER), f32),
            pltpu.VMEM((16, 128), f32),
            pltpu.VMEM((SHARE_PAD, 2 * WIDE), f32),
            pltpu.VMEM((SHARE_PAD, 2 * WIDE), f32),
            pltpu.VMEM((8, 128), f32),
            dma((sides,)),
            dma((sides,)),
            dma((sides,)),
            dma((sides,)),
            dma((7,)),
            dma,
            dma((7,)),
            dma((7,)),
            dma((24,)),
            dma((24,)),
            dma((32,)),
            dma((32,)),
        ],
        compiler_params=pltpu.CompilerParams(
            collective_id=0, has_side_effects=True, vmem_limit_bytes=LIMIT
        ),
        name="first",
    )(*(in_hbm(x) for x in (displacement, point_leaf, near_list, stiffness, surf, up_inverse)))


def near_kernel(lists, comp_ref, lefts, spots, rights, own_sums, out_ref, even_pairs, odd_pairs, sums):
    portion = lax.axis_index("leaf")

    def pair(index):
        code = lists[index >> 7, index & 127]
        return code >> 6, code & 63

    def multiply(index, products):
        t, c = pair(index)
        w = jnp.clip(lists[7, c] - lists[7, t] + 1, 0, 2)
        products[...] = dot(lefts[3 * t + w], rights[c])

    sums[...] = own_sums[...]
    multiply(0, even_pairs)

    def some_pairs(index, carry):
        for k in range(TOGETHER):
            now, after = (odd_pairs, even_pairs) if k % 2 else (even_pairs, odd_pairs)
            at = TOGETHER * index + k
            multiply(at + 1, after)
            add_pair(comp_ref, sums, *pair(at), now)
        return carry

    lax.fori_loop(0, (lists[2, 0] + (TOGETHER - 1)) // TOGETHER, some_pairs, 0)
    pick_row, pick_lane = iota((SHARE_PAD, WIDE), 0), iota((SHARE_PAD, WIDE), 1)
    pick = (pick_lane == pick_row + SHARE * portion) & (pick_row < SHARE)

    def finish(index, carry):
        for t in (2 * index, 2 * index + 1):
            for a in range(3):
                total = sums[t, a] + spots[t, a] * sums[t, 3]
                column = jnp.sum(total, axis=1, keepdims=True) * inv_eight_pi
                row = jnp.sum(jnp.where(pick, column, 0.0), axis=0, keepdims=True)
                out_ref[a, pl.ds(t, 1), :] = row
        return carry

    lax.fori_loop(0, CPD // 2, finish, 0)


def near_field(lists, comp, lefts, spots, rights, own_sums):
    return pl.pallas_call(
        near_kernel,
        out_shape=jax.ShapeDtypeStruct((3, 8, WIDE), f32),
        in_specs=[SMEM] + [VMEM] * 5,
        out_specs=VMEM,
        scratch_shapes=[
            pltpu.VMEM((SHARE_PAD, 2 * WIDE), f32),
            pltpu.VMEM((SHARE_PAD, 2 * WIDE), f32),
            pltpu.VMEM((CPD, 4, SHARE_PAD, 128), f32),
        ],
        compiler_params=pltpu.CompilerParams(vmem_limit_bytes=LIMIT),
        name="near_field",
    )(lists, comp, lefts, spots, rights, own_sums)


def far_part(
    left_ref,
    quarter_ref,
    gat_ref,
    far_ref,
    far_load,
    surf_ref,
    inverse_ref,
    local_ref,
    far4,
    sources,
    packed,
    pushes,
    mids,
    total,
    quarter,
    even_rows,
    odd_rows,
    even_blocks,
    odd_blocks,
):
    me = lax.axis_index("cells")
    portion = lax.axis_index("leaf")
    lane = iota((16, 128), 1)

    def one_tile(tile, carry):
        for half in range(2):
            rows = [jnp.zeros((16, 128), f32) for _ in range(3)]
            for v in range(4):
                at = 8 * tile + 4 * half + v
                value = gat_ref[at // 8, at - at // 8 * 8]
                for a in range(3):
                    shift = (PER_OWNER * (v - a)) % 128
                    moved = pltpu.roll(value, shift, 1) if shift else value
                    rows[a] = jnp.where(lane // PER_OWNER == v, moved, rows[a])
            top, low = halves(jnp.concatenate(rows, axis=0))
            packed[tile, 0:48, 128 * half : 128 * half + 128] = top
            packed[tile, 48:96, 128 * half : 128 * half + 128] = low
        return carry

    lax.fori_loop(0, 8, one_tile, 0)

    far_load.wait()
    entries = far_ref[...]
    mine = lax.rem(me, 4)
    lane48 = iota((FAR, 128), 1) // PER_OWNER
    picked = jnp.zeros((FAR, 128), i32)
    for place in range(4):
        moved = entries
        for k in range(1, 4):
            turned = pltpu.roll(entries, PER_OWNER * k, 1)
            moved = jnp.where(lax.rem(mine + k, 4) == place, turned, moved)
        far4[place] = moved
    for place in range(4):
        rows = far4[place, pl.ds(place, FAR // 4, stride=4), :]
        chosen = iota((FAR // 4, 128), 1) // PER_OWNER == place
        if place == 0:
            merged = rows
        else:
            merged = jnp.where(chosen, rows, merged)
    owner = merged >> 5
    spot = (((owner & 1) << 5) + (owner >> 1)) * PER_OWNER + (merged & 31)
    sources[0:12, :] = jnp.where(merged >= 0, spot, -1)
    target = me * PER_OWNER + (iota((12, 128), 1) & 31)
    mids[0, 0:12, :] = (2 * ((target >> 4) - (merged >> 4))).astype(f32)
    mids[1, 0:12, :] = (2 * (((target >> 2) & 3) - ((merged >> 2) & 3))).astype(f32)
    mids[2, 0:12, :] = (2 * ((target & 3) - (merged & 3))).astype(f32)

    def gather_two(index):
        first = sources[pl.ds(2 * index, 1), :]
        second = sources[pl.ds(2 * index + 1, 1), :]
        wanted = jnp.concatenate([first, second], axis=1)
        found = jnp.zeros((96, 256), f32)
        for tile in range(8):
            onehot = (iota((256, 256), 0) + 256 * tile == wanted).astype(f32).astype(bf16)
            found = found + dot(packed[tile], onehot)
        value = found[0:48] + found[48:96]
        pushes[2 * index] = value[:, 0:128]
        pushes[2 * index + 1] = value[:, 128:256]

    def some_gathers(index, carry):
        for k in range(3):
            gather_two(3 * index + k)
        return carry

    lax.fori_loop(0, 2, some_gathers, 0)
    total[...] = jnp.zeros_like(total)

    left = left_ref[...].astype(bf16)
    for a in range(3):
        quarter[a] = jnp.broadcast_to(quarter_ref[portion, :, a : a + 1], (16, 128))
    steps = thirds(jnp.full((16, 128), (inner_radius / 3.0) ** 2, f32))
    for rows in (even_rows, odd_rows):
        rows[...] = jnp.zeros_like(rows)
        for k in range(3):
            rows[pl.ds(12 + k, 16, stride=32), :] = steps[k]

    def prepare_block(index, rows, blocks):
        push = [pushes[index, 16 * a : 16 * a + 16, :] for a in range(3)]
        gap = [mids[a, pl.ds(index, 1), :] - quarter[a] for a in range(3)]
        square = (gap[0] * gap[0] + gap[1] * gap[1]) + (gap[2] * gap[2] + smooth_sq)
        inner = (gap[0] * push[0] + gap[1] * push[1]) + gap[2] * push[2]
        scale = inner_radius / 3.0
        for a in range(3):
            for k, third in enumerate(thirds((2.0 * scale) * gap[a])):
                rows[pl.ds(3 * a + k, 16, stride=32), :] = third
            for k, third in enumerate(thirds(scale * push[a])):
                rows[pl.ds(16 + 3 * a + k, 16, stride=32), :] = third
        for k, third in enumerate(thirds(square)):
            rows[pl.ds(9 + k, 16, stride=32), :] = third
        for k, third in enumerate(thirds(inner)):
            rows[pl.ds(25 + k, 16, stride=32), :] = third
        for j in range(14):
            right = jnp.concatenate(
                [rows[32 * j : 32 * j + 16, :], rows[32 * j + 16 : 32 * j + 32, :]], axis=1
            )
            blocks[j] = dot(left, right.astype(bf16))

    def add_block(index, blocks):
        groups = EQUIV // 8
        sums = [[jnp.zeros((8, 128), f32) for _ in range(4)] for _ in range(groups)]
        for j in range(14):
            f = [pushes[index, 16 * a + j : 16 * a + j + 1, :] for a in range(3)]
            shift = [quarter[a, j : j + 1, :] for a in range(3)]
            for g in range(groups):
                at = slice(8 * g, 8 * g + 8)
                shifted = blocks[j, at, 0:128]
                inner = blocks[j, at, 128:256]
                root = lax.rsqrt(shifted)
                cube = root * root * root
                even = root + smooth_sq * cube
                along = cube * inner
                for a in range(3):
                    sums[g][a] = sums[g][a] + (even * f[a] - along * shift[a])
                sums[g][3] = sums[g][3] + along
        mid = [mids[a, pl.ds(index, 1), :] for a in range(3)]
        for g in range(groups):
            at = slice(8 * g, 8 * g + 8)
            for a in range(3):
                check = mid[a] + inner_radius * surf_ref[at, a : a + 1]
                row = EQUIV * a + 8 * g
                total[row : row + 8, :] += sums[g][a] + check * sums[g][3]

    prepare_block(0, even_rows, even_blocks)

    def two_blocks(index, carry):
        prepare_block(2 * index + 1, odd_rows, odd_blocks)
        add_block(2 * index, even_blocks)
        prepare_block(jnp.minimum(2 * index + 2, 11), even_rows, even_blocks)
        add_block(2 * index + 1, odd_blocks)
        return carry

    lax.fori_loop(0, 6, two_blocks, 0)
    value = total[...] * inv_eight_pi
    value = value + pltpu.roll(value, 64, 1)
    value = value + pltpu.roll(value, 32, 1)
    local_ref[...] = dot_wide(inverse_ref[...], value)


def last_kernel(
    left_ref,
    quarter_ref,
    gat_ref,
    far_hbm,
    surf_ref,
    inverse_ref,
    comp_ref,
    near_ref,
    out_ref,
    far_ref,
    load_sem,
    far4,
    sources,
    packed,
    pushes,
    mids,
    total,
    quarter,
    even_rows,
    odd_rows,
    even_blocks,
    odd_blocks,
    local_ref,
    packed_local,
    held_local,
    factors,
    spread_ref,
    cell_ref,
    part_ref,
    held_part,
    send_local,
    recv_local,
    send_part,
    recv_part,
):
    block = pl.multiple_of(lax.axis_index("cells") // 4 * 128, 128)
    far_load = pltpu.make_async_copy(far_hbm.at[:, pl.ds(block, 128)], far_ref, load_sem)
    far_load.start()
    packed_local[...] = jnp.zeros_like(packed_local)
    sides = beside("cells", (1, -1))
    mates = beside("leaf", (1, 2, 3))
    barrier = pltpu.get_barrier_semaphore()
    for target in (*sides, *mates):
        pl.semaphore_signal(barrier, inc=1, device_id=target, device_id_type=MESH)
    far_part(
        left_ref,
        quarter_ref,
        gat_ref,
        far_ref,
        far_load,
        surf_ref,
        inverse_ref,
        local_ref,
        far4,
        sources,
        packed,
        pushes,
        mids,
        total,
        quarter,
        even_rows,
        odd_rows,
        even_blocks,
        odd_blocks,
    )
    pl.semaphore_wait(barrier, 5)
    lane = iota((48, 128), 1) // PER_OWNER
    for k in range(4):
        rows = min(48, ROWS - 48 * k)
        piece = local_ref[48 * k : 48 * k + rows, :]
        here = lane[0:rows] == k
        packed_local[0:rows, :] = jnp.where(here, piece, packed_local[0:rows, :])
    copies = [
        remote(packed_local, held_local.at[k], send_local.at[k], recv_local.at[k], target)
        for k, target in enumerate(sides)
    ]
    for copy in copies:
        copy.start()
    for copy in copies:
        copy.wait()
    lane = iota((48, 128), 1) // PER_OWNER
    for k in range(4):
        rows = min(48, ROWS - 48 * k)
        value = local_ref[48 * k : 48 * k + rows, :]
        for side in range(2):
            place = 2 * side
            moved = held_local[side, 0:rows, :]
            if place != k:
                moved = pltpu.roll(moved, (PER_OWNER * (place - k)) % 128, 1)
            value = jnp.where(lane[0:rows] == place, moved, value)
        top, low = halves(value)
        factors[48 * k : 48 * k + rows, 0:128] = top
        factors[48 * k : 48 * k + rows, 128:256] = low

    def spread_out(t):
        rel = comp_ref[REL, pl.ds(t, 1), :].astype(i32) - 3 * PER_OWNER
        member = (iota((128, WIDE), 0) == rel).astype(f32).astype(bf16)
        spread_ref[t] = dot(factors[...], jnp.concatenate([member, member], axis=0))

    def three_cells(index, carry):
        for k in range(3):
            spread_out(3 * index + k)
        return carry

    lax.fori_loop(0, 2, three_cells, 0)

    def one_cell(t):
        d = [comp_ref[DX + a, pl.ds(t, 1), :] for a in range(3)]
        sums = [jnp.zeros((8, WIDE), f32) for _ in range(3)]
        for g in range(EQUIV // 8):
            at = slice(8 * g, 8 * g + 8)
            r = [d[a] - outer_radius * surf_ref[at, a : a + 1] for a in range(3)]
            f = [spread_ref[t, EQUIV * a + 8 * g : EQUIV * a + 8 * g + 8, :] for a in range(3)]
            even, along = pull(r, f)
            sums = [sums[a] + (even * f[a] + along * r[a]) for a in range(3)]
        for a in range(3):
            row = jnp.sum(sums[a], axis=0, keepdims=True) * inv_eight_pi
            cell_ref[a, pl.ds(t, 1), :] = row + near_ref[a, pl.ds(t, 1), :]

    def two_cells(index, carry):
        one_cell(2 * index)
        one_cell(2 * index + 1)
        return carry

    lax.fori_loop(0, CPD // 2, two_cells, 0)
    for t in range(CPD):
        for a in range(3):
            part_ref[a : a + 1, NPT * t : NPT * (t + 1)] = cell_ref[a, t : t + 1, 0:NPT]
    copies = [
        remote(part_ref, held_part.at[k], send_part.at[k], recv_part.at[k], target)
        for k, target in enumerate(mates)
    ]
    for copy in copies:
        copy.start()
    for copy in copies:
        copy.wait()
    out_ref[...] = (part_ref[...] + held_part[1]) + (held_part[0] + held_part[2])


def last(left, quarter, gathered, far_list, surf, down_inverse, comp, near, npoints):
    dma = pltpu.SemaphoreType.DMA
    return pl.pallas_call(
        last_kernel,
        out_shape=jax.ShapeDtypeStruct((3, npoints), f32),
        in_specs=[VMEM, VMEM, VMEM, HBM] + [VMEM] * 4,
        out_specs=VMEM,
        scratch_shapes=[
            pltpu.VMEM((FAR, 128), i32),
            dma,
            pltpu.VMEM((4, FAR, 128), i32),
            pltpu.VMEM((16, 128), i32),
            pltpu.VMEM((8, 96, 256), bf16),
            pltpu.VMEM((12, FAR, 128), f32),
            pltpu.VMEM((3, 16, 128), f32),
            pltpu.VMEM((ROWS, 128), f32),
            pltpu.VMEM((3, 16, 128), f32),
            pltpu.VMEM((512, 128), f32),
            pltpu.VMEM((512, 128), f32),
            pltpu.VMEM((14, EQUIV, 256), f32),
            pltpu.VMEM((14, EQUIV, 256), f32),
            pltpu.VMEM((ROWS, 128), f32),
            pltpu.VMEM((48, 128), f32),
            pltpu.VMEM((2, 48, 128), f32),
            pltpu.VMEM((ROWS, 256), bf16),
            pltpu.VMEM((CPD, ROWS, WIDE), f32),
            pltpu.VMEM((3, 8, WIDE), f32),
            pltpu.VMEM((3, npoints), f32),
            pltpu.VMEM((3, 3, npoints), f32),
            dma((2,)),
            dma((2,)),
            dma((3,)),
            dma((3,)),
        ],
        compiler_params=pltpu.CompilerParams(
            collective_id=1, has_side_effects=True, vmem_limit_bytes=LIMIT
        ),
        name="last",
    )(left, quarter, gathered, in_hbm(far_list), surf, down_inverse, comp, near)


def body(displacement, point_leaf, near_list, far_list, stiffness, up_inverse, down_inverse):
    table = surface_table()
    surf = jnp.asarray(np.pad(table, ((0, 0), (0, 5))))
    whole = np.round(3.0 * table)
    ones = np.ones((EQUIV, 3), np.float32)
    square = np.sum(whole * whole, axis=1, keepdims=True)
    left = np.concatenate([np.repeat(whole, 3, axis=1), ones, ones * square, 0.0 * square], axis=1)
    left = jnp.asarray(left.astype(np.float32))
    quarter = inner_radius * table.reshape(4, 14, 3)
    quarter = jnp.asarray(np.pad(quarter, ((0, 0), (0, 2), (0, 5))).astype(np.float32))
    comp, lists, gathered, lefts, spots, rights, own_sums = first(
        displacement, point_leaf, near_list, stiffness, surf, up_inverse
    )
    near = near_field(lists, comp, lefts, spots, rights, own_sums)
    return last(
        left, quarter, gathered, far_list, surf, down_inverse, comp, near, displacement.shape[1]
    )


def solution(mesh):
    in_specs = (P(None, "cells"), P("cells"), P(), P(), P(), P(), P())
    out_specs = P(None, "cells")
    return jax.shard_map(body, mesh=mesh, in_specs=in_specs, out_specs=out_specs, check_vma=False)
```

```python
import math

import jax
import jax.numpy as jnp
import numpy as np
from jax import lax
from jax.experimental import pallas as pl
from jax.experimental.pallas import tpu as pltpu
from jax.sharding import PartitionSpec as P

NPT = 312
CPD = 6
SLICE = 16
EQUIV = 56
FAR = 48
ROWS = 3 * EQUIV
PER_OWNER = 2 * SLICE
WIDE = 384
OFFSETS = (1, -1, 2, -2, 3, -3)
CELLS = CPD * (len(OFFSETS) + 1)
OWNABLE = 3 * CPD
SHARE = NPT // 4
SHARE_PAD = 80

inv_eight_pi = 1.0 / (8.0 * math.pi)
smooth_sq = 0.0625
inner_radius = 1.05
outer_radius = 2.95
MESH = pl.DeviceIdType.MESH
VMEM = pl.BlockSpec(memory_space=pltpu.VMEM)
SMEM = pl.BlockSpec(memory_space=pltpu.SMEM)
f32 = jnp.float32
bf16 = jnp.bfloat16
i32 = jnp.int32


def surface_table():
    ladder = [-1.0, -1.0 / 3.0, 1.0 / 3.0, 1.0]
    corners = [
        (a, b, c)
        for a in ladder
        for b in ladder
        for c in ladder
        if max(abs(a), abs(b), abs(c)) == 1.0
    ]
    return np.array(corners, dtype=np.float32)


def iota(shape, dim):
    return lax.broadcasted_iota(i32, shape, dim)


def dot(a, b):
    return jnp.dot(a, b, preferred_element_type=f32)


def dot_nt(a, b):
    return lax.dot_general(a, b, (((1,), (1,)), ((), ())), preferred_element_type=f32)


def halves(value):
    top = value.astype(bf16)
    return top, (value - top.astype(f32)).astype(bf16)


def dot_wide(a, b):
    a_top, a_low = halves(a)
    b_top, b_low = halves(b)
    return dot(a_top, b_top) + (dot(a_top, b_low) + dot(a_low, b_top))


DX, DY, DZ, FX, FY, FZ, PX, PY, PZ, REL = range(10)
FEATURES = 24
DEPTH = FEATURES + 8 * CPD
FAR_AWAY = 1e30
LIMIT = 20 << 20
HBM = pl.BlockSpec(memory_space=pltpu.HBM)
DUMMY = CELLS
TOGETHER = 6
BATCH = 6
PARTS = 2
STEPS = (0, 1, 7, 2, 6, 3, 5, 4)


def thirds(value):
    top = value.astype(bf16).astype(f32)
    rest = value - top
    middle = rest.astype(bf16).astype(f32)
    return top, middle, rest - middle


def pull(offset, strength):
    dx, dy, dz = offset
    fx, fy, fz = strength
    shifted = (dx * dx + dy * dy) + (dz * dz + smooth_sq)
    inner = (dx * fx + dy * fy) + dz * fz
    root = lax.rsqrt(shifted)
    cube = root * root * root
    return root + smooth_sq * cube, cube * inner


def in_hbm(array):
    return pltpu.with_memory_space_constraint(array, pltpu.HBM)


def remote(src, dst, send_sem, recv_sem, target):
    return pltpu.make_async_remote_copy(
        src_ref=src,
        dst_ref=dst,
        send_sem=send_sem,
        recv_sem=recv_sem,
        device_id=target,
        device_id_type=MESH,
    )


def greet(targets):
    barrier = pltpu.get_barrier_semaphore()
    for target in targets:
        pl.semaphore_signal(barrier, inc=1, device_id=target, device_id_type=MESH)
    pl.semaphore_wait(barrier, len(targets))


def beside(axis, offsets):
    count = lax.axis_size(axis)
    me = lax.axis_index(axis)
    return [{axis: lax.rem(me + (off + count), count)} for off in offsets]


def add_pair(comp_ref, sums, t, c, products):
    p = [comp_ref[PX + a, pl.ds(c, 1), :] for a in range(3)]
    f = [comp_ref[FX + a, pl.ds(c, 1), :] for a in range(3)]
    for part in range(PARTS):
        groups = range(part * 10 // PARTS, (part + 1) * 10 // PARTS)
        added = {}
        for b in range(WIDE // 128):
            lanes = slice(128 * b, 128 * b + 128)
            pb = [value[:, lanes] for value in p]
            fb = [value[:, lanes] for value in f]
            for g in groups:
                at = slice(8 * g, 8 * g + 8)
                shifted = products[at, lanes]
                inner = products[at, WIDE + 128 * b : WIDE + 128 * b + 128]
                root = lax.rsqrt(shifted)
                cube = root * root * root
                even = root + smooth_sq * cube
                along = cube * inner
                one = [even * fb[a] - along * pb[a] for a in range(3)] + [along]
                added[g] = [u + v for u, v in zip(added[g], one)] if b else one
        for g in groups:
            at = slice(8 * g, 8 * g + 8)
            for a in range(4):
                sums[t, a, at, :] += added[g][a]


def first_kernel(
    disp_hbm,
    leaf_hbm,
    near_hbm,
    stiff_hbm,
    surf_hbm,
    inverse_hbm,
    comp_ref,
    lists_ref,
    gat_ref,
    lefts_ref,
    spots_ref,
    rights_ref,
    sums_ref,
    held_disp,
    held_leaf,
    disp_ref,
    surf_ref,
    leaf_ref,
    near_ref,
    stiff_ref,
    inverse_ref,
    disp,
    leaves,
    force,
    listed_ref,
    relation,
    wanted_ref,
    wide,
    owned_ref,
    terms_top,
    terms_low,
    member_ref,
    total,
    density,
    block_ref,
    even_pairs,
    odd_pairs,
    owners_ref,
    send_disp,
    recv_disp,
    send_leaf,
    recv_leaf,
    load_sem,
    own_sem,
    z_send,
    z_recv,
    y_send,
    y_recv,
    c_send,
    c_recv,
):
    me = lax.axis_index("cells")
    portion = lax.axis_index("leaf")
    start = lax.rem(me + 63, 64)
    block = start // 4
    leaf_load = pltpu.make_async_copy(leaf_hbm, leaf_ref.at[0], load_sem.at[0])
    loads = [
        pltpu.make_async_copy(
            near_hbm.at[:, pl.ds(pl.multiple_of(lax.rem(block + k, 16) * 128, 128), 128)],
            near_ref.at[k],
            load_sem.at[1 + k],
        )
        for k in range(2)
    ]
    loads.append(pltpu.make_async_copy(stiff_hbm, stiff_ref, load_sem.at[3]))
    loads.append(pltpu.make_async_copy(inverse_hbm, inverse_ref, load_sem.at[4]))
    loads.append(pltpu.make_async_copy(surf_hbm, surf_ref, load_sem.at[5]))
    disp_load = pltpu.make_async_copy(disp_hbm, disp_ref, load_sem.at[6])
    disp_load.start()
    leaf_load.start()
    for load in loads:
        load.start()
    core = lax.rem(me, 2)
    z = lax.rem(me // 2, 8)
    y = me // 16

    def device(y_at, z_at, core_at):
        return {"cells": (y_at * 8 + z_at) * 2 + core_at}

    sides = beside("cells", OFFSETS)
    z_targets = [device(y, lax.rem(z + k, 8), core) for k in range(1, 8)]
    y_targets = [device(lax.rem(y + k, 4), z, core) for k in range(1, 4)]
    c_target = device(y, z, 1 - core)
    greet([*sides, *z_targets, *y_targets, c_target])
    disp_load.wait()
    leaf_load.wait()
    copies = []
    for slot, target in enumerate(sides):
        copies.append(
            remote(disp_ref, held_disp.at[slot], send_disp.at[slot], recv_disp.at[slot], target)
        )
        copies.append(
            remote(leaf_ref, held_leaf.at[slot], send_leaf.at[slot], recv_leaf.at[slot], target)
        )
    for copy in copies:
        copy.start()

    comp_ref[...] = jnp.zeros_like(comp_ref)
    disp[...] = jnp.zeros_like(disp)
    leaves[...] = jnp.zeros_like(leaves)

    def place_cells(home, points, leaf_row):
        for k in range(CPD):
            at = slice(NPT * k, NPT * (k + 1))
            row = home * CPD + k
            for a in range(3):
                disp[48 * a + row : 48 * a + row + 1, 0:NPT] = points[a : a + 1, at]
            leaves[row : row + 1, 0:NPT] = leaf_row[:, at]

    def fill_table(rows):
        live = iota((rows, WIDE), 1) < NPT
        rel = jnp.where(live, (leaves[0:rows, :] - PER_OWNER * (me - 4)) & 2047, -1)
        for a in range(3):
            comp_ref[DX + a, 0:rows, :] = disp[48 * a : 48 * a + rows, :]
        comp_ref[REL, 0:rows, :] = rel.astype(f32)
        comp_ref[PX, 0:rows, :] = comp_ref[DX, 0:rows, :] + (2 * (rel >> 4) + 1).astype(f32)
        comp_ref[PY, 0:rows, :] = comp_ref[DY, 0:rows, :] + (2 * ((rel >> 2) & 3) + 1).astype(f32)
        comp_ref[PZ, 0:rows, :] = comp_ref[DZ, 0:rows, :] + (2 * (rel & 3) + 1).astype(f32)
        relf = rel.astype(f32)
        first = jnp.min(jnp.where(live, relf, 1e9), axis=1, keepdims=True)
        last = jnp.max(relf, axis=1, keepdims=True)
        return first, last

    place_cells(0, disp_ref[...], leaf_ref[...])
    first, last = fill_table(8)

    for load in loads:
        load.wait()
    both = jnp.concatenate([near_ref[0], near_ref[1]], axis=1)
    listed = both[:, 0:128]
    for k in range(1, 4):
        listed = jnp.where(lax.rem(start, 4) == k, both[:, 32 * k : 32 * k + 128], listed)
    listed_ref[...] = jnp.where(listed >= 0, (listed - PER_OWNER * (me - 2)) & 2047, -1)
    source_leaf = iota((160, 128), 0)

    def eight_entries(index, near):
        rows = listed_ref[pl.ds(pl.multiple_of(8 * index, 8), 8), :]
        for k in range(8):
            near = near + jnp.where(rows[k : k + 1, :] == source_leaf, 1.0, 0.0)
        return near

    near = lax.fori_loop(0, 6, eight_entries, jnp.zeros((160, 128), f32))
    relation[...] = near.astype(bf16)
    row8, lane8 = iota((8, 128), 0).astype(f32), iota((8, 128), 1).astype(f32)
    leaf_rows = [
        jnp.where((lane8 == first[t : t + 1] - 3.0 * PER_OWNER + row8) & (row8 < 3.0), 1.0, 0.0)
        for t in range(CPD)
    ]
    wanted_ref[...] = dot_nt(
        jnp.concatenate(leaf_rows, axis=0).astype(bf16), relation[...]
    ).astype(bf16)

    pick_row, pick_lane = iota((SHARE_PAD, WIDE), 0), iota((SHARE_PAD, WIDE), 1)
    pick16 = ((pick_lane == pick_row + SHARE * portion) & (pick_row < SHARE)).astype(f32).astype(bf16)
    slot = iota((SHARE_PAD, 128), 1)
    slot_turn = lax.rem(slot, 6)
    left_first = (slot < 18) & (slot_turn < 3) | (slot == 18)
    left_second = (slot < 18) & (slot_turn >= 3) & (slot_turn < 5) | (slot == 19)
    row32 = iota((32, WIDE), 0)

    def one_own(t):
        rel = comp_ref[REL, pl.ds(t, 1), :]
        px, py, pz = [comp_ref[PX + a, pl.ds(t, 1), :] for a in range(3)]
        lowest = jnp.min(jnp.where(rel >= 0.0, rel, 1e9), axis=1, keepdims=True)
        owner = jnp.floor(lowest * (1.0 / PER_OWNER))
        py4, pz4 = py - 4.0, pz - 4.0
        rows = []
        for w in range(3):
            px4 = px - (4.0 * (owner + float(w - 1)) + 2.0)
            square = (px4 * px4 + py4 * py4) + pz4 * pz4
            rows.append(
                jnp.where(
                    row32 < 6,
                    px4,
                    jnp.where(row32 < 12, py4, jnp.where(row32 < 18, pz4, square)),
                )
            )
        place = jnp.where(row32 == 0, px, jnp.where(row32 == 1, py, jnp.where(row32 == 2, pz, rel)))
        top, middle, low = thirds(jnp.concatenate([*rows, place], axis=0))
        found = dot_nt(pick16, top.astype(bf16)) + (
            dot_nt(pick16, middle.astype(bf16)) + dot_nt(pick16, low.astype(bf16))
        )
        for a in range(3):
            spots_ref[t, a] = jnp.broadcast_to(found[:, 96 + a : 97 + a], (SHARE_PAD, 128))
        leaf_at = (found[:, 99:100] - lowest).astype(i32)
        matched = (slot - (FEATURES + 8 * t) == leaf_at) & (leaf_at >= 0) & (leaf_at < 3)
        for w in range(3):
            value = pltpu.roll(found, 128 - 32 * w, 1) if w else found
            top, middle, low = thirds(value)
            chosen = jnp.where(left_first, top, jnp.where(left_second, middle, low))
            chosen = jnp.where((slot >= 21) & (slot < 24), 1.0, chosen)
            chosen = jnp.where(slot >= FEATURES, jnp.where(matched, 1.0, 0.0), chosen)
            lefts_ref[3 * t + w] = chosen[:, 0:DEPTH].astype(bf16)

    def two_own(index, carry):
        one_own(2 * index)
        one_own(2 * index + 1)
        return carry

    lax.fori_loop(0, CPD // 2, two_own, 0)
    for a in range(3):
        wide[a] = jnp.broadcast_to(outer_radius * surf_ref[:, a : a + 1], (EQUIV, 128))

    for copy in copies:
        copy.wait()
    for home in range(1, len(OFFSETS) + 1):
        place_cells(home, held_disp[home - 1], held_leaf[home - 1])
    first, last = fill_table(48)
    force[...] = dot_wide(disp[0:144, 0:NPT], stiff_ref[...])
    for a in range(3):
        comp_ref[FX + a, 0:48, 0:NPT] = force[48 * a : 48 * a + 48, :]

    cell = iota((48, 1), 0)
    mine = (jnp.floor(first * (1.0 / PER_OWNER)) == 4.0) & (cell < OWNABLE)
    mine = jnp.where(mine, 1.0, 0.0)
    before = (iota((48, 48), 0) > iota((48, 48), 1)).astype(f32)
    rank = dot(before, jnp.broadcast_to(mine, (48, 128)))
    chosen = jnp.where((rank == iota((48, 128), 1).astype(f32)) & (mine > 0.0), 1.0, 0.0)
    chosen = jnp.concatenate([chosen] * 3, axis=0).astype(bf16)
    for k, part in enumerate((DX, DY, DZ, FX, FY, FZ, REL)):
        pieces = jnp.concatenate(thirds(comp_ref[part]), axis=0).astype(bf16)
        found = lax.dot_general(
            chosen, pieces, (((0,), (0,)), ((), ())), preferred_element_type=f32
        )
        owned_ref[k] = found[0:16]
    total[...] = jnp.zeros_like(total)

    def one_home(home, carry):
        for k in range(3):
            c = 3 * home + k
            d = [owned_ref[a, pl.ds(c, 1), :] for a in range(3)]
            f = [owned_ref[3 + a, pl.ds(c, 1), :] for a in range(3)]
            rel = owned_ref[6, pl.ds(c, 1), :].astype(i32) - 4 * PER_OWNER
            member = (iota((PER_OWNER, WIDE), 0) == rel).astype(f32).astype(bf16)
            member_ref[:, WIDE * k : WIDE * (k + 1)] = member
            for b in range(WIDE // 128):
                lanes = slice(128 * b, 128 * b + 128)
                out = slice(WIDE * k + 128 * b, WIDE * k + 128 * b + 128)
                for g in range(EQUIV // 8):
                    at = slice(8 * g, 8 * g + 8)
                    r = [wide[a, at, :] - d[a][:, lanes] for a in range(3)]
                    fb = [f[a][:, lanes] for a in range(3)]
                    even, along = pull(r, fb)
                    for a in range(3):
                        row = EQUIV * a + 8 * g
                        top, low = halves(even * fb[a] + along * r[a])
                        terms_top[row : row + 8, out] = top
                        terms_low[row : row + 8, out] = low
        total[...] += dot_nt(terms_top[...], member_ref[...]) + dot_nt(terms_low[...], member_ref[...])
        return carry

    lax.fori_loop(0, 3, one_home, 0)
    density[...] = dot_wide(inverse_ref[...], total[...] * inv_eight_pi)
    block_ref[...] = jnp.zeros_like(block_ref)
    for part in range(4):

        @pl.when(portion == part)
        def _():
            for a in range(3):
                rows = density[EQUIV * a + 14 * part : EQUIV * a + 14 * part + 14, :]
                block_ref[0:14, PER_OWNER * a : PER_OWNER * (a + 1)] = rows

    row = core * 4 + y
    own = pltpu.make_async_copy(block_ref, gat_ref.at[row, z], own_sem)
    own.start()
    z_copies = [
        remote(block_ref, gat_ref.at[row, z], z_send.at[k], z_recv.at[k], target)
        for k, target in enumerate(z_targets)
    ]
    for copy in z_copies:
        copy.start()
    y_copies, c_copies = [], []

    def send_along_y(source, where, order):
        for side, target in enumerate(y_targets):
            index = 3 * order + side
            copy = remote(source, gat_ref.at[row, where], y_send.at[index], y_recv.at[index], target)
            copy.start()
            y_copies.append(copy)

    def pass_on(source, at, where, index):
        copy = remote(source, gat_ref.at[at, where], c_send.at[index], c_recv.at[index], c_target)
        copy.start()
        c_copies.append(copy)

    def take_z(orders):
        for order in orders:
            k = STEPS[order]
            where = lax.rem(z - k + 8, 8)
            z_copies[k - 1].wait_recv()
            place = gat_ref.at[row, where]
            send_along_y(place, where, order)
            pass_on(place, row, where, order)

    def take_y(orders):
        for order in orders:
            where = lax.rem(z - STEPS[order] + 8, 8)
            for side in range(3):
                index = 3 * order + side
                y_copies[index].wait_recv()
                at = core * 4 + lax.rem(y - side + 3, 4)
                pass_on(gat_ref.at[at, where], at, where, 8 + index)

    send_along_y(block_ref, z, 0)
    pass_on(block_ref, row, z, 0)

    low = jnp.floor(first * (1.0 / 16.0))
    high = jnp.floor(last * (1.0 / 16.0))
    lane = iota((48, 128), 1)
    which = iota((48, 1), 0).astype(f32)
    real = (which < float(CELLS)) & (which >= float(CPD))
    flags = []
    for t in range(CPD):
        low_t, high_t = low[t : t + 1], high[t : t + 1]
        flags.append(jnp.where((high >= low_t - 1.0) & (low <= high_t + 1.0) & real, 1.0, 0.0))
    owner = jnp.floor(low * 0.5)
    table = jnp.zeros((48, 128), f32)
    for t, flag in enumerate(flags):
        table = table + jnp.where(lane == t, flag, 0.0)
    rank = dot(before, table)
    count = jnp.sum(table, axis=0, keepdims=True)
    lane_row = iota((1, 128), 1).astype(f32)
    lists_ref[...] = jnp.zeros_like(lists_ref)
    lines = [jnp.zeros((1, 128), f32) for _ in range(2)]
    ahead = jnp.zeros((1, 1), f32)
    for t, flag in enumerate(flags):
        spot = rank[:, t : t + 1] + ahead
        for half in range(2):
            hit = (spot == lane.astype(f32) + 128.0 * half) & (flag > 0.0)
            lines[half] = lines[half] + jnp.sum(
                jnp.where(hit, which + 64.0 * t, 0.0), axis=0, keepdims=True
            )
        ahead = ahead + count[:, t : t + 1]
    for half in range(2):
        line = jnp.where(lane_row + 128.0 * half >= ahead, float(DUMMY), lines[half])
        lists_ref[half : half + 1, :] = line.astype(i32)
    lists_ref[2:3, :] = jnp.broadcast_to(ahead, (1, 128)).astype(i32)
    square = iota((48, 128), 0) == lane
    line = jnp.sum(jnp.where(square, owner, 0.0), axis=0, keepdims=True)
    lists_ref[7:8, :] = line.astype(i32)

    feature = iota((FEATURES, WIDE), 0)
    turn = lax.rem(feature, 6)
    use_top = (feature < 18) & ((turn == 0) | (turn == 3) | (turn == 5)) | (feature == 21)
    use_middle = (feature < 18) & ((turn == 1) | (turn == 4)) | (feature == 22)

    def factors(x, y, z, last):
        value = jnp.where(
            feature < 6, x, jnp.where(feature < 12, y, jnp.where(feature < 18, z, last))
        )
        top, middle, low = thirds(value)
        return jnp.where(use_top, top, jnp.where(use_middle, middle, low))

    def some_sources(index, carry):
        cells = [BATCH * index + k for k in range(BATCH)]
        rels = [comp_ref[REL, pl.ds(c, 1), :].astype(i32) for c in cells]
        hits = [
            (iota((160, WIDE), 0) == rel - 2 * PER_OWNER).astype(f32).astype(bf16) for rel in rels
        ]
        reaches = [dot(wanted_ref[...], hit) for hit in hits]
        for k, c in enumerate(cells):
            rel = rels[k]
            px = comp_ref[PX, pl.ds(c, 1), :] - (4 * (rel >> 5) + 2).astype(f32)
            py = comp_ref[PY, pl.ds(c, 1), :] - 4.0
            pz = comp_ref[PZ, pl.ds(c, 1), :] - 4.0
            fx, fy, fz = [comp_ref[FX + a, pl.ds(c, 1), :] for a in range(3)]
            square = (px * px + py * py) + (pz * pz + smooth_sq)
            along = (px * fx + py * fy) + pz * fz
            near_rows = factors(-2.0 * px, -2.0 * py, -2.0 * pz, square)
            near_rows = jnp.where((feature >= 18) & (feature < 21), 1.0, near_rows)
            push_rows = factors(fx, fy, fz, -along)
            push_rows = jnp.where((feature >= 18) & (feature < 21), 0.0, push_rows)
            mask_rows = FAR_AWAY - FAR_AWAY * reaches[k]
            rights_ref[c, :, 0:WIDE] = jnp.concatenate([near_rows, mask_rows], axis=0).astype(bf16)
            rights_ref[c, :, WIDE : 2 * WIDE] = jnp.concatenate(
                [push_rows, jnp.zeros((8 * CPD, WIDE), f32)], axis=0
            ).astype(bf16)
        return carry

    owners_ref[...] = jnp.broadcast_to(owner[0:8], (8, 128))

    def multiply_own(t, c, products):
        apart = owners_ref[pl.ds(c, 1), 0:1] - owners_ref[pl.ds(t, 1), 0:1]
        left = [lefts_ref[3 * t + w].astype(f32) for w in range(3)]
        left = jnp.where(apart < -0.5, left[0], jnp.where(apart > 0.5, left[2], left[1]))
        products[...] = dot(left.astype(bf16), rights_ref[c])

    def own_target(t, carry):
        for k in range(CPD // 2):
            multiply_own(t, 2 * k + 1, odd_pairs)
            add_pair(comp_ref, sums_ref, t, 2 * k, even_pairs)
            if k + 1 < CPD // 2:
                multiply_own(t, 2 * k + 2, even_pairs)
            else:
                multiply_own(jnp.minimum(t + 1, CPD - 1), 0, even_pairs)
            add_pair(comp_ref, sums_ref, t, 2 * k + 1, odd_pairs)
        return carry

    sums_ref[...] = jnp.zeros_like(sums_ref)
    rights_ref[DUMMY] = jnp.where(iota((DEPTH, 2 * WIDE), 0) == 21, FAR_AWAY, 0.0).astype(bf16)
    lax.fori_loop(0, 3, some_sources, 0)
    take_z((1, 2))
    lax.fori_loop(3, 5, some_sources, 0)
    own.wait()
    take_z(range(3, 8))
    lax.fori_loop(5, CELLS // BATCH, some_sources, 0)
    multiply_own(0, 0, even_pairs)
    lax.fori_loop(0, 2, own_target, 0)
    take_y(range(3))
    lax.fori_loop(2, 4, own_target, 0)
    take_y(range(3, 8))
    lax.fori_loop(4, CPD, own_target, 0)
    for copy in (*z_copies, *y_copies):
        copy.wait_send()
    for copy in c_copies:
        copy.wait()


def first(displacement, point_leaf, near_list, stiffness, surf, up_inverse):
    npoints = displacement.shape[1]
    sides = len(OFFSETS)
    dma = pltpu.SemaphoreType.DMA
    return pl.pallas_call(
        first_kernel,
        out_shape=(
            jax.ShapeDtypeStruct((10, 48, WIDE), f32),
            jax.ShapeDtypeStruct((8, 128), i32),
            jax.ShapeDtypeStruct((8, 8, 16, 128), f32),
            jax.ShapeDtypeStruct((3 * CPD, SHARE_PAD, DEPTH), bf16),
            jax.ShapeDtypeStruct((CPD, 3, SHARE_PAD, 128), f32),
            jax.ShapeDtypeStruct((CELLS + 1, DEPTH, 2 * WIDE), bf16),
            jax.ShapeDtypeStruct((CPD, 4, SHARE_PAD, 128), f32),
        ),
        in_specs=[HBM] * 6,
        out_specs=(VMEM,) * 7,
        scratch_shapes=[
            pltpu.VMEM((sides, 3, npoints), f32),
            pltpu.VMEM((sides, 1, npoints), i32),
            pltpu.VMEM((3, npoints), f32),
            pltpu.VMEM((EQUIV, 8), f32),
            pltpu.VMEM((1, npoints), i32),
            pltpu.VMEM((2, FAR, 128), i32),
            pltpu.VMEM((NPT, NPT), f32),
            pltpu.VMEM((ROWS, ROWS), f32),
            pltpu.VMEM((144, WIDE), f32),
            pltpu.VMEM((48, WIDE), i32),
            pltpu.VMEM((144, NPT), f32),
            pltpu.VMEM((FAR, 128), i32),
            pltpu.VMEM((160, 128), bf16),
            pltpu.VMEM((8 * CPD, 160), bf16),
            pltpu.VMEM((3, EQUIV, 128), f32),
            pltpu.VMEM((7, 16, WIDE), f32),
            pltpu.VMEM((ROWS, 3 * WIDE), bf16),
            pltpu.VMEM((ROWS, 3 * WIDE), bf16),
            pltpu.VMEM((PER_OWNER, 3 * WIDE), bf16),
            pltpu.VMEM((ROWS, PER_OWNER), f32),
            pltpu.VMEM((ROWS, PER_OWNER), f32),
            pltpu.VMEM((16, 128), f32),
            pltpu.VMEM((SHARE_PAD, 2 * WIDE), f32),
            pltpu.VMEM((SHARE_PAD, 2 * WIDE), f32),
            pltpu.VMEM((8, 128), f32),
            dma((sides,)),
            dma((sides,)),
            dma((sides,)),
            dma((sides,)),
            dma((7,)),
            dma,
            dma((7,)),
            dma((7,)),
            dma((24,)),
            dma((24,)),
            dma((32,)),
            dma((32,)),
        ],
        compiler_params=pltpu.CompilerParams(
            collective_id=0, has_side_effects=True, vmem_limit_bytes=LIMIT
        ),
        name="first",
    )(*(in_hbm(x) for x in (displacement, point_leaf, near_list, stiffness, surf, up_inverse)))


def near_kernel(lists, comp_ref, lefts, spots, rights, own_sums, out_ref, even_pairs, odd_pairs, sums):
    portion = lax.axis_index("leaf")

    def pair(index):
        code = lists[index >> 7, index & 127]
        return code >> 6, code & 63

    def multiply(index, products):
        t, c = pair(index)
        w = jnp.clip(lists[7, c] - lists[7, t] + 1, 0, 2)
        products[...] = dot(lefts[3 * t + w], rights[c])

    sums[...] = own_sums[...]
    multiply(0, even_pairs)

    def some_pairs(index, carry):
        for k in range(TOGETHER):
            now, after = (odd_pairs, even_pairs) if k % 2 else (even_pairs, odd_pairs)
            at = TOGETHER * index + k
            multiply(at + 1, after)
            add_pair(comp_ref, sums, *pair(at), now)
        return carry

    lax.fori_loop(0, (lists[2, 0] + (TOGETHER - 1)) // TOGETHER, some_pairs, 0)
    pick_row, pick_lane = iota((SHARE_PAD, WIDE), 0), iota((SHARE_PAD, WIDE), 1)
    pick = (pick_lane == pick_row + SHARE * portion) & (pick_row < SHARE)

    def finish(index, carry):
        for t in (2 * index, 2 * index + 1):
            for a in range(3):
                total = sums[t, a] + spots[t, a] * sums[t, 3]
                column = jnp.sum(total, axis=1, keepdims=True) * inv_eight_pi
                row = jnp.sum(jnp.where(pick, column, 0.0), axis=0, keepdims=True)
                out_ref[a, pl.ds(t, 1), :] = row
        return carry

    lax.fori_loop(0, CPD // 2, finish, 0)


def near_field(lists, comp, lefts, spots, rights, own_sums):
    return pl.pallas_call(
        near_kernel,
        out_shape=jax.ShapeDtypeStruct((3, 8, WIDE), f32),
        in_specs=[SMEM] + [VMEM] * 5,
        out_specs=VMEM,
        scratch_shapes=[
            pltpu.VMEM((SHARE_PAD, 2 * WIDE), f32),
            pltpu.VMEM((SHARE_PAD, 2 * WIDE), f32),
            pltpu.VMEM((CPD, 4, SHARE_PAD, 128), f32),
        ],
        compiler_params=pltpu.CompilerParams(vmem_limit_bytes=LIMIT),
        name="near_field",
    )(lists, comp, lefts, spots, rights, own_sums)


def far_part(
    left_ref,
    quarter_ref,
    gat_ref,
    far_ref,
    far_load,
    surf_ref,
    inverse_ref,
    local_ref,
    far4,
    sources,
    packed,
    pushes,
    mids,
    total,
    quarter,
    even_rows,
    odd_rows,
    even_blocks,
    odd_blocks,
):
    me = lax.axis_index("cells")
    portion = lax.axis_index("leaf")
    lane = iota((16, 128), 1)

    def one_tile(tile, carry):
        for half in range(2):
            rows = [jnp.zeros((16, 128), f32) for _ in range(3)]
            for v in range(4):
                at = 8 * tile + 4 * half + v
                value = gat_ref[at // 8, at - at // 8 * 8]
                for a in range(3):
                    shift = (PER_OWNER * (v - a)) % 128
                    moved = pltpu.roll(value, shift, 1) if shift else value
                    rows[a] = jnp.where(lane // PER_OWNER == v, moved, rows[a])
            top, low = halves(jnp.concatenate(rows, axis=0))
            packed[tile, 0:48, 128 * half : 128 * half + 128] = top
            packed[tile, 48:96, 128 * half : 128 * half + 128] = low
        return carry

    lax.fori_loop(0, 8, one_tile, 0)

    far_load.wait()
    entries = far_ref[...]
    mine = lax.rem(me, 4)
    lane48 = iota((FAR, 128), 1) // PER_OWNER
    picked = jnp.zeros((FAR, 128), i32)
    for place in range(4):
        moved = entries
        for k in range(1, 4):
            turned = pltpu.roll(entries, PER_OWNER * k, 1)
            moved = jnp.where(lax.rem(mine + k, 4) == place, turned, moved)
        far4[place] = moved
    for place in range(4):
        rows = far4[place, pl.ds(place, FAR // 4, stride=4), :]
        chosen = iota((FAR // 4, 128), 1) // PER_OWNER == place
        if place == 0:
            merged = rows
        else:
            merged = jnp.where(chosen, rows, merged)
    owner = merged >> 5
    spot = (((owner & 1) << 5) + (owner >> 1)) * PER_OWNER + (merged & 31)
    sources[0:12, :] = jnp.where(merged >= 0, spot, -1)
    target = me * PER_OWNER + (iota((12, 128), 1) & 31)
    mids[0, 0:12, :] = (2 * ((target >> 4) - (merged >> 4))).astype(f32)
    mids[1, 0:12, :] = (2 * (((target >> 2) & 3) - ((merged >> 2) & 3))).astype(f32)
    mids[2, 0:12, :] = (2 * ((target & 3) - (merged & 3))).astype(f32)

    def gather_two(index):
        first = sources[pl.ds(2 * index, 1), :]
        second = sources[pl.ds(2 * index + 1, 1), :]
        wanted = jnp.concatenate([first, second], axis=1)
        found = jnp.zeros((96, 256), f32)
        for tile in range(8):
            onehot = (iota((256, 256), 0) + 256 * tile == wanted).astype(f32).astype(bf16)
            found = found + dot(packed[tile], onehot)
        value = found[0:48] + found[48:96]
        pushes[2 * index] = value[:, 0:128]
        pushes[2 * index + 1] = value[:, 128:256]

    def some_gathers(index, carry):
        for k in range(3):
            gather_two(3 * index + k)
        return carry

    lax.fori_loop(0, 2, some_gathers, 0)
    total[...] = jnp.zeros_like(total)

    left = left_ref[...].astype(bf16)
    for a in range(3):
        quarter[a] = jnp.broadcast_to(quarter_ref[portion, :, a : a + 1], (16, 128))
    steps = thirds(jnp.full((16, 128), (inner_radius / 3.0) ** 2, f32))
    for rows in (even_rows, odd_rows):
        rows[...] = jnp.zeros_like(rows)
        for k in range(3):
            rows[pl.ds(12 + k, 16, stride=32), :] = steps[k]

    def prepare_block(index, rows, blocks):
        push = [pushes[index, 16 * a : 16 * a + 16, :] for a in range(3)]
        gap = [mids[a, pl.ds(index, 1), :] - quarter[a] for a in range(3)]
        square = (gap[0] * gap[0] + gap[1] * gap[1]) + (gap[2] * gap[2] + smooth_sq)
        inner = (gap[0] * push[0] + gap[1] * push[1]) + gap[2] * push[2]
        scale = inner_radius / 3.0
        for a in range(3):
            for k, third in enumerate(thirds((2.0 * scale) * gap[a])):
                rows[pl.ds(3 * a + k, 16, stride=32), :] = third
            for k, third in enumerate(thirds(scale * push[a])):
                rows[pl.ds(16 + 3 * a + k, 16, stride=32), :] = third
        for k, third in enumerate(thirds(square)):
            rows[pl.ds(9 + k, 16, stride=32), :] = third
        for k, third in enumerate(thirds(inner)):
            rows[pl.ds(25 + k, 16, stride=32), :] = third
        for j in range(14):
            right = jnp.concatenate(
                [rows[32 * j : 32 * j + 16, :], rows[32 * j + 16 : 32 * j + 32, :]], axis=1
            )
            blocks[j] = dot(left, right.astype(bf16))

    def add_block(index, blocks):
        groups = EQUIV // 8
        sums = [[jnp.zeros((8, 128), f32) for _ in range(4)] for _ in range(groups)]
        for j in range(14):
            f = [pushes[index, 16 * a + j : 16 * a + j + 1, :] for a in range(3)]
            shift = [quarter[a, j : j + 1, :] for a in range(3)]
            for g in range(groups):
                at = slice(8 * g, 8 * g + 8)
                shifted = blocks[j, at, 0:128]
                inner = blocks[j, at, 128:256]
                root = lax.rsqrt(shifted)
                cube = root * root * root
                even = root + smooth_sq * cube
                along = cube * inner
                for a in range(3):
                    sums[g][a] = sums[g][a] + (even * f[a] - along * shift[a])
                sums[g][3] = sums[g][3] + along
        mid = [mids[a, pl.ds(index, 1), :] for a in range(3)]
        for g in range(groups):
            at = slice(8 * g, 8 * g + 8)
            for a in range(3):
                check = mid[a] + inner_radius * surf_ref[at, a : a + 1]
                row = EQUIV * a + 8 * g
                total[row : row + 8, :] += sums[g][a] + check * sums[g][3]

    prepare_block(0, even_rows, even_blocks)

    def two_blocks(index, carry):
        prepare_block(2 * index + 1, odd_rows, odd_blocks)
        add_block(2 * index, even_blocks)
        prepare_block(jnp.minimum(2 * index + 2, 11), even_rows, even_blocks)
        add_block(2 * index + 1, odd_blocks)
        return carry

    lax.fori_loop(0, 6, two_blocks, 0)
    value = total[...] * inv_eight_pi
    value = value + pltpu.roll(value, 64, 1)
    value = value + pltpu.roll(value, 32, 1)
    local_ref[...] = dot_wide(inverse_ref[...], value)


def last_kernel(
    left_ref,
    quarter_ref,
    gat_ref,
    far_hbm,
    surf_ref,
    inverse_ref,
    comp_ref,
    near_ref,
    out_ref,
    far_ref,
    load_sem,
    far4,
    sources,
    packed,
    pushes,
    mids,
    total,
    quarter,
    even_rows,
    odd_rows,
    even_blocks,
    odd_blocks,
    local_ref,
    packed_local,
    held_local,
    factors,
    member_ref,
    spread_ref,
    cell_ref,
    part_ref,
    held_part,
    send_local,
    recv_local,
    send_part,
    recv_part,
):
    block = pl.multiple_of(lax.axis_index("cells") // 4 * 128, 128)
    far_load = pltpu.make_async_copy(far_hbm.at[:, pl.ds(block, 128)], far_ref, load_sem)
    far_load.start()
    packed_local[...] = jnp.zeros_like(packed_local)
    sides = beside("cells", (1, -1))
    mates = beside("leaf", (1, 2, 3))
    barrier = pltpu.get_barrier_semaphore()
    for target in (*sides, *mates):
        pl.semaphore_signal(barrier, inc=1, device_id=target, device_id_type=MESH)
    far_part(
        left_ref,
        quarter_ref,
        gat_ref,
        far_ref,
        far_load,
        surf_ref,
        inverse_ref,
        local_ref,
        far4,
        sources,
        packed,
        pushes,
        mids,
        total,
        quarter,
        even_rows,
        odd_rows,
        even_blocks,
        odd_blocks,
    )
    pl.semaphore_wait(barrier, 5)
    lane = iota((48, 128), 1) // PER_OWNER
    for k in range(4):
        rows = min(48, ROWS - 48 * k)
        piece = local_ref[48 * k : 48 * k + rows, :]
        here = lane[0:rows] == k
        packed_local[0:rows, :] = jnp.where(here, piece, packed_local[0:rows, :])
    copies = [
        remote(packed_local, held_local.at[k], send_local.at[k], recv_local.at[k], target)
        for k, target in enumerate(sides)
    ]
    for copy in copies:
        copy.start()
    for t in range(CPD):
        rel = comp_ref[REL, t : t + 1, :].astype(i32) - 3 * PER_OWNER
        member = (iota((128, WIDE), 0) == rel).astype(f32).astype(bf16)
        member_ref[t, 0:128, :] = member
        member_ref[t, 128:256, :] = member
    for copy in copies:
        copy.wait()
    lane = iota((48, 128), 1) // PER_OWNER
    for k in range(4):
        rows = min(48, ROWS - 48 * k)
        value = local_ref[48 * k : 48 * k + rows, :]
        for side in range(2):
            place = 2 * side
            moved = held_local[side, 0:rows, :]
            if place != k:
                moved = pltpu.roll(moved, (PER_OWNER * (place - k)) % 128, 1)
            value = jnp.where(lane[0:rows] == place, moved, value)
        top, low = halves(value)
        factors[48 * k : 48 * k + rows, 0:128] = top
        factors[48 * k : 48 * k + rows, 128:256] = low

    def spread_out(t):
        spread_ref[t] = dot(factors[...], member_ref[t])

    for t in range(CPD):
        spread_out(t)

    def one_cell(t):
        d = [comp_ref[DX + a, pl.ds(t, 1), :] for a in range(3)]
        sums = [jnp.zeros((8, WIDE), f32) for _ in range(3)]
        for g in range(EQUIV // 8):
            at = slice(8 * g, 8 * g + 8)
            r = [d[a] - outer_radius * surf_ref[at, a : a + 1] for a in range(3)]
            f = [spread_ref[t, EQUIV * a + 8 * g : EQUIV * a + 8 * g + 8, :] for a in range(3)]
            even, along = pull(r, f)
            sums = [sums[a] + (even * f[a] + along * r[a]) for a in range(3)]
        for a in range(3):
            row = jnp.sum(sums[a], axis=0, keepdims=True) * inv_eight_pi
            cell_ref[a, pl.ds(t, 1), :] = row + near_ref[a, pl.ds(t, 1), :]

    def two_cells(index, carry):
        one_cell(2 * index)
        one_cell(2 * index + 1)
        return carry

    lax.fori_loop(0, CPD // 2, two_cells, 0)
    for t in range(CPD):
        for a in range(3):
            part_ref[a : a + 1, NPT * t : NPT * (t + 1)] = cell_ref[a, t : t + 1, 0:NPT]
    copies = [
        remote(part_ref, held_part.at[k], send_part.at[k], recv_part.at[k], target)
        for k, target in enumerate(mates)
    ]
    for copy in copies:
        copy.start()
    for copy in copies:
        copy.wait()
    out_ref[...] = (part_ref[...] + held_part[1]) + (held_part[0] + held_part[2])


def last(left, quarter, gathered, far_list, surf, down_inverse, comp, near, npoints):
    dma = pltpu.SemaphoreType.DMA
    return pl.pallas_call(
        last_kernel,
        out_shape=jax.ShapeDtypeStruct((3, npoints), f32),
        in_specs=[VMEM, VMEM, VMEM, HBM] + [VMEM] * 4,
        out_specs=VMEM,
        scratch_shapes=[
            pltpu.VMEM((FAR, 128), i32),
            dma,
            pltpu.VMEM((4, FAR, 128), i32),
            pltpu.VMEM((16, 128), i32),
            pltpu.VMEM((8, 96, 256), bf16),
            pltpu.VMEM((12, FAR, 128), f32),
            pltpu.VMEM((3, 16, 128), f32),
            pltpu.VMEM((ROWS, 128), f32),
            pltpu.VMEM((3, 16, 128), f32),
            pltpu.VMEM((512, 128), f32),
            pltpu.VMEM((512, 128), f32),
            pltpu.VMEM((14, EQUIV, 256), f32),
            pltpu.VMEM((14, EQUIV, 256), f32),
            pltpu.VMEM((ROWS, 128), f32),
            pltpu.VMEM((48, 128), f32),
            pltpu.VMEM((2, 48, 128), f32),
            pltpu.VMEM((ROWS, 256), bf16),
            pltpu.VMEM((CPD, 256, WIDE), bf16),
            pltpu.VMEM((CPD, ROWS, WIDE), f32),
            pltpu.VMEM((3, 8, WIDE), f32),
            pltpu.VMEM((3, npoints), f32),
            pltpu.VMEM((3, 3, npoints), f32),
            dma((2,)),
            dma((2,)),
            dma((3,)),
            dma((3,)),
        ],
        compiler_params=pltpu.CompilerParams(
            collective_id=1, has_side_effects=True, vmem_limit_bytes=LIMIT
        ),
        name="last",
    )(left, quarter, gathered, in_hbm(far_list), surf, down_inverse, comp, near)


def body(displacement, point_leaf, near_list, far_list, stiffness, up_inverse, down_inverse):
    table = surface_table()
    surf = jnp.asarray(np.pad(table, ((0, 0), (0, 5))))
    whole = np.round(3.0 * table)
    ones = np.ones((EQUIV, 3), np.float32)
    square = np.sum(whole * whole, axis=1, keepdims=True)
    left = np.concatenate([np.repeat(whole, 3, axis=1), ones, ones * square, 0.0 * square], axis=1)
    left = jnp.asarray(left.astype(np.float32))
    quarter = inner_radius * table.reshape(4, 14, 3)
    quarter = jnp.asarray(np.pad(quarter, ((0, 0), (0, 2), (0, 5))).astype(np.float32))
    comp, lists, gathered, lefts, spots, rights, own_sums = first(
        displacement, point_leaf, near_list, stiffness, surf, up_inverse
    )
    near = near_field(lists, comp, lefts, spots, rights, own_sums)
    return last(
        left, quarter, gathered, far_list, surf, down_inverse, comp, near, displacement.shape[1]
    )


def solution(mesh):
    in_specs = (P(None, "cells"), P("cells"), P(), P(), P(), P(), P())
    out_specs = P(None, "cells")
    return jax.shard_map(body, mesh=mesh, in_specs=in_specs, out_specs=out_specs, check_vma=False)
```
